8 devices in a mesh: data: 4 (over z, y, x), model: 2 (over core).
Axes of the slice: x: 2, y: 2, z: 1, core: 2. Of those that a mesh axis runs over, the one named last changes fastest.
Arguments:
- teacher_in: bfloat16 [8, 1024, 4096], P('data', 'model')
- student_in: bfloat16 [8, 1024, 2048], P(('data', 'model'))
- teacher_gain: float32 [3, 4096], replicated
- teacher_up: bfloat16 [3, 4096, 16384], P(None, None, 'model')
- teacher_down: bfloat16 [3, 16384, 4096], P(None, 'model')
- student_gain: float32 [1, 2048], replicated
- student_up: bfloat16 [1, 2048, 8192], replicated
- student_down: bfloat16 [1, 8192, 2048], replicated
- student_proj: bfloat16 [1, 4096, 2048], replicated
Outputs:
- output 1: float32 [], replicated
- output 2: float32 [1, 2048, 8192], replicated
- output 3: float32 [1, 8192, 2048], replicated
- output 4: float32 [1, 2048], replicated
- output 5: float32 [1, 4096, 2048], replicated
All inputs are finite; a program needn't handle non-finite values.
Results may differ from the reference program's by a relative error of at most 0.0137251.
Values are sent between devices in bfloat16 or wider.
A program may use at most 2.5 GiB of HBM per device.

```python
import jax
import jax.numpy as jnp
from jax import lax

T_WIDTH = 4096
S_WIDTH = 2048
T_LAYERS = 3
N_FEATS = 1
SEQ_LEN = 1024
N_SEQS = 8
EPS = 1e-6


def setup_inputs(seed: int = 0) -> dict:
    keys = jax.random.split(jax.random.key(seed), 9)
    teach_ff = 4 * T_WIDTH
    stud_ff = 4 * S_WIDTH
    base = jax.random.normal(keys[0], (N_SEQS, SEQ_LEN, T_WIDTH), jnp.float32)
    noise = jax.random.normal(keys[1], (N_SEQS, SEQ_LEN, S_WIDTH), jnp.float32)
    return {
        "teacher_in": base.astype(jnp.bfloat16),
        "student_in": (0.8 * base[:, :, :S_WIDTH] + 0.6 * noise).astype(jnp.bfloat16),
        "teacher_gain": jax.random.uniform(keys[2], (T_LAYERS, T_WIDTH), jnp.float32, 0.25, 1.75),
        "teacher_up": (jax.random.normal(keys[3], (T_LAYERS, T_WIDTH, teach_ff), jnp.float32) * T_WIDTH ** -0.5).astype(jnp.bfloat16),
        "teacher_down": (jax.random.normal(keys[4], (T_LAYERS, teach_ff, T_WIDTH), jnp.float32) * teach_ff ** -0.5).astype(jnp.bfloat16),
        "student_gain": jax.random.uniform(keys[5], (N_FEATS, S_WIDTH), jnp.float32, 0.25, 1.75),
        "student_up": (jax.random.normal(keys[6], (N_FEATS, S_WIDTH, stud_ff), jnp.float32) * S_WIDTH ** -0.5).astype(jnp.bfloat16),
        "student_down": (jax.random.normal(keys[7], (N_FEATS, stud_ff, S_WIDTH), jnp.float32) * stud_ff ** -0.5).astype(jnp.bfloat16),
        "student_proj": (jax.random.normal(keys[8], (N_FEATS, T_WIDTH, S_WIDTH), jnp.float32) * T_WIDTH ** -0.5).astype(jnp.bfloat16),
    }


def rms_unit(values):
    return values * lax.rsqrt(jnp.mean(values * values, axis=-1, keepdims=True) + EPS)


def rms_back(values, grad_out):
    inv_rms = lax.rsqrt(jnp.mean(values * values, axis=-1, keepdims=True) + EPS)
    unit = values * inv_rms
    return inv_rms * (grad_out - unit * jnp.mean(grad_out * unit, axis=-1, keepdims=True))


def gelu_back(pre_act, grad_out):
    return jax.vjp(jax.nn.gelu, pre_act)[1](grad_out)[0]


def reference(teacher_in, student_in, teacher_gain, teacher_up, teacher_down, student_gain, student_up, student_down, student_proj):
    t_step = T_LAYERS // N_FEATS
    total = N_FEATS * N_SEQS * SEQ_LEN * S_WIDTH
    grad_scale = 2.0 / total
    teacher_groups = (
        teacher_gain.reshape(N_FEATS, t_step, T_WIDTH),
        teacher_up.reshape(N_FEATS, t_step, T_WIDTH, 4 * T_WIDTH),
        teacher_down.reshape(N_FEATS, t_step, 4 * T_WIDTH, T_WIDTH),
        student_proj,
    )

    def teacher_layer(hidden, layer):
        gain, w_up, w_down = layer
        act_in = (rms_unit(hidden.astype(jnp.float32)) * gain).astype(jnp.bfloat16)
        up_act = jax.nn.gelu(jnp.dot(act_in, w_up, preferred_element_type=jnp.float32)).astype(jnp.bfloat16)
        delta = jnp.dot(up_act, w_down, preferred_element_type=jnp.float32).astype(jnp.bfloat16)
        return (hidden.astype(jnp.float32) + delta.astype(jnp.float32)).astype(jnp.bfloat16), None

    def feature_group(hidden, group):
        gains, ups, downs, project = group
        hidden, _ = lax.scan(teacher_layer, hidden, (gains, ups, downs))
        target = jnp.dot(hidden, project, preferred_element_type=jnp.float32).astype(jnp.bfloat16)
        return hidden, (hidden, target)

    def student_block(state, block):
        gain, w_up, w_down, target = block
        normed = rms_unit(state.astype(jnp.float32))
        act_in = (normed * gain).astype(jnp.bfloat16)
        pre_act = jnp.dot(act_in, w_up, preferred_element_type=jnp.float32)
        up_act = jax.nn.gelu(pre_act).astype(jnp.bfloat16)
        new_state = (state.astype(jnp.float32) + jnp.dot(up_act, w_down, preferred_element_type=jnp.float32)).astype(jnp.bfloat16)
        error = target.astype(jnp.float32) - rms_unit(new_state.astype(jnp.float32))
        return new_state, (state, new_state, error)

    def student_back(d_res, saved):
        state, new_state, error, gain, w_up, w_down = saved
        d_res = d_res + rms_back(new_state.astype(jnp.float32), -grad_scale * error)
        normed = rms_unit(state.astype(jnp.float32))
        act_in = (normed * gain).astype(jnp.bfloat16)
        pre_act = jnp.dot(act_in, w_up, preferred_element_type=jnp.float32)
        up_act = jax.nn.gelu(pre_act).astype(jnp.bfloat16)
        d_out = d_res.astype(jnp.bfloat16)
        g_down = jnp.dot(up_act.T, d_out, preferred_element_type=jnp.float32)
        d_up = jnp.dot(d_out, w_down.T, preferred_element_type=jnp.float32)
        d_pre = gelu_back(pre_act, d_up).astype(jnp.bfloat16)
        g_up = jnp.dot(act_in.T, d_pre, preferred_element_type=jnp.float32)
        d_act = jnp.dot(d_pre, w_up.T, preferred_element_type=jnp.float32)
        g_gain = jnp.sum(d_act * normed, axis=0)
        d_res = d_res + rms_back(state.astype(jnp.float32), d_act * gain)
        return d_res, (g_up, g_down, g_gain)

    def proj_grad(pair):
        feature, error = pair
        return jnp.dot(feature.T, error.astype(jnp.bfloat16), preferred_element_type=jnp.float32)

    def one_sequence(carry, rows):
        teach_row, stud_row = rows
        _, (features, targets) = lax.scan(feature_group, teach_row, teacher_groups)
        _, saved = lax.scan(student_block, stud_row, (student_gain, student_up, student_down, targets))
        states, new_states, errors = saved
        _, (g_up, g_down, g_gain) = lax.scan(
            student_back,
            jnp.zeros((SEQ_LEN, S_WIDTH), jnp.float32),
            (states, new_states, errors, student_gain, student_up, student_down),
            reverse=True,
        )
        g_proj = grad_scale * lax.map(proj_grad, (features, errors))
        increment = (jnp.sum(errors * errors), g_up, g_down, g_gain, g_proj)
        return jax.tree.map(jnp.add, carry, increment), None

    start_sums = (
        jnp.zeros((), jnp.float32),
        jnp.zeros((N_FEATS, S_WIDTH, 4 * S_WIDTH), jnp.float32),
        jnp.zeros((N_FEATS, 4 * S_WIDTH, S_WIDTH), jnp.float32),
        jnp.zeros((N_FEATS, S_WIDTH), jnp.float32),
        jnp.zeros((N_FEATS, T_WIDTH, S_WIDTH), jnp.float32),
    )
    totals, _ = lax.scan(one_sequence, start_sums, (teacher_in, student_in))
    return (totals[0] / total, totals[1], totals[2], totals[3], totals[4])
```

```python
import functools

import jax
import jax.numpy as jnp
from jax import lax
from jax.experimental import pallas as pl
from jax.experimental.pallas import tpu as pltpu
from jax.sharding import PartitionSpec as P


EPS = 1e-6
VMEM_CAP = 64 * 1024 * 1024 - 65536
AXES = ("data", "model")


def after(values, dep):
    return lax.optimization_barrier((values, dep))[0]


def rms_unit(values):
    return values * lax.rsqrt(jnp.mean(values * values, axis=-1, keepdims=True) + EPS)


def up_kernel(sub, a_ref, w_ref, u_ref):
    for j in range(u_ref.shape[1] // sub):
        cols = slice(j * sub, (j + 1) * sub)
        acc = jnp.dot(a_ref[...], w_ref[:, cols], preferred_element_type=jnp.float32)
        u_ref[:, cols] = jax.nn.gelu(acc).astype(jnp.bfloat16)


def teacher_up(act, weights, layer, tn=1024, sub=256):
    rows, depth = act.shape
    cols = weights.shape[2]
    return pl.pallas_call(
        functools.partial(up_kernel, sub),
        grid=(cols // tn,),
        in_specs=[
            pl.BlockSpec((rows, depth), lambda j: (0, 0)),
            pl.BlockSpec((None, depth, tn), lambda j: (layer, 0, j)),
        ],
        out_specs=pl.BlockSpec((rows, tn), lambda j: (0, j)),
        out_shape=jax.ShapeDtypeStruct((rows, cols), jnp.bfloat16),
        compiler_params=pltpu.CompilerParams(vmem_limit_bytes=VMEM_CAP),
        cost_estimate=pl.CostEstimate(
            flops=2 * rows * depth * cols,
            bytes_accessed=2 * (rows * depth + depth * cols + rows * cols),
            transcendentals=rows * cols,
        ),
        name="teacher_up",
    )(act, weights)


def norm_kernel(h_ref, g_ref, a_ref):
    state = h_ref[...].astype(jnp.float32)
    inv = lax.rsqrt(jnp.mean(state * state, axis=-1, keepdims=True) + EPS)
    a_ref[...] = (state * inv * g_ref[...]).astype(jnp.bfloat16)


def step_kernel(h_ref, y_ref, g_ref, o_ref, a_ref):
    state = (h_ref[...].astype(jnp.float32) + y_ref[...].astype(jnp.float32)).astype(jnp.bfloat16)
    o_ref[...] = state
    state = state.astype(jnp.float32)
    inv = lax.rsqrt(jnp.mean(state * state, axis=-1, keepdims=True) + EPS)
    a_ref[...] = (state * inv * g_ref[...]).astype(jnp.bfloat16)


def teacher_norm(hidden, delta, gains, layer, block=128):
    rows, width = hidden.shape
    spec = pl.BlockSpec((block, width), lambda i: (i, 0))
    gain_spec = pl.BlockSpec((1, width), lambda i: (0, 0))
    shape = jax.ShapeDtypeStruct((rows, width), jnp.bfloat16)
    count = rows * width
    common = dict(
        grid=(rows // block,),
        compiler_params=pltpu.CompilerParams(vmem_limit_bytes=48 * 1024 * 1024),
    )
    gain = gains[layer : layer + 1]
    if delta is None:
        cost = pl.CostEstimate(flops=8 * count, bytes_accessed=4 * count, transcendentals=0)
        return hidden, pl.pallas_call(norm_kernel, in_specs=[spec, gain_spec], out_specs=spec, out_shape=shape, cost_estimate=cost, name="norm", **common)(hidden, gain)
    cost = pl.CostEstimate(flops=10 * count, bytes_accessed=8 * count, transcendentals=0)
    return pl.pallas_call(step_kernel, in_specs=[spec, spec, gain_spec], out_specs=[spec, spec], out_shape=[shape, shape], cost_estimate=cost, name="step", **common)(hidden, delta, gain)


def error_kernel(grad_scale, z_ref, s_ref, e_ref, d_ref, sq_ref):
    @pl.when((pl.program_id(0) == 0) & (pl.program_id(1) == 0))
    def _():
        sq_ref[...] = jnp.zeros_like(sq_ref)

    state = s_ref[...].astype(jnp.float32)
    inv = lax.rsqrt(jnp.mean(state * state, axis=-1, keepdims=True) + EPS)
    unit = state * inv
    error = z_ref[...].astype(jnp.float32) - unit
    lean = jnp.mean(error * unit, axis=-1, keepdims=True)
    e_ref[...] = error.astype(jnp.bfloat16)
    d_ref[...] = ((error - unit * lean) * (-grad_scale * inv)).astype(jnp.bfloat16)
    rows, width = error.shape
    sq_ref[...] += jnp.sum((error * error).reshape(rows // 8, 8, width), axis=0)


def errors_of(targets, states, parity, grad_scale, block=256):
    n_seq, seq_len, width = states.shape
    half = n_seq // 2
    spec = pl.BlockSpec((None, block, width), lambda i, j: (i, j, 0))
    shape = jax.ShapeDtypeStruct((half, seq_len, width), jnp.bfloat16)
    count = half * seq_len * width
    return pl.pallas_call(
        functools.partial(error_kernel, grad_scale),
        grid=(half, seq_len // block),
        in_specs=[spec, pl.BlockSpec((None, block, width), lambda i, j: (2 * i + parity, j, 0))],
        out_specs=[spec, spec, pl.BlockSpec((8, width), lambda i, j: (0, 0))],
        out_shape=[shape, shape, jax.ShapeDtypeStruct((8, width), jnp.float32)],
        compiler_params=pltpu.CompilerParams(vmem_limit_bytes=48 * 1024 * 1024),
        cost_estimate=pl.CostEstimate(flops=16 * count, bytes_accessed=8 * count, transcendentals=0),
        name="errors",
    )(targets.reshape(half, seq_len, width), states)


def act_kernel(s_ref, g_ref, a_ref):
    state = s_ref[...].astype(jnp.float32)
    inv = lax.rsqrt(jnp.mean(state * state, axis=-1, keepdims=True) + EPS)
    a_ref[...] = (state * inv * g_ref[...]).astype(jnp.bfloat16)


def acts_of(states, gain, parity, block=256):
    n_seq, seq_len, width = states.shape
    half = n_seq // 2
    count = half * seq_len * width
    return pl.pallas_call(
        act_kernel,
        grid=(half, seq_len // block),
        in_specs=[
            pl.BlockSpec((None, block, width), lambda i, j: (2 * i + parity, j, 0)),
            pl.BlockSpec((1, width), lambda i, j: (0, 0)),
        ],
        out_specs=pl.BlockSpec((None, block, width), lambda i, j: (i, j, 0)),
        out_shape=jax.ShapeDtypeStruct((half, seq_len, width), jnp.bfloat16),
        compiler_params=pltpu.CompilerParams(vmem_limit_bytes=48 * 1024 * 1024),
        cost_estimate=pl.CostEstimate(flops=8 * count, bytes_accessed=4 * count, transcendentals=0),
        name="acts",
    )(states, gain).reshape(half * seq_len, width)


def place_kernel(where_ref, piece_ref, *rest):
    rest[-1][...] = piece_ref[...].astype(jnp.float32)


def place(out, piece, where, shape, block):
    rows, cols = piece.shape
    steps = rows // block
    specs = [pl.BlockSpec((block, cols), lambda i, w: (i, 0))]
    args = [where, piece]
    alias = {}
    if out is not None:
        specs.append(pl.BlockSpec(memory_space=pl.ANY))
        args.append(out)
        alias = {2: 0}
    return pl.pallas_call(
        place_kernel,
        grid_spec=pltpu.PrefetchScalarGridSpec(
            num_scalar_prefetch=1,
            grid=(steps,),
            in_specs=specs,
            out_specs=pl.BlockSpec((block, cols), lambda i, w: (w[0] * steps + i, w[1])),
        ),
        out_shape=jax.ShapeDtypeStruct(shape, jnp.float32),
        input_output_aliases=alias,
        compiler_params=pltpu.CompilerParams(vmem_limit_bytes=32 * 1024 * 1024),
        cost_estimate=pl.CostEstimate(flops=rows * cols, bytes_accessed=6 * rows * cols, transcendentals=0),
        name="place",
    )(*args)


def flip(value, bits, size):
    return lax.ppermute(value, AXES, [(i, i ^ bits) for i in range(size)])


def share(halves, me, size, shape, by_cols, block):
    first, second = halves
    x_first, y_second = flip(first, 2, size), flip(second, 4, size)
    x_second, y_first = flip(second, 2, size), flip(first, 4, size)
    d_second, d_first = flip(y_second, 2, size), flip(x_first, 4, size)
    have = [(0, 0, first), (0, 1, second), (2, 0, x_first), (4, 1, y_second), (2, 1, x_second), (4, 0, y_first), (6, 1, d_second), (6, 0, d_first)]
    other = [(bits | 1, half, flip(value, 1, size)) for bits, half, value in have]
    out = None
    for pair in zip(have, other):
        for bits, half, value in pair:
            owner = me ^ bits
            where = jnp.stack([jnp.int32(half), owner]) if by_cols else jnp.stack([2 * owner + half, jnp.int32(0)])
            out = place(out, value, where.astype(jnp.int32), shape, block)
    return out


def gelu_back(pre_act, grad_out):
    return jax.vjp(jax.nn.gelu, pre_act)[1](grad_out)[0]


def dot(a, b, dims):
    return lax.dot_general(a, b, (dims, ((), ())), preferred_element_type=jnp.float32)


def solution(mesh):
    size = mesh.shape["data"] * mesh.shape["model"]

    def step(teacher_in, student_in, teacher_gain, teacher_up_w, teacher_down, student_gain, student_up, student_down, student_proj):
        me = lax.axis_index("data") * 2 + lax.axis_index("model")
        n_layers = teacher_up_w.shape[0]
        t_width = teacher_in.shape[2]
        _, seq_len, s_width = student_in.shape
        s_hidden = student_up.shape[2]
        part = s_hidden // size
        t_part = t_width // size
        total = size * seq_len * s_width
        grad_scale = 2.0 / total
        gain = student_gain[0]
        v_up, v_down, q_proj = student_up[0], student_down[0], student_proj[0]

        targets, feats = [], []

        def finish(c):
            hidden[c] = (hidden[c].astype(jnp.float32) + delta[c].astype(jnp.float32)).astype(jnp.bfloat16)
            target = dot(hidden[c], q_proj, ((1,), (0,))).astype(jnp.bfloat16)
            targets.append(lax.all_gather(target, AXES, axis=0, tiled=True))
            return target

        def columns(source):
            rows = source.shape[0]
            feat = jnp.zeros((size * rows, t_part), jnp.bfloat16)
            for bits in range(size):
                other = me ^ bits
                piece = lax.dynamic_slice(source, (0, other * t_part), (rows, t_part))
                if bits:
                    piece = flip(piece, bits, size)
                feat = lax.dynamic_update_slice(feat, piece, (other * rows, 0))
            return feat

        own = student_in[0]
        all_in = lax.all_gather(own, AXES, axis=0, tiled=False)

        hidden = [teacher_in[c] for c in range(2)]
        delta = [None, None]
        for layer in range(n_layers):
            if layer == 1:
                own_act = (rms_unit(own.astype(jnp.float32)) * gain).astype(jnp.bfloat16)
                own_up = jax.nn.gelu(dot(own_act, v_up, ((1,), (0,)))).astype(jnp.bfloat16)
                own_out = (own.astype(jnp.float32) + dot(own_up, v_down, ((1,), (0,)))).astype(jnp.bfloat16)
                delta[1] = after(delta[1], (own_out, all_in))
                all_out = lax.all_gather(own_out, AXES, axis=0, tiled=False)
            if layer == 2:
                delta[1] = after(delta[1], all_out)
            for c in range(2):
                hidden[c], act = teacher_norm(hidden[c], delta[c], teacher_gain, layer)
                act = lax.all_gather(act, "model", axis=0, tiled=True)
                up_act = teacher_up(act, teacher_up_w, layer)
                if layer == n_layers - 1 and c == 1:
                    up_act = after(up_act, finish(0))
                partial = dot(up_act, teacher_down[layer], ((1,), (0,))).astype(jnp.bfloat16)
                delta[c] = lax.psum_scatter(partial, "model", scatter_dimension=0, tiled=True)

        target = finish(1)
        feats.append(columns(hidden[0]))
        feats.append(columns(after(hidden[1], targets[1])))

        all_in, all_out, targets[0] = after((all_in, all_out, targets[0]), target)
        up_part = lax.dynamic_slice(v_up, (0, me * part), (s_width, part))
        down_part = lax.dynamic_slice(v_down, (me * part, 0), (part, s_width))
        acts = [acts_of(all_in, student_gain, c) for c in range(2)]
        pre = [dot(acts[c], up_part, ((1,), (0,))) for c in range(2)]
        ups = [jax.nn.gelu(pre[c]).astype(jnp.bfloat16) for c in range(2)]
        errors, d_outs, squares = [], [], []
        for c in range(2):
            if c == 1:
                targets[1] = after(targets[1], (ups, errors[0]))
            error, d_out, square = errors_of(targets[c], all_out, c, grad_scale)
            errors.append(error.reshape(-1, s_width))
            d_outs.append(d_out.reshape(-1, s_width))
            squares.append(square)
        loss = (jnp.sum(squares[0]) + jnp.sum(squares[1])) / total

        def both(make):
            return (make(0) + make(1)).astype(jnp.bfloat16)

        halves_down = [both(lambda c: dot(ups[c][:, h * part // 2 : (h + 1) * part // 2], d_outs[c], ((0,), (0,)))) for h in range(2)]
        grad_down = share(halves_down, me, size, (s_hidden, s_width), False, 256)

        d_outs = after(d_outs, halves_down)
        d_pres = [gelu_back(pre[c], dot(d_outs[c], down_part, ((1,), (1,)))).astype(jnp.bfloat16) for c in range(2)]
        halves_up = [both(lambda c: dot(acts[c][:, h * s_width // 2 : (h + 1) * s_width // 2], d_pres[c], ((0,), (0,)))) for h in range(2)]
        grad_up = share(halves_up, me, size, (s_width, s_hidden), True, 512)

        errors = after(errors, halves_up)
        halves_proj = []
        for h in range(2):
            cols = slice(h * t_part // 2, (h + 1) * t_part // 2)
            halves_proj.append((grad_scale * (dot(feats[0][:, cols], errors[0], ((0,), (0,))) + dot(feats[1][:, cols], errors[1], ((0,), (0,))))).astype(jnp.bfloat16))
        grad_proj = share(halves_proj, me, size, (t_width, s_width), False, 256)

        d_pres = after(d_pres, halves_proj)
        gain_sum = jnp.zeros((s_width,), jnp.float32)
        seqs = all_in.reshape(size // 2, 2, seq_len, s_width)
        for c in range(2):
            d_act = dot(d_pres[c], up_part, ((1,), (1,))).reshape(size // 2, seq_len, s_width)
            gain_sum = gain_sum + jnp.sum(d_act * rms_unit(seqs[:, c].astype(jnp.float32)), axis=(0, 1))
        grad_gain = lax.psum(gain_sum, AXES)
        return (loss, grad_up[None], grad_down[None], grad_gain[None], grad_proj[None])

    return jax.shard_map(
        step,
        mesh=mesh,
        in_specs=(
            P("data", "model", None),
            P(("data", "model"), None, None),
            P(),
            P(None, None, "model"),
            P(None, "model", None),
            P(),
            P(),
            P(),
            P(),
        ),
        out_specs=(P(), P(), P(), P(), P()),
        check_vma=False,
    )
```

```python
import functools

import jax
import jax.numpy as jnp
from jax import lax
from jax.experimental import pallas as pl
from jax.experimental.pallas import tpu as pltpu
from jax.sharding import PartitionSpec as P


EPS = 1e-6
VMEM_CAP = 64 * 1024 * 1024 - 65536
AXES = ("data", "model")


def after(values, dep):
    return lax.optimization_barrier((values, dep))[0]


def rms_unit(values):
    return values * lax.rsqrt(jnp.mean(values * values, axis=-1, keepdims=True) + EPS)


def mlp_kernel(layer, steps, wide, residual, where_ref, *refs):
    if residual:
        a_hbm, up_hbm, down_hbm, s_hbm, o_hbm, a_ref, up_ref, down_ref, first, second, act, acc, out, a_sem, up_sem, down_sem, o_sem, s_ref, s_sem = refs
    else:
        a_hbm, up_hbm, down_hbm, o_hbm, a_ref, up_ref, down_ref, first, second, act, acc, out, a_sem, up_sem, down_sem, o_sem = refs
    j = pl.program_id(0)
    rows, width = acc.shape
    tile = act.shape[2]
    half = tile // 2
    parts = 4
    size = rows // parts
    now = lax.rem(j, 2)

    def a_copy(r):
        source = pl.ds(pl.multiple_of(where_ref[0] * rows + r * size, size), size)
        return pltpu.make_async_copy(a_hbm.at[source], a_ref.at[pl.ds(r * size, size)], a_sem.at[r])

    def up_copy(k):
        return pltpu.make_async_copy(up_hbm.at[layer, :, pl.ds(pl.multiple_of(k * tile, tile), tile)], up_ref.at[lax.rem(k, 2)], up_sem.at[lax.rem(k, 2)])

    def down_copy(k):
        return pltpu.make_async_copy(down_hbm.at[layer, pl.ds(pl.multiple_of(k * tile, tile), tile)], down_ref.at[lax.rem(k, 2)], down_sem.at[lax.rem(k, 2)])

    def out_copy(k):
        cols = pl.ds(k * wide, wide)
        return pltpu.make_async_copy(out.at[:, cols], o_hbm.at[:, cols], o_sem.at[k])

    @pl.when(j == 0)
    def _():
        up_copy(0).start()
        for r in range(parts):
            a_copy(r).start()
        up_copy(1).start()
        down_copy(0).start()
        if residual:
            pltpu.make_async_copy(s_hbm, s_ref, s_sem.at[0]).start()
        up_copy(0).wait()
        for r in range(parts):
            part = slice(r * size, (r + 1) * size)
            a_copy(r).wait()
            first[part, :] = jnp.dot(a_ref[part, :], up_ref[0, :, :half], preferred_element_type=jnp.float32)
            second[part, :] = jnp.dot(a_ref[part, :], up_ref[0, :, half:], preferred_element_type=jnp.float32)
        act[0, :, :half] = jax.nn.gelu(first[...]).astype(jnp.bfloat16)

    @pl.when((j > 0) & (j < steps))
    def _():
        @pl.when(j + 1 < steps)
        def _():
            up_copy(j + 1).start()

        down_copy(j).start()
        up_copy(j).wait()
        act[1 - now, :, half:] = jax.nn.gelu(second[...]).astype(jnp.bfloat16)
        first[...] = jnp.dot(a_ref[...], up_ref[now, :, :half], preferred_element_type=jnp.float32)
        for r in range(parts):
            part = slice(r * size, (r + 1) * size)
            act[now, part, :half] = jax.nn.gelu(first[part, :]).astype(jnp.bfloat16)
            second[part, :] = jnp.dot(a_ref[part, :], up_ref[now, :, half:], preferred_element_type=jnp.float32)

    @pl.when(j == steps)
    def _():
        act[1 - now, :, half:] = jax.nn.gelu(second[...]).astype(jnp.bfloat16)

    def down(first_tile, last_tile):
        down_copy(j - 1).wait()
        if last_tile and residual:
            pltpu.make_async_copy(s_hbm, s_ref, s_sem.at[0]).wait()
        for k in range(width // wide):
            cols = slice(k * wide, (k + 1) * wide)
            total = jnp.dot(act[1 - now], down_ref[1 - now, :, cols], preferred_element_type=jnp.float32)
            if not first_tile:
                total = acc[:, cols] + total
            if not last_tile:
                acc[:, cols] = total
            else:
                if residual:
                    total = s_ref[:, cols].astype(jnp.float32) + total
                out[:, cols] = total.astype(jnp.bfloat16)
                out_copy(k).start()
        if last_tile:
            for k in range(width // wide):
                out_copy(k).wait()

    @pl.when(j == 1)
    def _():
        down(True, False)

    @pl.when((j > 1) & (j < steps))
    def _():
        down(False, False)

    @pl.when(j == steps)
    def _():
        down(False, True)


def mlp(a, up, down, layer, state=None, rows=None, where=None, tile=512, wide=512):
    depth = a.shape[1]
    rows = rows or a.shape[0]
    where = jnp.zeros((1,), jnp.int32) if where is None else where.astype(jnp.int32).reshape(1)
    hidden = up.shape[2]
    width = down.shape[2]
    steps = hidden // tile
    hbm = pl.BlockSpec(memory_space=pl.ANY)
    scratch = [
        pltpu.VMEM((rows, depth), jnp.bfloat16),
        pltpu.VMEM((2, depth, tile), jnp.bfloat16),
        pltpu.VMEM((2, tile, width), jnp.bfloat16),
        pltpu.VMEM((rows, tile // 2), jnp.float32),
        pltpu.VMEM((rows, tile // 2), jnp.float32),
        pltpu.VMEM((2, rows, tile), jnp.bfloat16),
        pltpu.VMEM((rows, width), jnp.float32),
        pltpu.VMEM((rows, width), jnp.bfloat16),
        pltpu.SemaphoreType.DMA((4,)),
        pltpu.SemaphoreType.DMA((2,)),
        pltpu.SemaphoreType.DMA((2,)),
        pltpu.SemaphoreType.DMA((width // wide,)),
    ]
    args = [a, up, down]
    if state is not None:
        args.append(state)
        scratch += [pltpu.VMEM((rows, width), jnp.bfloat16), pltpu.SemaphoreType.DMA((1,))]
    return pl.pallas_call(
        functools.partial(mlp_kernel, layer, steps, wide, state is not None),
        grid_spec=pltpu.PrefetchScalarGridSpec(
            num_scalar_prefetch=1,
            grid=(steps + 1,),
            in_specs=[hbm] * len(args),
            out_specs=hbm,
            scratch_shapes=scratch,
        ),
        out_shape=jax.ShapeDtypeStruct((rows, width), jnp.bfloat16),
        compiler_params=pltpu.CompilerParams(vmem_limit_bytes=VMEM_CAP),
        cost_estimate=pl.CostEstimate(
            flops=2 * rows * hidden * (depth + width),
            bytes_accessed=2 * (rows * (depth + width) + hidden * (depth + width)),
            transcendentals=rows * hidden,
        ),
        name="mlp",
    )(where, *args)


def norm_kernel(h_ref, g_ref, a_ref):
    state = h_ref[...].astype(jnp.float32)
    inv = lax.rsqrt(jnp.mean(state * state, axis=-1, keepdims=True) + EPS)
    a_ref[...] = (state * inv * g_ref[...]).astype(jnp.bfloat16)


def step_kernel(h_ref, *refs):
    *parts, g_ref, o_ref, a_ref = refs
    delta = parts[0][...].astype(jnp.float32)
    if len(parts) > 1:
        delta = (delta + parts[1][...].astype(jnp.float32)).astype(jnp.bfloat16).astype(jnp.float32)
    state = (h_ref[...].astype(jnp.float32) + delta).astype(jnp.bfloat16)
    o_ref[...] = state
    state = state.astype(jnp.float32)
    inv = lax.rsqrt(jnp.mean(state * state, axis=-1, keepdims=True) + EPS)
    a_ref[...] = (state * inv * g_ref[...]).astype(jnp.bfloat16)


def teacher_norm(hidden, delta, gains, layer, which=0, block=128):
    rows, width = hidden.shape[-2:]
    spec = pl.BlockSpec((block, width), lambda i: (i, 0))
    source = spec if hidden.ndim == 2 else pl.BlockSpec((None, block, width), lambda i: (which, i, 0))
    gain_spec = pl.BlockSpec((1, width), lambda i: (0, 0))
    shape = jax.ShapeDtypeStruct((rows, width), jnp.bfloat16)
    count = rows * width
    common = dict(
        grid=(rows // block,),
        compiler_params=pltpu.CompilerParams(vmem_limit_bytes=VMEM_CAP),
    )
    gain = gains[layer : layer + 1]
    if not delta:
        cost = pl.CostEstimate(flops=8 * count, bytes_accessed=4 * count, transcendentals=0)
        return hidden, pl.pallas_call(norm_kernel, in_specs=[source, gain_spec], out_specs=spec, out_shape=shape, cost_estimate=cost, name="norm", **common)(hidden, gain)
    cost = pl.CostEstimate(flops=10 * count, bytes_accessed=8 * count, transcendentals=0)
    return pl.pallas_call(step_kernel, in_specs=[source] + [spec] * len(delta) + [gain_spec], out_specs=[spec, spec], out_shape=[shape, shape], cost_estimate=cost, name="step", **common)(hidden, *delta, gain)


def pre_kernel(sub, s_ref, g_ref, w_ref, a_ref, p_ref, u_ref):
    for r in range(s_ref.shape[0] // sub):
        part = slice(r * sub, (r + 1) * sub)
        state = s_ref[part, :].astype(jnp.float32)
        inv = lax.rsqrt(jnp.mean(state * state, axis=-1, keepdims=True) + EPS)
        a_ref[part, :] = (state * inv * g_ref[...]).astype(jnp.bfloat16)
    for r in range(s_ref.shape[0] // sub):
        part = slice(r * sub, (r + 1) * sub)
        pre = jnp.dot(a_ref[part, :], w_ref[...], preferred_element_type=jnp.float32)
        p_ref[part, :] = pre
        u_ref[part, :] = jax.nn.gelu(pre).astype(jnp.bfloat16)


def pre_of(states, gain, weights, parity, block=512, sub=256):
    n_seq, seq_len, width = states.shape
    cols = weights.shape[1]
    half = n_seq // 2
    rows = half * seq_len
    steps = seq_len // block
    out = lambda w: pl.BlockSpec((block, w), lambda i, j: (i * steps + j, 0))
    return pl.pallas_call(
        functools.partial(pre_kernel, sub),
        grid=(half, steps),
        in_specs=[
            pl.BlockSpec((None, block, width), lambda i, j: (2 * i + parity, j, 0)),
            pl.BlockSpec((1, width), lambda i, j: (0, 0)),
            pl.BlockSpec((width, cols), lambda i, j: (0, 0)),
        ],
        out_specs=[out(width), out(cols), out(cols)],
        out_shape=[
            jax.ShapeDtypeStruct((rows, width), jnp.bfloat16),
            jax.ShapeDtypeStruct((rows, cols), jnp.float32),
            jax.ShapeDtypeStruct((rows, cols), jnp.bfloat16),
        ],
        compiler_params=pltpu.CompilerParams(vmem_limit_bytes=VMEM_CAP),
        cost_estimate=pl.CostEstimate(flops=2 * rows * width * cols, bytes_accessed=rows * (4 * width + 6 * cols), transcendentals=rows * cols),
        name="pre",
    )(states, gain, weights)


def proj_kernel(scale, first, last, me_ref, f_ref, z_ref, s_ref, *refs):
    state = s_ref[...].astype(jnp.float32)
    inv = lax.rsqrt(jnp.mean(state * state, axis=-1, keepdims=True) + EPS)
    error = z_ref[...].astype(jnp.float32) - state * inv
    rows, width = error.shape
    out_ref, sq_ref = refs[-3:-1]
    total = refs[-1]
    k = pl.program_id(0)

    @pl.when(k == 0)
    def _():
        sq_ref[...] = jnp.zeros_like(sq_ref)
        if first:
            total[...] = jnp.zeros_like(total)
        else:
            total[...] = refs[0][...]

    sq_ref[...] += jnp.sum((error * error).reshape(rows // 8, 8, width), axis=0)
    total[...] += lax.dot_general(f_ref[...], error.astype(jnp.bfloat16), (((0,), (0,)), ((), ())), preferred_element_type=jnp.float32)

    @pl.when(k == pl.num_programs(0) - 1)
    def _():
        out_ref[...] = (scale * total[...]).astype(jnp.bfloat16) if last else total[...]


def proj_part(me, feat, targets, states, parity, scale, total, last):
    n_seq, _, width = states.shape
    size = n_seq
    cols = feat.shape[1]
    rows = feat.shape[0] // size
    whole = pl.BlockSpec((cols, width), lambda k, me: (0, 0))
    in_specs = [
        pl.BlockSpec((rows, cols), lambda k, me: (k, 0)),
        pl.BlockSpec((rows, width), lambda k, me: (me[0] ^ k, 0)),
        pl.BlockSpec((None, rows, width), lambda k, me: (2 * ((me[0] ^ k) // 2) + parity, (me[0] ^ k) % 2, 0)),
    ]
    args = [me.reshape(1), feat, targets, states]
    if total is not None:
        in_specs.append(whole)
        args.append(total)
    return pl.pallas_call(
        functools.partial(proj_kernel, scale, total is None, last),
        grid_spec=pltpu.PrefetchScalarGridSpec(
            num_scalar_prefetch=1,
            grid=(size,),
            in_specs=in_specs,
            out_specs=[whole, pl.BlockSpec((8, width), lambda k, me: (0, 0))],
            scratch_shapes=[pltpu.VMEM((cols, width), jnp.float32)],
        ),
        out_shape=[
            jax.ShapeDtypeStruct((cols, width), jnp.bfloat16 if last else jnp.float32),
            jax.ShapeDtypeStruct((8, width), jnp.float32),
        ],
        compiler_params=pltpu.CompilerParams(vmem_limit_bytes=VMEM_CAP),
        cost_estimate=pl.CostEstimate(flops=2 * size * rows * cols * width, bytes_accessed=size * rows * (4 * width + 2 * cols), transcendentals=0),
        name="proj",
    )(*args)


def down_kernel(scale, first, z_ref, s_ref, u_ref, *refs):
    d_ref, out_ref, total = refs[-3:]
    k = pl.program_id(0) * pl.num_programs(1) + pl.program_id(1)

    @pl.when(k == 0)
    def _():
        total[...] = jnp.zeros_like(total) if first else refs[0][...]

    state = s_ref[...].astype(jnp.float32)
    inv = lax.rsqrt(jnp.mean(state * state, axis=-1, keepdims=True) + EPS)
    unit = state * inv
    error = z_ref[...].astype(jnp.float32) - unit
    lean = jnp.mean(error * unit, axis=-1, keepdims=True)
    d_out = ((error - unit * lean) * (-scale * inv)).astype(jnp.bfloat16)
    d_ref[...] = d_out
    cols = total.shape[0]
    for h in range(4):
        part = slice(h * cols // 4, (h + 1) * cols // 4)
        total[part, :] += lax.dot_general(u_ref[:, part], d_out, (((0,), (0,)), ((), ())), preferred_element_type=jnp.float32)

    @pl.when(k == pl.num_programs(0) * pl.num_programs(1) - 1)
    def _():
        out_ref[...] = total[...].astype(out_ref.dtype)


def down_part_of(ups, targets, states, parity, scale, total, last, block=512):
    n_seq, seq_len, width = states.shape
    half = n_seq // 2
    cols = ups.shape[1]
    rows = half * seq_len
    steps = seq_len // block
    spec = lambda w: pl.BlockSpec((block, w), lambda i, j: (i * steps + j, 0))
    whole = pl.BlockSpec((cols, width), lambda i, j: (0, 0), pipeline_mode=pl.Buffered(1))
    in_specs = [spec(width), pl.BlockSpec((None, block, width), lambda i, j: (2 * i + parity, j, 0)), spec(cols)]
    args = [targets, states, ups]
    if total is not None:
        in_specs.append(whole)
        args.append(total)
    return pl.pallas_call(
        functools.partial(down_kernel, scale, total is None),
        grid=(half, steps),
        in_specs=in_specs,
        out_specs=[spec(width), whole],
        out_shape=[
            jax.ShapeDtypeStruct((rows, width), jnp.bfloat16),
            jax.ShapeDtypeStruct((cols, width), jnp.bfloat16 if last else jnp.float32),
        ],
        scratch_shapes=[pltpu.VMEM((cols, width), jnp.float32)],
        compiler_params=pltpu.CompilerParams(vmem_limit_bytes=VMEM_CAP),
        cost_estimate=pl.CostEstimate(flops=2 * rows * width * cols, bytes_accessed=rows * (6 * width + 2 * cols), transcendentals=0),
        name="down",
    )(*args)


def spread_kernel(piece_ref, *rest):
    rest[-1][...] = piece_ref[...].astype(jnp.float32)


def spread(out, pieces, first_row, shape, block=512):
    count, rows, cols = pieces.shape
    specs = [pl.BlockSpec((None, block, cols), lambda k, i: (k, i, 0))]
    args = [pieces]
    alias = {}
    if out is not None:
        specs.append(pl.BlockSpec(memory_space=pl.ANY))
        args.append(out)
        alias = {1: 0}
    return pl.pallas_call(
        spread_kernel,
        grid=(count, rows // block),
        in_specs=specs,
        out_specs=pl.BlockSpec((block, cols), lambda k, i: (first_row // block + i, k)),
        out_shape=jax.ShapeDtypeStruct(shape, jnp.float32),
        input_output_aliases=alias,
        compiler_params=pltpu.CompilerParams(vmem_limit_bytes=VMEM_CAP),
        cost_estimate=pl.CostEstimate(flops=count * rows * cols, bytes_accessed=6 * count * rows * cols, transcendentals=0),
        name="spread",
    )(*args)


def flip(value, bits, size):
    return lax.ppermute(value, AXES, [(i, i ^ bits) for i in range(size)])


def gelu_back(pre_act, grad_out):
    return jax.vjp(jax.nn.gelu, pre_act)[1](grad_out)[0]


def dot(a, b, dims):
    return lax.dot_general(a, b, (dims, ((), ())), preferred_element_type=jnp.float32)


def solution(mesh):
    size = mesh.shape["data"] * mesh.shape["model"]

    def step(teacher_in, student_in, teacher_gain, teacher_up_w, teacher_down, student_gain, student_up, student_down, student_proj):
        me = lax.axis_index("data") * 2 + lax.axis_index("model")
        n_layers = teacher_up_w.shape[0]
        t_width = teacher_in.shape[2]
        _, seq_len, s_width = student_in.shape
        s_hidden = student_up.shape[2]
        part = s_hidden // size
        t_part = t_width // size
        total = size * seq_len * s_width
        grad_scale = 2.0 / total
        v_up, v_down, q_proj = student_up[0], student_down[0], student_proj[0]

        own = student_in[0]
        side = lax.axis_index("model")
        last = n_layers - 1
        hidden = [teacher_in, teacher_in]

        def finish(c, delta):
            total = sum(part.astype(jnp.float32) for part in delta).astype(jnp.bfloat16)
            hidden[c] = (hidden[c].astype(jnp.float32) + total.astype(jnp.float32)).astype(jnp.bfloat16)
            target = dot(hidden[c], q_proj, ((1,), (0,))).astype(jnp.bfloat16)
            return target, lax.all_gather(target, AXES, axis=0, tiled=True)

        def columns(c):
            rows = hidden[c].shape[0]
            pieces = []
            for bits in range(size):
                piece = lax.dynamic_slice(hidden[c], (0, (me ^ bits) * t_part), (rows, t_part))
                pieces.append(flip(piece, bits, size) if bits else piece)
            return jnp.concatenate(pieces, axis=0)

        def normed(c, delta, layer):
            hidden[c], act = teacher_norm(hidden[c], delta, teacher_gain, layer, c)
            return act, lax.all_gather(act, "model", axis=0, tiled=True)

        def teach(act, layer, **window):
            return mlp(act, teacher_up_w, teacher_down, layer, **window)

        acts = [normed(c, (), 0)[1] for c in range(2)]
        for layer in range(n_layers):
            if layer == 0:
                all_in = lax.all_gather(after(own, acts[0]), AXES, axis=0, tiled=False)
            if layer == 1:
                all_out = lax.all_gather(after(own_out, acts[0]), AXES, axis=0, tiled=False)
            partial = teach(acts[0], layer)
            delta_0 = (lax.psum_scatter(partial, "model", scatter_dimension=0, tiled=True),)
            if layer == 0:
                partial = teach(acts[1], layer)
                delta_1 = (lax.psum_scatter(partial, "model", scatter_dimension=0, tiled=True),)
                act, acts[0] = normed(0, after(delta_0, partial), layer + 1)
                own_act = teacher_norm(after(own, act), (), student_gain, 0)[1]
                own_out = mlp(own_act, student_up, student_down, 0, own)
                delta_1 = after(delta_1, (own_out, all_in))
            else:
                rows = acts[1].shape[0] // 2
                partial = teach(acts[1], layer, rows=rows, where=1 - side)
                moved = flip(partial, 1, size)
                delta_0 = after(delta_0, partial)
                if layer < last:
                    ready, acts[0] = normed(0, delta_0, layer + 1)
                else:
                    ready, targets_0 = finish(0, delta_0)
                    feat_0 = columns(0)
                partial = teach(after(acts[1], ready), layer, rows=rows, where=side)
                delta_1 = (partial, moved)
            if layer < last:
                if layer == 1:
                    delta_1 = after(delta_1, all_out)
                acts[1] = normed(1, delta_1, layer + 1)[1]
        target_1, targets_1 = finish(1, delta_1)
        feat_1 = columns(1)

        all_in, all_out, targets_0 = after((all_in, all_out, targets_0), target_1)
        up_part = lax.dynamic_slice(v_up, (0, me * part), (s_width, part))
        down_part = lax.dynamic_slice(v_down, (me * part, 0), (part, s_width))
        proj_sum, square_0 = proj_part(me, feat_0, targets_0, all_out, 0, grad_scale, None, False)
        acts, pre, ups = zip(*[pre_of(all_in, student_gain, up_part, c) for c in range(2)])
        d_out_0, down_sum = down_part_of(ups[0], targets_0, all_out, 0, grad_scale, None, False)
        targets_1 = after(targets_1, (proj_sum, ups[1], down_sum))
        proj_piece, square_1 = proj_part(me, feat_1, targets_1, all_out, 1, grad_scale, proj_sum, True)
        proj_all = lax.all_gather(proj_piece, AXES, axis=0, tiled=True)
        loss = (jnp.sum(square_0) + jnp.sum(square_1)) / total
        d_out_1, down_piece = down_part_of(ups[1], after(targets_1, proj_piece), all_out, 1, grad_scale, down_sum, True)
        down_all = lax.all_gather(down_piece, AXES, axis=0, tiled=True)

        d_outs = after((d_out_0, d_out_1), down_piece)
        d_pres = [gelu_back(pre[c], dot(d_outs[c], down_part, ((1,), (1,)))).astype(jnp.bfloat16) for c in range(2)]

        def up_rows(first, count):
            cols = slice(first, first + count)
            return (dot(acts[0][:, cols], d_pres[0], ((0,), (0,))) + dot(acts[1][:, cols], d_pres[1], ((0,), (0,)))).astype(jnp.bfloat16)

        half = s_width // 2
        up_piece = up_rows(0, half)
        up_all_0 = lax.all_gather(up_piece, AXES, axis=0, tiled=False)
        up_piece = up_rows(half, half)
        up_all_1 = lax.all_gather(up_piece[: half // 2], AXES, axis=0, tiled=False)
        up_all_2 = lax.all_gather(up_piece[half // 2 :], AXES, axis=0, tiled=False)

        d_pres = after(d_pres, up_piece)
        gain_sum = jnp.zeros((s_width,), jnp.float32)
        seqs = all_in.reshape(size // 2, 2, seq_len, s_width)
        for c in range(2):
            d_act = dot(d_pres[c], up_part, ((1,), (1,))).reshape(size // 2, seq_len, s_width)
            gain_sum = gain_sum + jnp.sum(d_act * rms_unit(seqs[:, c].astype(jnp.float32)), axis=(0, 1))
        grad_gain = lax.psum(gain_sum, AXES)
        grad_proj = after(proj_all, gain_sum).astype(jnp.float32)
        grad_down = after(down_all, grad_gain).astype(jnp.float32)
        shape = (s_width, s_hidden)
        grad_up = spread(None, up_all_0, 0, shape)
        grad_up = spread(grad_up, up_all_1, half, shape)
        grad_up = spread(grad_up, up_all_2, half + half // 2, shape)
        return (loss, grad_up[None], grad_down[None], grad_gain[None], grad_proj[None])

    return jax.shard_map(
        step,
        mesh=mesh,
        in_specs=(
            P("data", "model", None),
            P(("data", "model"), None, None),
            P(),
            P(None, None, "model"),
            P(None, "model", None),
            P(),
            P(),
            P(),
            P(),
        ),
        out_specs=(P(), P(), P(), P(), P()),
        check_vma=False,
    )
```

```python
import functools

import jax
import jax.numpy as jnp
from jax import lax
from jax.experimental import pallas as pl
from jax.experimental.pallas import tpu as pltpu
from jax.sharding import PartitionSpec as P


EPS = 1e-6
VMEM_CAP = 64 * 1024 * 1024 - 65536
AXES = ("data", "model")


def after(values, dep):
    return lax.optimization_barrier((values, dep))[0]


def rms_unit(values):
    return values * lax.rsqrt(jnp.mean(values * values, axis=-1, keepdims=True) + EPS)


def mlp_kernel(layer, steps, wide, residual, where_ref, *refs):
    if residual:
        a_hbm, up_hbm, down_hbm, s_hbm, o_hbm, a_ref, up_ref, down_ref, first, second, act, acc, out, a_sem, up_sem, down_sem, o_sem, s_ref, s_sem = refs
    else:
        a_hbm, up_hbm, down_hbm, o_hbm, a_ref, up_ref, down_ref, first, second, act, acc, out, a_sem, up_sem, down_sem, o_sem = refs
    j = pl.program_id(0)
    rows, width = acc.shape
    tile = act.shape[2]
    half = tile // 2
    parts = 4
    size = rows // parts
    now = lax.rem(j, 2)

    def a_copy(r):
        source = pl.ds(pl.multiple_of(where_ref[0] * rows + r * size, size), size)
        return pltpu.make_async_copy(a_hbm.at[source], a_ref.at[pl.ds(r * size, size)], a_sem.at[r])

    def up_copy(k):
        return pltpu.make_async_copy(up_hbm.at[layer, :, pl.ds(pl.multiple_of(k * tile, tile), tile)], up_ref.at[lax.rem(k, 2)], up_sem.at[lax.rem(k, 2)])

    def down_copy(k):
        return pltpu.make_async_copy(down_hbm.at[layer, pl.ds(pl.multiple_of(k * tile, tile), tile)], down_ref.at[lax.rem(k, 2)], down_sem.at[lax.rem(k, 2)])

    def out_copy(k):
        cols = pl.ds(k * wide, wide)
        return pltpu.make_async_copy(out.at[:, cols], o_hbm.at[:, cols], o_sem.at[k])

    @pl.when(j == 0)
    def _():
        up_copy(0).start()
        for r in range(parts):
            a_copy(r).start()
        up_copy(1).start()
        down_copy(0).start()
        if residual:
            pltpu.make_async_copy(s_hbm, s_ref, s_sem.at[0]).start()
        up_copy(0).wait()
        for r in range(parts):
            part = slice(r * size, (r + 1) * size)
            a_copy(r).wait()
            first[part, :] = jnp.dot(a_ref[part, :], up_ref[0, :, :half], preferred_element_type=jnp.float32)
            second[part, :] = jnp.dot(a_ref[part, :], up_ref[0, :, half:], preferred_element_type=jnp.float32)
        act[0, :, :half] = jax.nn.gelu(first[...]).astype(jnp.bfloat16)

    @pl.when((j > 0) & (j < steps))
    def _():
        @pl.when(j + 1 < steps)
        def _():
            up_copy(j + 1).start()

        down_copy(j).start()
        up_copy(j).wait()
        act[1 - now, :, half:] = jax.nn.gelu(second[...]).astype(jnp.bfloat16)
        first[...] = jnp.dot(a_ref[...], up_ref[now, :, :half], preferred_element_type=jnp.float32)
        for r in range(parts):
            part = slice(r * size, (r + 1) * size)
            act[now, part, :half] = jax.nn.gelu(first[part, :]).astype(jnp.bfloat16)
            second[part, :] = jnp.dot(a_ref[part, :], up_ref[now, :, half:], preferred_element_type=jnp.float32)

    @pl.when(j == steps)
    def _():
        act[1 - now, :, half:] = jax.nn.gelu(second[...]).astype(jnp.bfloat16)

    def down(first_tile, last_tile):
        down_copy(j - 1).wait()
        if last_tile and residual:
            pltpu.make_async_copy(s_hbm, s_ref, s_sem.at[0]).wait()
        for k in range(width // wide):
            cols = slice(k * wide, (k + 1) * wide)
            total = jnp.dot(act[1 - now], down_ref[1 - now, :, cols], preferred_element_type=jnp.float32)
            if not first_tile:
                total = acc[:, cols] + total
            if not last_tile:
                acc[:, cols] = total
            else:
                if residual:
                    total = s_ref[:, cols].astype(jnp.float32) + total
                out[:, cols] = total.astype(jnp.bfloat16)
                out_copy(k).start()
        if last_tile:
            for k in range(width // wide):
                out_copy(k).wait()

    @pl.when(j == 1)
    def _():
        down(True, False)

    @pl.when((j > 1) & (j < steps))
    def _():
        down(False, False)

    @pl.when(j == steps)
    def _():
        down(False, True)


def mlp(a, up, down, layer, state=None, rows=None, where=None, tile=512, wide=512):
    depth = a.shape[1]
    rows = rows or a.shape[0]
    where = jnp.zeros((1,), jnp.int32) if where is None else where.astype(jnp.int32).reshape(1)
    hidden = up.shape[2]
    width = down.shape[2]
    steps = hidden // tile
    hbm = pl.BlockSpec(memory_space=pl.ANY)
    scratch = [
        pltpu.VMEM((rows, depth), jnp.bfloat16),
        pltpu.VMEM((2, depth, tile), jnp.bfloat16),
        pltpu.VMEM((2, tile, width), jnp.bfloat16),
        pltpu.VMEM((rows, tile // 2), jnp.float32),
        pltpu.VMEM((rows, tile // 2), jnp.float32),
        pltpu.VMEM((2, rows, tile), jnp.bfloat16),
        pltpu.VMEM((rows, width), jnp.float32),
        pltpu.VMEM((rows, width), jnp.bfloat16),
        pltpu.SemaphoreType.DMA((4,)),
        pltpu.SemaphoreType.DMA((2,)),
        pltpu.SemaphoreType.DMA((2,)),
        pltpu.SemaphoreType.DMA((width // wide,)),
    ]
    args = [a, up, down]
    if state is not None:
        args.append(state)
        scratch += [pltpu.VMEM((rows, width), jnp.bfloat16), pltpu.SemaphoreType.DMA((1,))]
    return pl.pallas_call(
        functools.partial(mlp_kernel, layer, steps, wide, state is not None),
        grid_spec=pltpu.PrefetchScalarGridSpec(
            num_scalar_prefetch=1,
            grid=(steps + 1,),
            in_specs=[hbm] * len(args),
            out_specs=hbm,
            scratch_shapes=scratch,
        ),
        out_shape=jax.ShapeDtypeStruct((rows, width), jnp.bfloat16),
        compiler_params=pltpu.CompilerParams(vmem_limit_bytes=VMEM_CAP),
        cost_estimate=pl.CostEstimate(
            flops=2 * rows * hidden * (depth + width),
            bytes_accessed=2 * (rows * (depth + width) + hidden * (depth + width)),
            transcendentals=rows * hidden,
        ),
        name="mlp",
    )(where, *args)


def norm_kernel(h_ref, g_ref, a_ref):
    state = h_ref[...].astype(jnp.float32)
    inv = lax.rsqrt(jnp.mean(state * state, axis=-1, keepdims=True) + EPS)
    a_ref[...] = (state * inv * g_ref[...]).astype(jnp.bfloat16)


def step_kernel(h_ref, *refs):
    *parts, g_ref, o_ref, a_ref = refs
    delta = parts[0][...].astype(jnp.float32)
    if len(parts) > 1:
        delta = (delta + parts[1][...].astype(jnp.float32)).astype(jnp.bfloat16).astype(jnp.float32)
    state = (h_ref[...].astype(jnp.float32) + delta).astype(jnp.bfloat16)
    o_ref[...] = state
    state = state.astype(jnp.float32)
    inv = lax.rsqrt(jnp.mean(state * state, axis=-1, keepdims=True) + EPS)
    a_ref[...] = (state * inv * g_ref[...]).astype(jnp.bfloat16)


def teacher_norm(hidden, delta, gains, layer, which=0, block=128):
    rows, width = hidden.shape[-2:]
    spec = pl.BlockSpec((block, width), lambda i: (i, 0))
    source = spec if hidden.ndim == 2 else pl.BlockSpec((None, block, width), lambda i: (which, i, 0))
    gain_spec = pl.BlockSpec((1, width), lambda i: (0, 0))
    shape = jax.ShapeDtypeStruct((rows, width), jnp.bfloat16)
    count = rows * width
    common = dict(
        grid=(rows // block,),
        compiler_params=pltpu.CompilerParams(vmem_limit_bytes=VMEM_CAP),
    )
    gain = gains[layer : layer + 1]
    if not delta:
        cost = pl.CostEstimate(flops=8 * count, bytes_accessed=4 * count, transcendentals=0)
        return hidden, pl.pallas_call(norm_kernel, in_specs=[source, gain_spec], out_specs=spec, out_shape=shape, cost_estimate=cost, name="norm", **common)(hidden, gain)
    cost = pl.CostEstimate(flops=10 * count, bytes_accessed=8 * count, transcendentals=0)
    return pl.pallas_call(step_kernel, in_specs=[source] + [spec] * len(delta) + [gain_spec], out_specs=[spec, spec], out_shape=[shape, shape], cost_estimate=cost, name="step", **common)(hidden, *delta, gain)


def pre_kernel(sub, me_ref, s_ref, g_ref, w_ref, a_ref, p_ref, u_ref):
    for r in range(s_ref.shape[0] // sub):
        part = slice(r * sub, (r + 1) * sub)
        state = s_ref[part, :].astype(jnp.float32)
        inv = lax.rsqrt(jnp.mean(state * state, axis=-1, keepdims=True) + EPS)
        a_ref[part, :] = (state * inv * g_ref[...]).astype(jnp.bfloat16)
    for r in range(s_ref.shape[0] // sub):
        part = slice(r * sub, (r + 1) * sub)
        pre = jnp.dot(a_ref[part, :], w_ref[...], preferred_element_type=jnp.float32)
        p_ref[part, :] = pre
        u_ref[part, :] = jax.nn.gelu(pre).astype(jnp.bfloat16)


def pre_of(me, states, gain, weights, parity, cols, block=512, sub=256):
    n_seq, seq_len, width = states.shape
    half = n_seq // 2
    rows = half * seq_len
    steps = seq_len // block
    out = lambda w: pl.BlockSpec((block, w), lambda i, j, me: (i * steps + j, 0))
    return pl.pallas_call(
        functools.partial(pre_kernel, sub),
        grid_spec=pltpu.PrefetchScalarGridSpec(
            num_scalar_prefetch=1,
            grid=(half, steps),
            in_specs=[
                pl.BlockSpec((None, block, width), lambda i, j, me: (2 * i + parity, j, 0)),
                pl.BlockSpec((1, width), lambda i, j, me: (0, 0)),
                pl.BlockSpec((None, width, cols), lambda i, j, me: (0, 0, me[0])),
            ],
            out_specs=[out(width), out(cols), out(cols)],
        ),
        out_shape=[
            jax.ShapeDtypeStruct((rows, width), jnp.bfloat16),
            jax.ShapeDtypeStruct((rows, cols), jnp.float32),
            jax.ShapeDtypeStruct((rows, cols), jnp.bfloat16),
        ],
        compiler_params=pltpu.CompilerParams(vmem_limit_bytes=VMEM_CAP),
        cost_estimate=pl.CostEstimate(flops=2 * rows * width * cols, bytes_accessed=rows * (4 * width + 6 * cols), transcendentals=rows * cols),
        name="pre",
    )(me.reshape(1), states, gain, weights)


def errors_at(z_ref, s_ref, part):
    state = s_ref[part, :].astype(jnp.float32)
    inv = lax.rsqrt(jnp.mean(state * state, axis=-1, keepdims=True) + EPS)
    unit = state * inv
    return z_ref[part, :].astype(jnp.float32) - unit, unit, inv


def finish_kernel(count, me_ref, h_ref, *refs):
    parts = refs[:count]
    q_ref, f_ref, z_ref, acc = refs[count:]
    k = pl.program_id(0)
    delta = parts[0][...].astype(jnp.float32)
    if count > 1:
        delta = (delta + parts[1][...].astype(jnp.float32)).astype(jnp.bfloat16).astype(jnp.float32)
    feat = (h_ref[...].astype(jnp.float32) + delta).astype(jnp.bfloat16)
    f_ref[...] = feat
    term = jnp.dot(feat, q_ref[...], preferred_element_type=jnp.float32)

    @pl.when(k == 0)
    def _():
        acc[...] = term

    @pl.when((k > 0) & (k < pl.num_programs(0) - 1))
    def _():
        acc[...] += term

    @pl.when(k == pl.num_programs(0) - 1)
    def _():
        z_ref[...] = (acc[...] + term).astype(jnp.bfloat16)


def finish_part(me, hidden, delta, proj, size):
    rows, width = hidden.shape
    cols = width // size
    out = proj.shape[2]
    spec = pl.BlockSpec((rows, cols), lambda k, me: (0, k))
    return pl.pallas_call(
        functools.partial(finish_kernel, len(delta)),
        grid_spec=pltpu.PrefetchScalarGridSpec(
            num_scalar_prefetch=1,
            grid=(size,),
            in_specs=[spec] * (1 + len(delta)) + [pl.BlockSpec((None, cols, out), lambda k, me: (0, k, 0))],
            out_specs=[
                pl.BlockSpec((None, rows, cols), lambda k, me: (me[0] ^ k, 0, 0)),
                pl.BlockSpec((rows, out), lambda k, me: (0, 0)),
            ],
            scratch_shapes=[pltpu.VMEM((rows, out), jnp.float32)],
        ),
        out_shape=[
            jax.ShapeDtypeStruct((size, rows, cols), jnp.bfloat16),
            jax.ShapeDtypeStruct((rows, out), jnp.bfloat16),
        ],
        compiler_params=pltpu.CompilerParams(vmem_limit_bytes=VMEM_CAP),
        cost_estimate=pl.CostEstimate(flops=2 * rows * width * out, bytes_accessed=2 * width * (4 * rows + out), transcendentals=0),
        name="finish",
    )(me.reshape(1), hidden, *delta, proj)


def proj_kernel(scale, first, last, count, chunk, me_ref, *refs):
    pieces = refs[:count]
    z_ref, s_ref = refs[count : count + 2]
    out_ref, sq_ref, total, feat, error_buf = refs[-5:]
    k = pl.program_id(0)
    rows, width = z_ref.shape

    @pl.when(k == 0)
    def _():
        sq_ref[...] = jnp.zeros_like(sq_ref)
        if first:
            total[...] = jnp.zeros_like(total)
        else:
            total[...] = refs[count + 2][...]

    for i in range(count):

        @pl.when(k == i)
        def _():
            feat[...] = pieces[i][...]

    for r in range(rows // chunk):
        part = slice(r * chunk, (r + 1) * chunk)
        error = errors_at(z_ref, s_ref, part)[0]
        error_buf[part, :] = error.astype(jnp.bfloat16)
        sq_ref[...] += jnp.sum((error * error).reshape(chunk // 8, 8, width), axis=0)
    total[...] += lax.dot_general(feat[...], error_buf[...], (((0,), (0,)), ((), ())), preferred_element_type=jnp.float32)

    @pl.when(k == pl.num_programs(0) - 1)
    def _():
        out_ref[...] = (scale * total[...]).astype(jnp.bfloat16) if last else total[...]


def proj_part(me, pieces, targets, states, parity, scale, total, last, chunk=16):
    n_seq, _, width = states.shape
    size = n_seq
    rows, cols = pieces[0].shape
    whole = pl.BlockSpec((cols, width), lambda k, me: (0, 0))
    in_specs = [pl.BlockSpec((rows, cols), lambda k, me: (0, 0))] * size + [
        pl.BlockSpec((rows, width), lambda k, me: (me[0] ^ k, 0)),
        pl.BlockSpec((None, rows, width), lambda k, me: (2 * ((me[0] ^ k) // 2) + parity, (me[0] ^ k) % 2, 0)),
    ]
    args = [me.reshape(1), *pieces, targets, states]
    if total is not None:
        in_specs.append(whole)
        args.append(total)
    return pl.pallas_call(
        functools.partial(proj_kernel, scale, total is None, last, size, chunk),
        grid_spec=pltpu.PrefetchScalarGridSpec(
            num_scalar_prefetch=1,
            grid=(size,),
            in_specs=in_specs,
            out_specs=[whole, pl.BlockSpec((8, width), lambda k, me: (0, 0))],
            scratch_shapes=[
                pltpu.VMEM((cols, width), jnp.float32),
                pltpu.VMEM((rows, cols), jnp.bfloat16),
                pltpu.VMEM((rows, width), jnp.bfloat16),
            ],
        ),
        out_shape=[
            jax.ShapeDtypeStruct((cols, width), jnp.bfloat16 if last else jnp.float32),
            jax.ShapeDtypeStruct((8, width), jnp.float32),
        ],
        compiler_params=pltpu.CompilerParams(vmem_limit_bytes=VMEM_CAP),
        cost_estimate=pl.CostEstimate(flops=2 * size * rows * cols * width, bytes_accessed=size * rows * (4 * width + 2 * cols), transcendentals=0),
        name="proj",
    )(*args)


def down_kernel(scale, first, chunk, cuts, z_ref, s_ref, u_ref, *refs):
    d_ref, out_ref, total, z_scale, s_scale = refs[-5:]
    k = pl.program_id(0) * pl.num_programs(1) + pl.program_id(1)

    @pl.when(k == 0)
    def _():
        total[...] = jnp.zeros_like(total) if first else refs[0][...]

    width = z_ref.shape[1]
    for r in range(z_ref.shape[0] // chunk):
        part = slice(r * chunk, (r + 1) * chunk)
        state = s_ref[part, :].astype(jnp.float32)
        square = jnp.sum(state * state, axis=-1, keepdims=True) / width
        cross = jnp.sum(state * z_ref[part, :].astype(jnp.float32), axis=-1, keepdims=True) / width
        inv = lax.rsqrt(square + EPS)
        lean = inv * cross - inv * inv * square
        z_scale[part, :] = jnp.broadcast_to(-scale * inv, (chunk, 128))
        s_scale[part, :] = jnp.broadcast_to(scale * inv * inv * (1.0 + lean), (chunk, 128))
    for r in range(z_ref.shape[0] // chunk):
        part = slice(r * chunk, (r + 1) * chunk)
        d_ref[part, :] = (s_ref[part, :].astype(jnp.float32) * s_scale[part, :1] + z_ref[part, :].astype(jnp.float32) * z_scale[part, :1]).astype(jnp.bfloat16)
    cols = total.shape[0]
    for h in range(cuts):
        part = slice(h * cols // cuts, (h + 1) * cols // cuts)
        total[part, :] += lax.dot_general(u_ref[:, part], d_ref[...], (((0,), (0,)), ((), ())), preferred_element_type=jnp.float32)

    @pl.when(k == pl.num_programs(0) * pl.num_programs(1) - 1)
    def _():
        out_ref[...] = total[...].astype(out_ref.dtype)


def down_part_of(ups, targets, states, parity, scale, total, last, block=512, chunk=16, cuts=1):
    n_seq, seq_len, width = states.shape
    half = n_seq // 2
    cols = ups.shape[1]
    rows = half * seq_len
    steps = seq_len // block
    spec = lambda w: pl.BlockSpec((block, w), lambda i, j: (i * steps + j, 0))
    whole = pl.BlockSpec((cols, width), lambda i, j: (0, 0), pipeline_mode=pl.Buffered(1))
    in_specs = [spec(width), pl.BlockSpec((None, block, width), lambda i, j: (2 * i + parity, j, 0)), spec(cols)]
    args = [targets, states, ups]
    if total is not None:
        in_specs.append(whole)
        args.append(total)
    return pl.pallas_call(
        functools.partial(down_kernel, scale, total is None, chunk, cuts),
        grid=(half, steps),
        in_specs=in_specs,
        out_specs=[spec(width), whole],
        out_shape=[
            jax.ShapeDtypeStruct((rows, width), jnp.bfloat16),
            jax.ShapeDtypeStruct((cols, width), jnp.bfloat16 if last else jnp.float32),
        ],
        scratch_shapes=[pltpu.VMEM((cols, width), jnp.float32), pltpu.VMEM((block, 128), jnp.float32), pltpu.VMEM((block, 128), jnp.float32)],
        compiler_params=pltpu.CompilerParams(vmem_limit_bytes=VMEM_CAP),
        cost_estimate=pl.CostEstimate(flops=2 * rows * width * cols, bytes_accessed=rows * (6 * width + 2 * cols), transcendentals=0),
        name="down",
    )(*args)


def spread_kernel(piece_ref, *rest):
    rest[-1][...] = piece_ref[...].astype(jnp.float32)


def spread(out, pieces, first_row, shape, block=512):
    count, rows, cols = pieces.shape
    specs = [pl.BlockSpec((None, block, cols), lambda k, i: (k, i, 0))]
    args = [pieces]
    alias = {}
    if out is not None:
        specs.append(pl.BlockSpec(memory_space=pl.ANY))
        args.append(out)
        alias = {1: 0}
    return pl.pallas_call(
        spread_kernel,
        grid=(count, rows // block),
        in_specs=specs,
        out_specs=pl.BlockSpec((block, cols), lambda k, i: (first_row // block + i, k)),
        out_shape=jax.ShapeDtypeStruct(shape, jnp.float32),
        input_output_aliases=alias,
        compiler_params=pltpu.CompilerParams(vmem_limit_bytes=VMEM_CAP),
        cost_estimate=pl.CostEstimate(flops=count * rows * cols, bytes_accessed=6 * count * rows * cols, transcendentals=0),
        name="spread",
    )(*args)


def flip(value, bits, size):
    return lax.ppermute(value, AXES, [(i, i ^ bits) for i in range(size)])


def gelu_back(pre_act, grad_out):
    return jax.vjp(jax.nn.gelu, pre_act)[1](grad_out)[0]


def dot(a, b, dims):
    return lax.dot_general(a, b, (dims, ((), ())), preferred_element_type=jnp.float32)


def solution(mesh):
    size = mesh.shape["data"] * mesh.shape["model"]

    def step(teacher_in, student_in, teacher_gain, teacher_up_w, teacher_down, student_gain, student_up, student_down, student_proj):
        me = lax.axis_index("data") * 2 + lax.axis_index("model")
        n_layers = teacher_up_w.shape[0]
        _, seq_len, s_width = student_in.shape
        s_hidden = student_up.shape[2]
        part = s_hidden // size
        total = size * seq_len * s_width
        grad_scale = 2.0 / total
        v_up, v_down = student_up[0], student_down[0]

        own = student_in[0]
        side = lax.axis_index("model")
        last = n_layers - 1
        hidden = [teacher_in, teacher_in]

        def finish(c, delta):
            feats, target = finish_part(me, hidden[c], delta, student_proj, size)
            targets = lax.all_gather(target, AXES, axis=0, tiled=True)
            pieces = [flip(feats[bits], bits, size) if bits else feats[0] for bits in range(size)]
            return target, targets, pieces

        def normed(c, delta, layer):
            hidden[c], act = teacher_norm(hidden[c], delta, teacher_gain, layer, c)
            return act, lax.all_gather(act, "model", axis=0, tiled=True)

        def teach(act, layer, **window):
            return mlp(act, teacher_up_w, teacher_down, layer, **window)

        acts = [normed(c, (), 0)[1] for c in range(2)]
        for layer in range(n_layers):
            if layer == 0:
                all_in = lax.all_gather(after(own, acts[0]), AXES, axis=0, tiled=False)
            if layer == 1:
                all_out = lax.all_gather(after(own_out, acts[0]), AXES, axis=0, tiled=False)
            partial = teach(acts[0], layer)
            delta_0 = (lax.psum_scatter(partial, "model", scatter_dimension=0, tiled=True),)
            if layer == 0:
                partial = teach(acts[1], layer)
                delta_1 = (lax.psum_scatter(partial, "model", scatter_dimension=0, tiled=True),)
                act, acts[0] = normed(0, after(delta_0, partial), layer + 1)
                own_act = teacher_norm(after(own, act), (), student_gain, 0)[1]
                own_out = mlp(own_act, student_up, student_down, 0, own)
                delta_1 = after(delta_1, (own_out, all_in))
            else:
                rows = acts[1].shape[0] // 2
                partial = teach(acts[1], layer, rows=rows, where=1 - side)
                moved = flip(partial, 1, size)
                delta_0 = after(delta_0, partial)
                if layer < last:
                    ready, acts[0] = normed(0, delta_0, layer + 1)
                else:
                    ready, targets_0, feat_0 = finish(0, delta_0)
                partial = teach(after(acts[1], ready), layer, rows=rows, where=side)
                delta_1 = (partial, moved)
            if layer < last:
                if layer == 1:
                    delta_1 = after(delta_1, all_out)
                acts[1] = normed(1, delta_1, layer + 1)[1]
        target_1, targets_1, feat_1 = finish(1, delta_1)

        all_in, all_out, targets_0 = after((all_in, all_out, targets_0), target_1)
        proj_sum, square_0 = proj_part(me, feat_0, targets_0, all_out, 0, grad_scale, None, False)
        acts, pre, ups = zip(*[pre_of(me, all_in, student_gain, student_up, c, part) for c in range(2)])
        d_out_0, down_sum = down_part_of(ups[0], after(targets_0, (proj_sum, ups[1])), all_out, 0, grad_scale, None, False)
        targets_1 = after(targets_1, down_sum)
        proj_piece, square_1 = proj_part(me, feat_1, targets_1, all_out, 1, grad_scale, proj_sum, True)
        proj_all = lax.all_gather(proj_piece, AXES, axis=0, tiled=True)
        loss = (jnp.sum(square_0) + jnp.sum(square_1)) / total
        d_out_1, down_piece = down_part_of(ups[1], after(targets_1, proj_piece), all_out, 1, grad_scale, down_sum, True)
        down_all = lax.all_gather(down_piece, AXES, axis=0, tiled=True)

        d_outs = after((d_out_0, d_out_1), down_piece)
        up_part = lax.dynamic_slice(after(v_up, proj_piece), (0, me * part), (s_width, part))
        down_part = lax.dynamic_slice(after(v_down, proj_piece), (me * part, 0), (part, s_width))
        d_pres = [gelu_back(pre[c], dot(d_outs[c], down_part, ((1,), (1,)))).astype(jnp.bfloat16) for c in range(2)]

        def up_rows(first, count):
            cols = slice(first, first + count)
            return (dot(acts[0][:, cols], d_pres[0], ((0,), (0,))) + dot(acts[1][:, cols], d_pres[1], ((0,), (0,)))).astype(jnp.bfloat16)

        most = s_width * 3 // 4
        up_piece_0 = up_rows(0, most)
        up_all_0 = lax.all_gather(up_piece_0, AXES, axis=0, tiled=False)
        up_piece = up_rows(most, s_width - most)
        up_all_1 = lax.all_gather(up_piece, AXES, axis=0, tiled=False)

        d_pres = after(d_pres, up_piece)
        gain_sum = jnp.zeros((s_width,), jnp.float32)
        seqs = all_in.reshape(size // 2, 2, seq_len, s_width)
        for c in range(2):
            d_act = dot(d_pres[c], up_part, ((1,), (1,))).reshape(size // 2, seq_len, s_width)
            gain_sum = gain_sum + jnp.sum(d_act * rms_unit(seqs[:, c].astype(jnp.float32)), axis=(0, 1))
        grad_gain = lax.psum(gain_sum, AXES)
        grad_proj = after(proj_all, gain_sum).astype(jnp.float32)
        grad_down = after(down_all, grad_gain).astype(jnp.float32)
        shape = (s_width, s_hidden)
        grad_up = spread(None, up_all_0, 0, shape)
        grad_up = spread(grad_up, up_all_1, most, shape)
        return (loss, grad_up[None], grad_down[None], grad_gain[None], grad_proj[None])

    return jax.shard_map(
        step,
        mesh=mesh,
        in_specs=(
            P("data", "model", None),
            P(("data", "model"), None, None),
            P(),
            P(None, None, "model"),
            P(None, "model", None),
            P(),
            P(),
            P(),
            P(),
        ),
        out_specs=(P(), P(), P(), P(), P()),
        check_vma=False,
    )
```

```python
import functools

import jax
import jax.numpy as jnp
from jax import lax
from jax.experimental import pallas as pl
from jax.experimental.pallas import tpu as pltpu
from jax.sharding import PartitionSpec as P


EPS = 1e-6
VMEM_CAP = 64 * 1024 * 1024 - 65536
AXES = ("data", "model")


def after(values, dep):
    return lax.optimization_barrier((values, dep))[0]


def mlp_kernel(layer, steps, wide, residual, where_ref, *refs):
    if residual:
        a_hbm, up_hbm, down_hbm, s_hbm, o_hbm, a_ref, up_ref, down_ref, first, second, act, acc, out, a_sem, up_sem, down_sem, o_sem, s_ref, s_sem = refs
    else:
        a_hbm, up_hbm, down_hbm, o_hbm, a_ref, up_ref, down_ref, first, second, act, acc, out, a_sem, up_sem, down_sem, o_sem = refs
    j = pl.program_id(0)
    rows, width = acc.shape
    tile = act.shape[2]
    half = tile // 2
    parts = 4
    size = rows // parts
    now = lax.rem(j, 2)

    def a_copy(r):
        source = pl.ds(pl.multiple_of(where_ref[0] * rows + r * size, size), size)
        return pltpu.make_async_copy(a_hbm.at[source], a_ref.at[pl.ds(r * size, size)], a_sem.at[r])

    def up_copy(k):
        return pltpu.make_async_copy(up_hbm.at[layer, :, pl.ds(pl.multiple_of(k * tile, tile), tile)], up_ref.at[lax.rem(k, 2)], up_sem.at[lax.rem(k, 2)])

    def down_copy(k):
        return pltpu.make_async_copy(down_hbm.at[layer, pl.ds(pl.multiple_of(k * tile, tile), tile)], down_ref.at[lax.rem(k, 2)], down_sem.at[lax.rem(k, 2)])

    def out_copy(k):
        cols = pl.ds(k * wide, wide)
        return pltpu.make_async_copy(out.at[:, cols], o_hbm.at[:, cols], o_sem.at[k])

    @pl.when(j == 0)
    def _():
        up_copy(0).start()
        for r in range(parts):
            a_copy(r).start()
        up_copy(1).start()
        down_copy(0).start()
        if residual:
            pltpu.make_async_copy(s_hbm, s_ref, s_sem.at[0]).start()
        up_copy(0).wait()
        for r in range(parts):
            part = slice(r * size, (r + 1) * size)
            a_copy(r).wait()
            first[part, :] = jnp.dot(a_ref[part, :], up_ref[0, :, :half], preferred_element_type=jnp.float32)
            second[part, :] = jnp.dot(a_ref[part, :], up_ref[0, :, half:], preferred_element_type=jnp.float32)
        act[0, :, :half] = jax.nn.gelu(first[...]).astype(jnp.bfloat16)

    @pl.when((j > 0) & (j < steps))
    def _():
        @pl.when(j + 1 < steps)
        def _():
            up_copy(j + 1).start()

        down_copy(j).start()
        up_copy(j).wait()
        act[1 - now, :, half:] = jax.nn.gelu(second[...]).astype(jnp.bfloat16)
        first[...] = jnp.dot(a_ref[...], up_ref[now, :, :half], preferred_element_type=jnp.float32)
        for r in range(parts):
            part = slice(r * size, (r + 1) * size)
            act[now, part, :half] = jax.nn.gelu(first[part, :]).astype(jnp.bfloat16)
            second[part, :] = jnp.dot(a_ref[part, :], up_ref[now, :, half:], preferred_element_type=jnp.float32)

    @pl.when(j == steps)
    def _():
        act[1 - now, :, half:] = jax.nn.gelu(second[...]).astype(jnp.bfloat16)

    def down(first_tile, last_tile):
        down_copy(j - 1).wait()
        if last_tile and residual:
            pltpu.make_async_copy(s_hbm, s_ref, s_sem.at[0]).wait()
        for k in range(width // wide):
            cols = slice(k * wide, (k + 1) * wide)
            total = jnp.dot(act[1 - now], down_ref[1 - now, :, cols], preferred_element_type=jnp.float32)
            if not first_tile:
                total = acc[:, cols] + total
            if not last_tile:
                acc[:, cols] = total
            else:
                if residual:
                    total = s_ref[:, cols].astype(jnp.float32) + total
                out[:, cols] = total.astype(jnp.bfloat16)
                out_copy(k).start()
        if last_tile:
            for k in range(width // wide):
                out_copy(k).wait()

    @pl.when(j == 1)
    def _():
        down(True, False)

    @pl.when((j > 1) & (j < steps))
    def _():
        down(False, False)

    @pl.when(j == steps)
    def _():
        down(False, True)


def mlp(a, up, down, layer, state=None, rows=None, where=None, tile=512, wide=512):
    depth = a.shape[1]
    rows = rows or a.shape[0]
    where = jnp.zeros((1,), jnp.int32) if where is None else where.astype(jnp.int32).reshape(1)
    hidden = up.shape[2]
    width = down.shape[2]
    steps = hidden // tile
    hbm = pl.BlockSpec(memory_space=pl.ANY)
    scratch = [
        pltpu.VMEM((rows, depth), jnp.bfloat16),
        pltpu.VMEM((2, depth, tile), jnp.bfloat16),
        pltpu.VMEM((2, tile, width), jnp.bfloat16),
        pltpu.VMEM((rows, tile // 2), jnp.float32),
        pltpu.VMEM((rows, tile // 2), jnp.float32),
        pltpu.VMEM((2, rows, tile), jnp.bfloat16),
        pltpu.VMEM((rows, width), jnp.float32),
        pltpu.VMEM((rows, width), jnp.bfloat16),
        pltpu.SemaphoreType.DMA((4,)),
        pltpu.SemaphoreType.DMA((2,)),
        pltpu.SemaphoreType.DMA((2,)),
        pltpu.SemaphoreType.DMA((width // wide,)),
    ]
    args = [a, up, down]
    if state is not None:
        args.append(state)
        scratch += [pltpu.VMEM((rows, width), jnp.bfloat16), pltpu.SemaphoreType.DMA((1,))]
    return pl.pallas_call(
        functools.partial(mlp_kernel, layer, steps, wide, state is not None),
        grid_spec=pltpu.PrefetchScalarGridSpec(
            num_scalar_prefetch=1,
            grid=(steps + 1,),
            in_specs=[hbm] * len(args),
            out_specs=hbm,
            scratch_shapes=scratch,
        ),
        out_shape=jax.ShapeDtypeStruct((rows, width), jnp.bfloat16),
        compiler_params=pltpu.CompilerParams(vmem_limit_bytes=VMEM_CAP),
        cost_estimate=pl.CostEstimate(
            flops=2 * rows * hidden * (depth + width),
            bytes_accessed=2 * (rows * (depth + width) + hidden * (depth + width)),
            transcendentals=rows * hidden,
        ),
        name="mlp",
    )(where, *args)


def norm_kernel(h_ref, g_ref, a_ref):
    state = h_ref[...].astype(jnp.float32)
    inv = lax.rsqrt(jnp.mean(state * state, axis=-1, keepdims=True) + EPS)
    a_ref[...] = (state * inv * g_ref[...]).astype(jnp.bfloat16)


def step_kernel(h_ref, *refs):
    *parts, g_ref, o_ref, a_ref = refs
    delta = parts[0][...].astype(jnp.float32)
    if len(parts) > 1:
        delta = (delta + parts[1][...].astype(jnp.float32)).astype(jnp.bfloat16).astype(jnp.float32)
    state = (h_ref[...].astype(jnp.float32) + delta).astype(jnp.bfloat16)
    o_ref[...] = state
    state = state.astype(jnp.float32)
    inv = lax.rsqrt(jnp.mean(state * state, axis=-1, keepdims=True) + EPS)
    a_ref[...] = (state * inv * g_ref[...]).astype(jnp.bfloat16)


def teacher_norm(hidden, delta, gains, layer, which=0, block=128):
    rows, width = hidden.shape[-2:]
    spec = pl.BlockSpec((block, width), lambda i: (i, 0))
    source = spec if hidden.ndim == 2 else pl.BlockSpec((None, block, width), lambda i: (which, i, 0))
    gain_spec = pl.BlockSpec((1, width), lambda i: (0, 0))
    shape = jax.ShapeDtypeStruct((rows, width), jnp.bfloat16)
    count = rows * width
    common = dict(
        grid=(rows // block,),
        compiler_params=pltpu.CompilerParams(vmem_limit_bytes=VMEM_CAP),
    )
    gain = gains[layer : layer + 1]
    if not delta:
        cost = pl.CostEstimate(flops=8 * count, bytes_accessed=4 * count, transcendentals=0)
        return hidden, pl.pallas_call(norm_kernel, in_specs=[source, gain_spec], out_specs=spec, out_shape=shape, cost_estimate=cost, name="norm", **common)(hidden, gain)
    cost = pl.CostEstimate(flops=10 * count, bytes_accessed=8 * count, transcendentals=0)
    return pl.pallas_call(step_kernel, in_specs=[source] + [spec] * len(delta) + [gain_spec], out_specs=[spec, spec], out_shape=[shape, shape], cost_estimate=cost, name="step", **common)(hidden, *delta, gain)


def pre_kernel(sub, me_ref, s_ref, g_ref, w_ref, a_ref, p_ref, u_ref):
    for r in range(s_ref.shape[0] // sub):
        part = slice(r * sub, (r + 1) * sub)
        state = s_ref[part, :].astype(jnp.float32)
        inv = lax.rsqrt(jnp.mean(state * state, axis=-1, keepdims=True) + EPS)
        a_ref[part, :] = (state * inv * g_ref[...]).astype(jnp.bfloat16)
    for r in range(s_ref.shape[0] // sub):
        part = slice(r * sub, (r + 1) * sub)
        pre = jnp.dot(a_ref[part, :], w_ref[...], preferred_element_type=jnp.float32)
        p_ref[part, :] = pre
        u_ref[part, :] = jax.nn.gelu(pre).astype(jnp.bfloat16)


def pre_of(me, states, gain, weights, parity, cols, block=512, sub=256):
    n_seq, seq_len, width = states.shape
    half = n_seq // 2
    rows = half * seq_len
    steps = seq_len // block
    out = lambda w: pl.BlockSpec((block, w), lambda i, j, me: (i * steps + j, 0))
    return pl.pallas_call(
        functools.partial(pre_kernel, sub),
        grid_spec=pltpu.PrefetchScalarGridSpec(
            num_scalar_prefetch=1,
            grid=(half, steps),
            in_specs=[
                pl.BlockSpec((None, block, width), lambda i, j, me: (2 * i + parity, j, 0)),
                pl.BlockSpec((1, width), lambda i, j, me: (0, 0)),
                pl.BlockSpec((None, width, cols), lambda i, j, me: (0, 0, me[0])),
            ],
            out_specs=[out(width), out(cols), out(cols)],
        ),
        out_shape=[
            jax.ShapeDtypeStruct((rows, width), jnp.bfloat16),
            jax.ShapeDtypeStruct((rows, cols), jnp.float32),
            jax.ShapeDtypeStruct((rows, cols), jnp.bfloat16),
        ],
        compiler_params=pltpu.CompilerParams(vmem_limit_bytes=VMEM_CAP),
        cost_estimate=pl.CostEstimate(flops=2 * rows * width * cols, bytes_accessed=rows * (4 * width + 6 * cols), transcendentals=rows * cols),
        name="pre",
    )(me.reshape(1), states, gain, weights)


def errors_at(z_ref, s_ref, part):
    state = s_ref[part, :].astype(jnp.float32)
    inv = lax.rsqrt(jnp.mean(state * state, axis=-1, keepdims=True) + EPS)
    unit = state * inv
    return z_ref[part, :].astype(jnp.float32) - unit, unit, inv


def finish_kernel(count, me_ref, h_ref, *refs):
    parts = refs[:count]
    q_ref, f_ref, z_ref, acc = refs[count:]
    k = pl.program_id(0)
    delta = parts[0][...].astype(jnp.float32)
    if count > 1:
        delta = (delta + parts[1][...].astype(jnp.float32)).astype(jnp.bfloat16).astype(jnp.float32)
    feat = (h_ref[...].astype(jnp.float32) + delta).astype(jnp.bfloat16)
    f_ref[...] = feat
    term = jnp.dot(feat, q_ref[...], preferred_element_type=jnp.float32)

    @pl.when(k == 0)
    def _():
        acc[...] = term

    @pl.when((k > 0) & (k < pl.num_programs(0) - 1))
    def _():
        acc[...] += term

    @pl.when(k == pl.num_programs(0) - 1)
    def _():
        z_ref[...] = (acc[...] + term).astype(jnp.bfloat16)


def finish_part(me, hidden, delta, proj, size):
    rows, width = hidden.shape
    cols = width // size
    out = proj.shape[2]
    spec = pl.BlockSpec((rows, cols), lambda k, me: (0, k))
    return pl.pallas_call(
        functools.partial(finish_kernel, len(delta)),
        grid_spec=pltpu.PrefetchScalarGridSpec(
            num_scalar_prefetch=1,
            grid=(size,),
            in_specs=[spec] * (1 + len(delta)) + [pl.BlockSpec((None, cols, out), lambda k, me: (0, k, 0))],
            out_specs=[
                pl.BlockSpec((None, rows, cols), lambda k, me: (me[0] ^ k, 0, 0)),
                pl.BlockSpec((rows, out), lambda k, me: (0, 0)),
            ],
            scratch_shapes=[pltpu.VMEM((rows, out), jnp.float32)],
        ),
        out_shape=[
            jax.ShapeDtypeStruct((size, rows, cols), jnp.bfloat16),
            jax.ShapeDtypeStruct((rows, out), jnp.bfloat16),
        ],
        compiler_params=pltpu.CompilerParams(vmem_limit_bytes=VMEM_CAP),
        cost_estimate=pl.CostEstimate(flops=2 * rows * width * out, bytes_accessed=2 * width * (4 * rows + out), transcendentals=0),
        name="finish",
    )(me.reshape(1), hidden, *delta, proj)


def proj_kernel(scale, first, last, count, chunk, me_ref, *refs):
    pieces = refs[:count]
    z_ref, s_ref = refs[count : count + 2]
    outs = refs[count + (2 if first else 3) : -4]
    sq_ref, total, feat, error_buf = refs[-4:]
    k = pl.program_id(0)
    rows, width = z_ref.shape

    @pl.when(k == 0)
    def _():
        sq_ref[...] = jnp.zeros_like(sq_ref)
        if first:
            total[...] = jnp.zeros_like(total)
        else:
            total[...] = refs[count + 2][...]

    for i in range(count):

        @pl.when(k == i)
        def _():
            feat[...] = pieces[i][...]

    for r in range(rows // chunk):
        part = slice(r * chunk, (r + 1) * chunk)
        error = errors_at(z_ref, s_ref, part)[0]
        error_buf[part, :] = error.astype(jnp.bfloat16)
        sq_ref[...] += jnp.sum((error * error).reshape(chunk // 8, 8, width), axis=0)
    total[...] += lax.dot_general(feat[...], error_buf[...], (((0,), (0,)), ((), ())), preferred_element_type=jnp.float32)

    @pl.when(k == pl.num_programs(0) - 1)
    def _():
        if last:
            half = total.shape[0] // 2
            outs[0][...] = (scale * total[:half, :]).astype(jnp.bfloat16)
            outs[1][...] = (scale * total[half:, :]).astype(jnp.bfloat16)
        else:
            outs[0][...] = total[...]


def proj_part(me, pieces, targets, states, parity, scale, total, last, chunk=16):
    n_seq, _, width = states.shape
    size = n_seq
    rows, cols = pieces[0].shape
    whole = pl.BlockSpec((cols, width), lambda k, me: (0, 0))
    in_specs = [pl.BlockSpec((rows, cols), lambda k, me: (0, 0))] * size + [
        pl.BlockSpec((rows, width), lambda k, me: (me[0] ^ k, 0)),
        pl.BlockSpec((None, rows, width), lambda k, me: (2 * ((me[0] ^ k) // 2) + parity, (me[0] ^ k) % 2, 0)),
    ]
    args = [me.reshape(1), *pieces, targets, states]
    if total is not None:
        in_specs.append(whole)
        args.append(total)
    outs = [(cols // 2, jnp.bfloat16)] * 2 if last else [(cols, jnp.float32)]
    return pl.pallas_call(
        functools.partial(proj_kernel, scale, total is None, last, size, chunk),
        grid_spec=pltpu.PrefetchScalarGridSpec(
            num_scalar_prefetch=1,
            grid=(size,),
            in_specs=in_specs,
            out_specs=[pl.BlockSpec((h, width), lambda k, me: (0, 0)) for h, _ in outs] + [pl.BlockSpec((8, width), lambda k, me: (0, 0))],
            scratch_shapes=[
                pltpu.VMEM((cols, width), jnp.float32),
                pltpu.VMEM((rows, cols), jnp.bfloat16),
                pltpu.VMEM((rows, width), jnp.bfloat16),
            ],
        ),
        out_shape=[jax.ShapeDtypeStruct((h, width), t) for h, t in outs] + [jax.ShapeDtypeStruct((8, width), jnp.float32)],
        compiler_params=pltpu.CompilerParams(vmem_limit_bytes=VMEM_CAP),
        cost_estimate=pl.CostEstimate(flops=2 * size * rows * cols * width, bytes_accessed=size * rows * (4 * width + 2 * cols), transcendentals=0),
        name="proj",
    )(*args)


def down_kernel(scale, first, last, chunk, cuts, z_ref, s_ref, u_ref, *refs):
    d_ref, *outs = refs[0 if first else 1 : -3]
    total, z_scale, s_scale = refs[-3:]
    k = pl.program_id(0) * pl.num_programs(1) + pl.program_id(1)

    @pl.when(k == 0)
    def _():
        total[...] = jnp.zeros_like(total) if first else refs[0][...]

    width = z_ref.shape[1]
    for r in range(z_ref.shape[0] // chunk):
        part = slice(r * chunk, (r + 1) * chunk)
        state = s_ref[part, :].astype(jnp.float32)
        square = jnp.sum(state * state, axis=-1, keepdims=True) / width
        cross = jnp.sum(state * z_ref[part, :].astype(jnp.float32), axis=-1, keepdims=True) / width
        inv = lax.rsqrt(square + EPS)
        lean = inv * cross - inv * inv * square
        z_scale[part, :] = jnp.broadcast_to(-scale * inv, (chunk, 128))
        s_scale[part, :] = jnp.broadcast_to(scale * inv * inv * (1.0 + lean), (chunk, 128))
    for r in range(z_ref.shape[0] // chunk):
        part = slice(r * chunk, (r + 1) * chunk)
        d_ref[part, :] = (s_ref[part, :].astype(jnp.float32) * s_scale[part, :1] + z_ref[part, :].astype(jnp.float32) * z_scale[part, :1]).astype(jnp.bfloat16)
    cols = total.shape[0]
    for h in range(cuts):
        part = slice(h * cols // cuts, (h + 1) * cols // cuts)
        total[part, :] += lax.dot_general(u_ref[:, part], d_ref[...], (((0,), (0,)), ((), ())), preferred_element_type=jnp.float32)

    @pl.when(k == pl.num_programs(0) * pl.num_programs(1) - 1)
    def _():
        if last:
            outs[0][...] = total[: cols // 2, :].astype(jnp.bfloat16)
            outs[1][...] = total[cols // 2 :, :].astype(jnp.bfloat16)
        else:
            outs[0][...] = total[...]


def down_part_of(ups, targets, states, parity, scale, total, last, block=512, chunk=16, cuts=1):
    n_seq, seq_len, width = states.shape
    half = n_seq // 2
    cols = ups.shape[1]
    rows = half * seq_len
    steps = seq_len // block
    spec = lambda w: pl.BlockSpec((block, w), lambda i, j: (i * steps + j, 0))
    whole = pl.BlockSpec((cols, width), lambda i, j: (0, 0), pipeline_mode=pl.Buffered(1))
    in_specs = [spec(width), pl.BlockSpec((None, block, width), lambda i, j: (2 * i + parity, j, 0)), spec(cols)]
    args = [targets, states, ups]
    if total is not None:
        in_specs.append(whole)
        args.append(total)
    outs = [(cols // 2, jnp.bfloat16)] * 2 if last else [(cols, jnp.float32)]
    return pl.pallas_call(
        functools.partial(down_kernel, scale, total is None, last, chunk, cuts),
        grid=(half, steps),
        in_specs=in_specs,
        out_specs=[spec(width)] + [pl.BlockSpec((h, width), lambda i, j: (0, 0), pipeline_mode=pl.Buffered(1)) for h, _ in outs],
        out_shape=[jax.ShapeDtypeStruct((rows, width), jnp.bfloat16)] + [jax.ShapeDtypeStruct((h, width), t) for h, t in outs],
        scratch_shapes=[pltpu.VMEM((cols, width), jnp.float32), pltpu.VMEM((block, 128), jnp.float32), pltpu.VMEM((block, 128), jnp.float32)],
        compiler_params=pltpu.CompilerParams(vmem_limit_bytes=VMEM_CAP),
        cost_estimate=pl.CostEstimate(flops=2 * rows * width * cols, bytes_accessed=rows * (6 * width + 2 * cols), transcendentals=0),
        name="down",
    )(*args)


def place_kernel(count, owner_ref, half_ref, *refs):
    for h in range(count):

        @pl.when(pl.program_id(0) == h)
        def _():
            refs[-1][...] = refs[h][...].astype(jnp.float32)


def place(out, pieces, owners, halves, shape, by_cols, block=512):
    rows, cols = pieces[0].shape
    block = min(block, rows)
    steps = rows // block
    count = len(pieces)
    specs = [pl.BlockSpec((block, cols), lambda h, i, owner, half, own=own: (jnp.where(h < own, 0, jnp.where(h > own, steps - 1, i)), 0)) for own in range(count)]
    if by_cols:
        where = lambda h, i, owner, half: (half[h] * steps + i, owner[h])
    else:
        where = lambda h, i, owner, half: ((owner[h] * 2 + half[h]) * steps + i, 0)
    args = [jnp.stack(owners).astype(jnp.int32), jnp.array(halves, jnp.int32), *pieces]
    alias = {}
    if out is not None:
        specs.append(pl.BlockSpec(memory_space=pl.ANY))
        args.append(out)
        alias = {count + 2: 0}
    return pl.pallas_call(
        functools.partial(place_kernel, count),
        grid_spec=pltpu.PrefetchScalarGridSpec(
            num_scalar_prefetch=2,
            grid=(count, steps),
            in_specs=specs,
            out_specs=pl.BlockSpec((block, cols), where),
        ),
        out_shape=jax.ShapeDtypeStruct(shape, jnp.float32),
        input_output_aliases=alias,
        compiler_params=pltpu.CompilerParams(vmem_limit_bytes=VMEM_CAP),
        cost_estimate=pl.CostEstimate(flops=count * rows * cols, bytes_accessed=6 * count * rows * cols, transcendentals=0),
        name="place",
    )(*args)


def gelu_slope(pre):
    scale = 0.7978845608028654
    square = pre * pre
    bend = jnp.tanh(scale * pre * (1.0 + 0.044715 * square))
    return 0.5 * (1.0 + bend) + (0.5 * scale) * pre * (1.0 - bend * bend) * (1.0 + 0.134145 * square)


def rest_kernel(first, last, sub, me_ref, d_ref, p_ref, a_ref, s_ref, up_ref, down_ref, *refs):
    outs, (gain_ref, total, dp) = refs[:-3], refs[-3:]
    outs = outs[0 if first else 1 :]
    k = pl.program_id(0) * pl.num_programs(1) + pl.program_id(1)
    rows, width = s_ref.shape

    @pl.when(k == 0)
    def _():
        gain_ref[...] = jnp.zeros_like(gain_ref)
        total[...] = jnp.zeros_like(total) if first else refs[0][...]

    for r in range(rows // sub):
        part = slice(r * sub, (r + 1) * sub)
        d_up = lax.dot_general(d_ref[part, :], down_ref[...], (((1,), (1,)), ((), ())), preferred_element_type=jnp.float32)
        dp[part, :] = (gelu_slope(p_ref[part, :]) * d_up).astype(jnp.bfloat16)
    total[...] += lax.dot_general(a_ref[...], dp[...], (((0,), (0,)), ((), ())), preferred_element_type=jnp.float32)
    for r in range(rows // sub):
        part = slice(r * sub, (r + 1) * sub)
        state = s_ref[part, :].astype(jnp.float32)
        inv = lax.rsqrt(jnp.mean(state * state, axis=-1, keepdims=True) + EPS)
        d_act = lax.dot_general(dp[part, :], up_ref[...], (((1,), (1,)), ((), ())), preferred_element_type=jnp.float32)
        gain_ref[...] += jnp.sum((d_act * (s_ref[part, :].astype(jnp.float32) * inv)).reshape(sub // 8, 8, width), axis=0)

    @pl.when(k == pl.num_programs(0) * pl.num_programs(1) - 1)
    def _():
        if last:
            half = width // 2
            outs[0][...] = total[:half, :].astype(jnp.bfloat16)
            outs[1][...] = total[half:, :].astype(jnp.bfloat16)
        else:
            outs[0][...] = total[...]


def rest_part(me, d_out, pre, act, states, up, down, parity, total, last, block=512, sub=256):
    n_seq, seq_len, width = states.shape
    cols = pre.shape[1]
    half = n_seq // 2
    rows = half * seq_len
    steps = seq_len // block
    spec = lambda w: pl.BlockSpec((block, w), lambda i, j, me: (i * steps + j, 0))
    once = pl.Buffered(1)
    whole = lambda h: pl.BlockSpec((h, cols), lambda i, j, me: (0, 0), pipeline_mode=once)
    in_specs = [
        spec(width),
        spec(cols),
        spec(width),
        pl.BlockSpec((None, block, width), lambda i, j, me: (2 * i + parity, j, 0)),
        pl.BlockSpec((None, width, cols), lambda i, j, me: (0, 0, me[0]), pipeline_mode=once),
        pl.BlockSpec((None, cols, width), lambda i, j, me: (0, me[0], 0), pipeline_mode=once),
    ]
    args = [me.reshape(1), d_out, pre, act, states, up, down]
    if total is not None:
        in_specs.append(whole(width))
        args.append(total)
    outs = [(width // 2, jnp.bfloat16)] * 2 if last else [(width, jnp.float32)]
    return pl.pallas_call(
        functools.partial(rest_kernel, total is None, last, sub),
        grid_spec=pltpu.PrefetchScalarGridSpec(
            num_scalar_prefetch=1,
            grid=(half, steps),
            in_specs=in_specs,
            out_specs=[whole(h) for h, _ in outs] + [pl.BlockSpec((8, width), lambda i, j, me: (0, 0))],
            scratch_shapes=[pltpu.VMEM((width, cols), jnp.float32), pltpu.VMEM((block, cols), jnp.bfloat16)],
        ),
        out_shape=[jax.ShapeDtypeStruct((h, cols), t) for h, t in outs] + [jax.ShapeDtypeStruct((8, width), jnp.float32)],
        compiler_params=pltpu.CompilerParams(vmem_limit_bytes=VMEM_CAP),
        cost_estimate=pl.CostEstimate(flops=6 * rows * width * cols, bytes_accessed=rows * (6 * width + 4 * cols), transcendentals=rows * cols),
        name="rest",
    )(*args)


def flip(value, bits, size):
    return lax.ppermute(value, AXES, [(i, i ^ bits) for i in range(size)])


def send(halves, size):
    first, second = halves
    have = {(0, 0): first, (0, 1): second}
    have[2, 0], have[4, 1] = flip(first, 2, size), flip(second, 4, size)
    have[2, 1], have[4, 0] = flip(second, 2, size), flip(first, 4, size)
    have[1, 0], have[1, 1] = flip(first, 1, size), flip(second, 1, size)
    return have


def relay(have, size):
    diag = {(6, 1): flip(have[4, 1], 2, size), (6, 0): flip(have[2, 0], 4, size)}
    near = {(bits | 1, half): flip(have[bits, half], 1, size) for bits in (2, 4) for half in range(2)}
    far = {(7, half): flip(diag[6, half], 1, size) for half in range(2)}
    return {**have, **diag, **near, **far}


def collect(out, have, me, chips, dep, shape, by_cols):
    for bits in chips:
        keys = [(bits | core, half) for half in range(2) for core in range(2)]
        pieces = after([have[key] for key in keys], dep)
        out = place(out, pieces, [me ^ key[0] for key in keys], [key[1] for key in keys], shape, by_cols)
        dep = ()
    return out


def solution(mesh):
    size = mesh.shape["data"] * mesh.shape["model"]

    def step(teacher_in, student_in, teacher_gain, teacher_up_w, teacher_down, student_gain, student_up, student_down, student_proj):
        me = lax.axis_index("data") * 2 + lax.axis_index("model")
        n_layers = teacher_up_w.shape[0]
        t_width = teacher_in.shape[2]
        _, seq_len, s_width = student_in.shape
        s_hidden = student_up.shape[2]
        part = s_hidden // size
        total = size * seq_len * s_width
        grad_scale = 2.0 / total

        own = student_in[0]
        side = lax.axis_index("model")
        last = n_layers - 1
        hidden = [teacher_in, teacher_in]

        def finish(c, delta):
            feats, target = finish_part(me, hidden[c], delta, student_proj, size)
            targets = lax.all_gather(target, AXES, axis=0, tiled=True)
            pieces = [flip(feats[bits], bits, size) if bits else feats[0] for bits in range(size)]
            return target, targets, pieces

        def normed(c, delta, layer):
            hidden[c], act = teacher_norm(hidden[c], delta, teacher_gain, layer, c)
            return act, lax.all_gather(act, "model", axis=0, tiled=True)

        def teach(act, layer, **window):
            return mlp(act, teacher_up_w, teacher_down, layer, **window)

        acts = [normed(c, (), 0)[1] for c in range(2)]
        for layer in range(n_layers):
            if layer == 0:
                all_in = lax.all_gather(after(own, acts[0]), AXES, axis=0, tiled=False)
            if layer == 1:
                all_out = lax.all_gather(after(own_out, acts[0]), AXES, axis=0, tiled=False)
            partial = teach(acts[0], layer)
            delta_0 = (lax.psum_scatter(partial, "model", scatter_dimension=0, tiled=True),)
            if layer == 0:
                partial = teach(acts[1], layer)
                delta_1 = (lax.psum_scatter(partial, "model", scatter_dimension=0, tiled=True),)
                act, acts[0] = normed(0, after(delta_0, partial), layer + 1)
                own_act = teacher_norm(after(own, act), (), student_gain, 0)[1]
                own_out = mlp(own_act, student_up, student_down, 0, own)
                delta_1 = after(delta_1, (own_out, all_in))
            else:
                rows = acts[1].shape[0] // 2
                partial = teach(acts[1], layer, rows=rows, where=1 - side)
                moved = flip(partial, 1, size)
                delta_0 = after(delta_0, partial)
                if layer < last:
                    ready, acts[0] = normed(0, delta_0, layer + 1)
                else:
                    ready, targets_0, feat_0 = finish(0, delta_0)
                partial = teach(after(acts[1], ready), layer, rows=rows, where=side)
                delta_1 = (partial, moved)
            if layer < last:
                if layer == 1:
                    delta_1 = after(delta_1, all_out)
                acts[1] = normed(1, delta_1, layer + 1)[1]
        target_1, targets_1, feat_1 = finish(1, delta_1)

        all_in, all_out, targets_0 = after((all_in, all_out, targets_0), target_1)
        proj_sum, square_0 = proj_part(me, feat_0, targets_0, all_out, 0, grad_scale, None, False)
        acts, pre, ups = zip(*[pre_of(me, all_in, student_gain, student_up, c, part) for c in range(2)])
        d_out_0, down_sum = down_part_of(ups[0], after(targets_0, (proj_sum, ups[1])), all_out, 0, grad_scale, None, False)
        targets_1 = after(targets_1, down_sum)
        *proj_halves, square_1 = proj_part(me, feat_1, targets_1, all_out, 1, grad_scale, proj_sum, True)
        proj_have = relay(send(proj_halves, size), size)
        loss = (jnp.sum(square_0) + jnp.sum(square_1)) / total
        d_out_1, *down_halves = down_part_of(ups[1], after(targets_1, proj_halves), all_out, 1, grad_scale, down_sum, True)
        down_have = relay(send(down_halves, size), size)
        up_sum, gain_0 = rest_part(me, after(d_out_0, down_halves), pre[0], acts[0], all_in, student_up, student_down, 0, None, False)
        *up_halves, gain_1 = rest_part(me, d_out_1, pre[1], acts[1], all_in, student_up, student_down, 1, up_sum, True)
        up_have = relay(send(up_halves, size), size)

        proj_shape, down_shape, up_shape = (t_width, s_width), (s_hidden, s_width), (s_width, s_hidden)
        grad_proj = collect(None, proj_have, me, (0, 2, 4, 6), up_halves, proj_shape, False)
        grad_down = collect(None, down_have, me, (0, 2, 4), grad_proj, down_shape, False)
        grad_down = collect(grad_down, down_have, me, (6,), grad_down, down_shape, False)
        gain_sum = jnp.sum(gain_0, axis=0) + jnp.sum(gain_1, axis=0)
        grad_gain = lax.psum(after(gain_sum, grad_down), AXES)
        grad_up = collect(None, up_have, me, (0, 2, 4, 6), (grad_down, grad_gain), up_shape, True)
        return (loss, grad_up[None], grad_down[None], grad_gain[None], grad_proj[None])

    return jax.shard_map(
        step,
        mesh=mesh,
        in_specs=(
            P("data", "model", None),
            P(("data", "model"), None, None),
            P(),
            P(None, None, "model"),
            P(None, "model", None),
            P(),
            P(),
            P(),
            P(),
        ),
        out_specs=(P(), P(), P(), P(), P()),
        check_vma=False,
    )
```

```python
import functools

import jax
import jax.numpy as jnp
from jax import lax
from jax.experimental import pallas as pl
from jax.experimental.pallas import tpu as pltpu
from jax.sharding import PartitionSpec as P


EPS = 1e-6
BF16 = jnp.bfloat16
F32 = jnp.float32
VMEM_CAP = 64 * 1024 * 1024 - 65536
AXES = ("data", "model")


PARAMS = pltpu.CompilerParams(vmem_limit_bytes=VMEM_CAP)
ONCE = pl.Buffered(1)
ANY = pl.BlockSpec(memory_space=pl.ANY)
ROWS = (((1,), (0,)), ((), ()))
BOTH_ROWS = (((0,), (0,)), ((), ()))
BOTH_COLS = (((1,), (1,)), ((), ()))


def dot(a, b, dims=ROWS):
    return lax.dot_general(a, b, dims, preferred_element_type=F32)


def fixed(*shape, **options):
    return pl.BlockSpec(shape, lambda *_: (0,) * len(shape), **options)


def cost(flops, nbytes, exps=0):
    return pl.CostEstimate(flops=flops, bytes_accessed=nbytes, transcendentals=exps)


def array(dtype, *shape):
    return jax.ShapeDtypeStruct(shape, dtype)


def inverse_rms(state):
    return lax.rsqrt(jnp.mean(state * state, axis=-1, keepdims=True) + EPS)


def cut(size, count):
    return [slice(start, start + size // count) for start in range(0, size, size // count)]


def after(values, dep):
    return lax.optimization_barrier((values, dep))[0]


def mlp_kernel(layer, steps, wide, residual, where_ref, *refs):
    if residual:
        a_hbm, up_hbm, down_hbm, s_hbm, o_hbm, a_ref, up_ref, down_ref, first, second, act, acc, out, a_sem, up_sem, down_sem, o_sem, s_ref, s_sem = refs
    else:
        a_hbm, up_hbm, down_hbm, o_hbm, a_ref, up_ref, down_ref, first, second, act, acc, out, a_sem, up_sem, down_sem, o_sem = refs
    j = pl.program_id(0)
    rows, width = acc.shape
    tile = act.shape[2]
    half = tile // 2
    parts = 4
    size = rows // parts
    now = lax.rem(j, 2)

    def a_copy(r):
        source = pl.ds(pl.multiple_of(where_ref[0] * rows + r * size, size), size)
        return pltpu.make_async_copy(a_hbm.at[source], a_ref.at[pl.ds(r * size, size)], a_sem.at[r])

    def up_copy(k):
        return pltpu.make_async_copy(up_hbm.at[layer, :, pl.ds(pl.multiple_of(k * tile, tile), tile)], up_ref.at[lax.rem(k, 2)], up_sem.at[lax.rem(k, 2)])

    def down_copy(k):
        return pltpu.make_async_copy(down_hbm.at[layer, pl.ds(pl.multiple_of(k * tile, tile), tile)], down_ref.at[lax.rem(k, 2)], down_sem.at[lax.rem(k, 2)])

    def out_copy(k):
        cols = pl.ds(k * wide, wide)
        return pltpu.make_async_copy(out.at[:, cols], o_hbm.at[:, cols], o_sem.at[k])

    @pl.when(j == 0)
    def _():
        up_copy(0).start()
        for r in range(parts):
            a_copy(r).start()
        up_copy(1).start()
        down_copy(0).start()
        if residual:
            pltpu.make_async_copy(s_hbm, s_ref, s_sem.at[0]).start()
        up_copy(0).wait()
        for r, part in enumerate(cut(rows, parts)):
            a_copy(r).wait()
            first[part, :] = dot(a_ref[part, :], up_ref[0, :, :half])
            second[part, :] = dot(a_ref[part, :], up_ref[0, :, half:])
        act[0, :, :half] = jax.nn.gelu(first[...]).astype(BF16)

    @pl.when((j > 0) & (j < steps))
    def _():
        @pl.when(j + 1 < steps)
        def _():
            up_copy(j + 1).start()

        down_copy(j).start()
        up_copy(j).wait()
        act[1 - now, :, half:] = jax.nn.gelu(second[...]).astype(BF16)
        first[...] = dot(a_ref[...], up_ref[now, :, :half])
        for part in cut(rows, parts):
            act[now, part, :half] = jax.nn.gelu(first[part, :]).astype(BF16)
            second[part, :] = dot(a_ref[part, :], up_ref[now, :, half:])

    @pl.when(j == steps)
    def _():
        act[1 - now, :, half:] = jax.nn.gelu(second[...]).astype(BF16)

    def down(first_tile, last_tile):
        down_copy(j - 1).wait()
        if last_tile and residual:
            pltpu.make_async_copy(s_hbm, s_ref, s_sem.at[0]).wait()
        for k, cols in enumerate(cut(width, width // wide)):
            total = dot(act[1 - now], down_ref[1 - now, :, cols])
            if not first_tile:
                total = acc[:, cols] + total
            if not last_tile:
                acc[:, cols] = total
            else:
                if residual:
                    total = s_ref[:, cols].astype(F32) + total
                out[:, cols] = total.astype(BF16)
                out_copy(k).start()
        if last_tile:
            for k in range(width // wide):
                out_copy(k).wait()

    @pl.when(j == 1)
    def _():
        down(True, False)

    @pl.when((j > 1) & (j < steps))
    def _():
        down(False, False)

    @pl.when(j == steps)
    def _():
        down(False, True)


def mlp(a, up, down, layer, state=None, rows=None, where=None, tile=512, wide=512):
    depth = a.shape[1]
    rows = rows or a.shape[0]
    where = jnp.zeros((1,), jnp.int32) if where is None else where.astype(jnp.int32).reshape(1)
    hidden = up.shape[2]
    width = down.shape[2]
    steps = hidden // tile
    hbm = ANY
    scratch = [
        pltpu.VMEM((rows, depth), BF16),
        pltpu.VMEM((2, depth, tile), BF16),
        pltpu.VMEM((2, tile, width), BF16),
        pltpu.VMEM((rows, tile // 2), F32),
        pltpu.VMEM((rows, tile // 2), F32),
        pltpu.VMEM((2, rows, tile), BF16),
        pltpu.VMEM((rows, width), F32),
        pltpu.VMEM((rows, width), BF16),
        pltpu.SemaphoreType.DMA((4,)),
        pltpu.SemaphoreType.DMA((2,)),
        pltpu.SemaphoreType.DMA((2,)),
        pltpu.SemaphoreType.DMA((width // wide,)),
    ]
    args = [a, up, down]
    if state is not None:
        args.append(state)
        scratch += [pltpu.VMEM((rows, width), BF16), pltpu.SemaphoreType.DMA((1,))]
    return pl.pallas_call(
        functools.partial(mlp_kernel, layer, steps, wide, state is not None),
        grid_spec=pltpu.PrefetchScalarGridSpec(
            num_scalar_prefetch=1,
            grid=(steps + 1,),
            in_specs=[hbm] * len(args),
            out_specs=hbm,
            scratch_shapes=scratch,
        ),
        out_shape=array(BF16, rows, width),
        compiler_params=PARAMS,
        cost_estimate=pl.CostEstimate(
            flops=2 * rows * hidden * (depth + width),
            bytes_accessed=2 * (rows * (depth + width) + hidden * (depth + width)),
            transcendentals=rows * hidden,
        ),
        name="mlp",
    )(where, *args)


def norm_kernel(h_ref, g_ref, a_ref):
    state = h_ref[...].astype(F32)
    inv = inverse_rms(state)
    a_ref[...] = (state * inv * g_ref[...]).astype(BF16)


def step_kernel(h_ref, *refs):
    *parts, g_ref, o_ref, a_ref = refs
    delta = parts[0][...].astype(F32)
    if len(parts) > 1:
        delta = (delta + parts[1][...].astype(F32)).astype(BF16).astype(F32)
    state = (h_ref[...].astype(F32) + delta).astype(BF16)
    o_ref[...] = state
    state = state.astype(F32)
    inv = inverse_rms(state)
    a_ref[...] = (state * inv * g_ref[...]).astype(BF16)


def teacher_norm(hidden, delta, gains, layer, which=0, block=128):
    rows, width = hidden.shape[-2:]
    spec = pl.BlockSpec((block, width), lambda i: (i, 0))
    source = spec if hidden.ndim == 2 else pl.BlockSpec((None, block, width), lambda i: (which, i, 0))
    gain_spec = fixed(1, width)
    shape = array(BF16, rows, width)
    count = rows * width
    common = dict(
        grid=(rows // block,),
        compiler_params=PARAMS,
    )
    gain = gains[layer : layer + 1]
    if not delta:
        price = cost(8 * count, 4 * count)
        return hidden, pl.pallas_call(norm_kernel, in_specs=[source, gain_spec], out_specs=spec, out_shape=shape, cost_estimate=price, name="norm", **common)(hidden, gain)
    price = cost(10 * count, 8 * count)
    return pl.pallas_call(step_kernel, in_specs=[source] + [spec] * len(delta) + [gain_spec], out_specs=[spec, spec], out_shape=[shape, shape], cost_estimate=price, name="step", **common)(hidden, *delta, gain)


def pre_kernel(sub, me_ref, s_ref, g_ref, w_ref, a_ref, p_ref, u_ref):
    for part in cut(s_ref.shape[0], s_ref.shape[0] // sub):
        state = s_ref[part, :].astype(F32)
        inv = inverse_rms(state)
        a_ref[part, :] = (state * inv * g_ref[...]).astype(BF16)
    for part in cut(s_ref.shape[0], s_ref.shape[0] // sub):
        pre = dot(a_ref[part, :], w_ref[...])
        p_ref[part, :] = pre
        u_ref[part, :] = jax.nn.gelu(pre).astype(BF16)


def pre_of(me, states, gain, weights, parity, cols, block=512, sub=256):
    n_seq, seq_len, width = states.shape
    half = n_seq // 2
    rows = half * seq_len
    steps = seq_len // block
    out = lambda w: pl.BlockSpec((block, w), lambda i, j, me: (i * steps + j, 0))
    return pl.pallas_call(
        functools.partial(pre_kernel, sub),
        grid_spec=pltpu.PrefetchScalarGridSpec(
            num_scalar_prefetch=1,
            grid=(half, steps),
            in_specs=[
                pl.BlockSpec((None, block, width), lambda i, j, me: (2 * i + parity, j, 0)),
                fixed(1, width),
                pl.BlockSpec((None, width, cols), lambda i, j, me: (0, 0, me[0])),
            ],
            out_specs=[out(width), out(cols), out(cols)],
        ),
        out_shape=[
            array(BF16, rows, width),
            array(F32, rows, cols),
            array(BF16, rows, cols),
        ],
        compiler_params=PARAMS,
        cost_estimate=cost(2 * rows * width * cols, rows * (4 * width + 6 * cols), rows * cols),
        name="pre",
    )(me.reshape(1), states, gain, weights)


def errors_at(z_ref, s_ref, part):
    state = s_ref[part, :].astype(F32)
    inv = inverse_rms(state)
    unit = state * inv
    return z_ref[part, :].astype(F32) - unit, unit, inv


def finish_kernel(count, size, me_ref, h_ref, *refs):
    parts = refs[:count]
    q_ref = refs[count]
    feats = refs[-2 - size : -2]
    z_ref, acc = refs[-2:]
    k = pl.program_id(0)
    delta = parts[0][...].astype(F32)
    if count > 1:
        delta = (delta + parts[1][...].astype(F32)).astype(BF16).astype(F32)
    feat = (h_ref[...].astype(F32) + delta).astype(BF16)
    for bits in range(size):

        @pl.when(me_ref[0] ^ k == bits)
        def _():
            feats[bits][...] = feat

    term = dot(feat, q_ref[...])

    @pl.when(k == 0)
    def _():
        acc[...] = term

    @pl.when((k > 0) & (k < size - 1))
    def _():
        acc[...] += term

    @pl.when(k == size - 1)
    def _():
        z_ref[...] = (acc[...] + term).astype(BF16)


def finish_part(me, hidden, delta, proj, size):
    rows, width = hidden.shape
    cols = width // size
    out = proj.shape[2]
    spec = pl.BlockSpec((rows, cols), lambda k, me: (0, k))
    return pl.pallas_call(
        functools.partial(finish_kernel, len(delta), size),
        grid_spec=pltpu.PrefetchScalarGridSpec(
            num_scalar_prefetch=1,
            grid=(size,),
            in_specs=[spec] * (1 + len(delta)) + [pl.BlockSpec((None, cols, out), lambda k, me: (0, k, 0))],
            out_specs=[fixed(rows, cols)] * size + [fixed(rows, out)],
            scratch_shapes=[pltpu.VMEM((rows, out), F32)],
        ),
        out_shape=[array(BF16, rows, cols)] * size + [array(BF16, rows, out)],
        compiler_params=PARAMS,
        cost_estimate=cost(2 * rows * width * out, 2 * width * (4 * rows + out)),
        name="finish",
    )(me.reshape(1), hidden, *delta, proj)


def proj_kernel(scale, first, last, count, chunk, me_ref, *refs):
    pieces = refs[:count]
    z_ref, s_ref = refs[count : count + 2]
    outs = refs[count + (2 if first else 3) : -4]
    sq_ref, total, feat, error_buf = refs[-4:]
    k = pl.program_id(0)
    rows, width = z_ref.shape

    @pl.when(k == 0)
    def _():
        sq_ref[...] = jnp.zeros_like(sq_ref)
        if first:
            total[...] = jnp.zeros_like(total)
        else:
            total[...] = refs[count + 2][...]

    for i in range(count):

        @pl.when(k == i)
        def _():
            feat[...] = pieces[i][...]

    for part in cut(rows, rows // chunk):
        error = errors_at(z_ref, s_ref, part)[0]
        error_buf[part, :] = error.astype(BF16)
        sq_ref[...] += jnp.sum((error * error).reshape(chunk // 8, 8, width), axis=0)
    total[...] += dot(feat[...], error_buf[...], BOTH_ROWS)

    @pl.when(k == pl.num_programs(0) - 1)
    def _():
        if last:
            half = total.shape[0] // 2
            outs[0][...] = (scale * total[:half, :]).astype(BF16)
            outs[1][...] = (scale * total[half:, :]).astype(BF16)
        else:
            outs[0][...] = total[...]


def proj_part(me, pieces, targets, states, parity, scale, total, last, chunk=16):
    n_seq, _, width = states.shape
    size = n_seq
    rows, cols = pieces[0].shape
    whole = fixed(cols, width)
    in_specs = [fixed(rows, cols)] * size + [
        pl.BlockSpec((rows, width), lambda k, me: (me[0] ^ k, 0)),
        pl.BlockSpec((None, rows, width), lambda k, me: (2 * ((me[0] ^ k) // 2) + parity, (me[0] ^ k) % 2, 0)),
    ]
    args = [me.reshape(1), *pieces, targets, states]
    if total is not None:
        in_specs.append(whole)
        args.append(total)
    outs = [(cols // 2, BF16)] * 2 if last else [(cols, F32)]
    return pl.pallas_call(
        functools.partial(proj_kernel, scale, total is None, last, size, chunk),
        grid_spec=pltpu.PrefetchScalarGridSpec(
            num_scalar_prefetch=1,
            grid=(size,),
            in_specs=in_specs,
            out_specs=[fixed(h, width) for h, _ in outs] + [fixed(8, width)],
            scratch_shapes=[
                pltpu.VMEM((cols, width), F32),
                pltpu.VMEM((rows, cols), BF16),
                pltpu.VMEM((rows, width), BF16),
            ],
        ),
        out_shape=[array(t, h, width) for h, t in outs] + [array(F32, 8, width)],
        compiler_params=PARAMS,
        cost_estimate=cost(2 * size * rows * cols * width, size * rows * (4 * width + 2 * cols)),
        name="proj",
    )(*args)


def down_kernel(scale, first, last, chunk, z_ref, s_ref, u_ref, *refs):
    d_ref, *outs = refs[0 if first else 1 : -3]
    total, z_scale, s_scale = refs[-3:]
    k = pl.program_id(0) * pl.num_programs(1) + pl.program_id(1)

    @pl.when(k == 0)
    def _():
        total[...] = jnp.zeros_like(total) if first else refs[0][...]

    width = z_ref.shape[1]
    for part in cut(z_ref.shape[0], z_ref.shape[0] // chunk):
        state = s_ref[part, :].astype(F32)
        square = jnp.sum(state * state, axis=-1, keepdims=True) / width
        cross = jnp.sum(state * z_ref[part, :].astype(F32), axis=-1, keepdims=True) / width
        inv = lax.rsqrt(square + EPS)
        lean = inv * cross - inv * inv * square
        z_scale[part, :] = jnp.broadcast_to(-scale * inv, (chunk, 128))
        s_scale[part, :] = jnp.broadcast_to(scale * inv * inv * (1.0 + lean), (chunk, 128))
    for part in cut(z_ref.shape[0], z_ref.shape[0] // chunk):
        d_ref[part, :] = (s_ref[part, :].astype(F32) * s_scale[part, :1] + z_ref[part, :].astype(F32) * z_scale[part, :1]).astype(BF16)
    cols = total.shape[0]
    total[...] += dot(u_ref[...], d_ref[...], BOTH_ROWS)

    @pl.when(k == pl.num_programs(0) * pl.num_programs(1) - 1)
    def _():
        if last:
            outs[0][...] = total[: cols // 2, :].astype(BF16)
            outs[1][...] = total[cols // 2 :, :].astype(BF16)
        else:
            outs[0][...] = total[...]


def down_part_of(ups, targets, states, parity, scale, total, last, block=512, chunk=16):
    n_seq, seq_len, width = states.shape
    half = n_seq // 2
    cols = ups.shape[1]
    rows = half * seq_len
    steps = seq_len // block
    spec = lambda w: pl.BlockSpec((block, w), lambda i, j: (i * steps + j, 0))
    whole = fixed(cols, width, pipeline_mode=ONCE)
    in_specs = [spec(width), pl.BlockSpec((None, block, width), lambda i, j: (2 * i + parity, j, 0)), spec(cols)]
    args = [targets, states, ups]
    if total is not None:
        in_specs.append(whole)
        args.append(total)
    outs = [(cols // 2, BF16)] * 2 if last else [(cols, F32)]
    return pl.pallas_call(
        functools.partial(down_kernel, scale, total is None, last, chunk),
        grid=(half, steps),
        in_specs=in_specs,
        out_specs=[spec(width)] + [fixed(h, width, pipeline_mode=ONCE) for h, _ in outs],
        out_shape=[array(BF16, rows, width)] + [array(t, h, width) for h, t in outs],
        scratch_shapes=[pltpu.VMEM((cols, width), F32), pltpu.VMEM((block, 128), F32), pltpu.VMEM((block, 128), F32)],
        compiler_params=PARAMS,
        cost_estimate=cost(2 * rows * width * cols, rows * (6 * width + 2 * cols)),
        name="down",
    )(*args)


def place_kernel(count, ahead, owner_ref, half_ref, *refs):
    pieces = refs[:count]
    out_ref, buf, sem = refs[-3:]
    block = out_ref.shape[0]
    steps = pl.num_programs(1)
    now = pl.program_id(0) * steps + pl.program_id(1)
    slots = ahead + 1

    def copy(own, step):
        slot = lax.rem(step, slots)
        rows = pl.ds(pl.multiple_of(lax.rem(step, steps) * block, block), block)
        return pltpu.make_async_copy(pieces[own].at[rows], buf.at[slot], sem.at[slot])

    def fetch(step):
        for own in range(count):

            @pl.when((step >= own * steps) & (step < (own + 1) * steps))
            def _():
                copy(own, step).start()

    @pl.when(now == 0)
    def _():
        for step in range(ahead):
            fetch(step)

    fetch(now + ahead)
    copy(0, now).wait()
    out_ref[...] = buf[lax.rem(now, slots)].astype(F32)


def place(out, pieces, owners, halves, shape, by_cols, ahead=3):
    rows, cols = pieces[0].shape
    block = rows // 2
    count = len(pieces)
    if by_cols:
        where = lambda h, i, owner, half: (half[h] * 2 + i, owner[h])
    else:
        where = lambda h, i, owner, half: ((owner[h] * 2 + half[h]) * 2 + i, 0)
    args = [jnp.stack(owners).astype(jnp.int32), jnp.array(halves, jnp.int32), *pieces]
    alias = {}
    if out is not None:
        alias = {len(args): 0}
        args.append(out)
    return pl.pallas_call(
        functools.partial(place_kernel, count, ahead),
        grid_spec=pltpu.PrefetchScalarGridSpec(
            num_scalar_prefetch=2,
            grid=(count, 2),
            in_specs=[ANY] * (len(args) - 2),
            out_specs=pl.BlockSpec((block, cols), where),
            scratch_shapes=[pltpu.VMEM((ahead + 1, block, cols), BF16), pltpu.SemaphoreType.DMA((ahead + 1,))],
        ),
        out_shape=array(F32, *shape),
        input_output_aliases=alias,
        compiler_params=PARAMS,
        cost_estimate=cost(count * rows * cols, 6 * count * rows * cols),
        name="place",
    )(*args)


def gelu_slope(pre):
    scale = 0.7978845608028654
    square = pre * pre
    bend = jnp.tanh(scale * pre * (1.0 + 0.044715 * square))
    return 0.5 * (1.0 + bend) + (0.5 * scale) * pre * (1.0 - bend * bend) * (1.0 + 0.134145 * square)


def rest_kernel(first, last, sub, me_ref, d_ref, p_ref, a_ref, s_ref, up_ref, down_ref, *refs):
    outs, (gain_ref, total, dp) = refs[:-3], refs[-3:]
    outs = outs[0 if first else 1 :]
    k = pl.program_id(0) * pl.num_programs(1) + pl.program_id(1)
    rows, width = s_ref.shape

    @pl.when(k == 0)
    def _():
        gain_ref[...] = jnp.zeros_like(gain_ref)
        total[...] = jnp.zeros_like(total) if first else refs[0][...]

    for part in cut(rows, rows // sub):
        d_up = dot(d_ref[part, :], down_ref[...], BOTH_COLS)
        dp[part, :] = (gelu_slope(p_ref[part, :]) * d_up).astype(BF16)
    total[...] += dot(a_ref[...], dp[...], BOTH_ROWS)
    for part in cut(rows, rows // sub):
        state = s_ref[part, :].astype(F32)
        inv = inverse_rms(state)
        d_act = dot(dp[part, :], up_ref[...], BOTH_COLS)
        gain_ref[...] += jnp.sum((d_act * (s_ref[part, :].astype(F32) * inv)).reshape(sub // 8, 8, width), axis=0)

    @pl.when(k == pl.num_programs(0) * pl.num_programs(1) - 1)
    def _():
        if last:
            half = width // 2
            outs[0][...] = total[:half, :].astype(BF16)
            outs[1][...] = total[half:, :].astype(BF16)
        else:
            outs[0][...] = total[...]


def rest_part(me, d_out, pre, act, states, up, down, parity, total, last, block=512, sub=256):
    n_seq, seq_len, width = states.shape
    cols = pre.shape[1]
    half = n_seq // 2
    rows = half * seq_len
    steps = seq_len // block
    spec = lambda w: pl.BlockSpec((block, w), lambda i, j, me: (i * steps + j, 0))
    whole = lambda h: fixed(h, cols, pipeline_mode=ONCE)
    in_specs = [
        spec(width),
        spec(cols),
        spec(width),
        pl.BlockSpec((None, block, width), lambda i, j, me: (2 * i + parity, j, 0)),
        pl.BlockSpec((None, width, cols), lambda i, j, me: (0, 0, me[0]), pipeline_mode=ONCE),
        pl.BlockSpec((None, cols, width), lambda i, j, me: (0, me[0], 0), pipeline_mode=ONCE),
    ]
    args = [me.reshape(1), d_out, pre, act, states, up, down]
    if total is not None:
        in_specs.append(whole(width))
        args.append(total)
    outs = [(width // 2, BF16)] * 2 if last else [(width, F32)]
    return pl.pallas_call(
        functools.partial(rest_kernel, total is None, last, sub),
        grid_spec=pltpu.PrefetchScalarGridSpec(
            num_scalar_prefetch=1,
            grid=(half, steps),
            in_specs=in_specs,
            out_specs=[whole(h) for h, _ in outs] + [fixed(8, width)],
            scratch_shapes=[pltpu.VMEM((width, cols), F32), pltpu.VMEM((block, cols), BF16)],
        ),
        out_shape=[array(t, h, cols) for h, t in outs] + [array(F32, 8, width)],
        compiler_params=PARAMS,
        cost_estimate=cost(6 * rows * width * cols, rows * (6 * width + 4 * cols), rows * cols),
        name="rest",
    )(*args)


def flip(value, bits, size):
    return lax.ppermute(value, AXES, [(i, i ^ bits) for i in range(size)])


CORE, X, Y = 1, 2, 4


def send(halves, size):
    have = {(0, half): value for half, value in enumerate(halves)}

    def pass_on(*moves):
        for bits, half in moves:
            have[bits, half] = flip(halves[half], bits, size)

    pass_on((X, 0), (Y, 1))
    pass_on((X, 1), (Y, 0))
    pass_on((CORE, 0), (CORE, 1))
    return have


def relay(have, size, dep=()):
    firsts = after((have[X, 0], have[Y, 1]), dep)
    diag = {(X | Y, half): flip(value, (X | Y) ^ bits, size) for half, (bits, value) in enumerate(zip((X, Y), firsts))}
    near = {(bits | CORE, half): flip(have[bits, half], CORE, size) for bits in (X, Y) for half in range(2)}
    far = {(bits | CORE, half): flip(value, CORE, size) for (bits, half), value in diag.items()}
    return {**have, **diag, **near, **far}


def collect(out, have, me, chips, dep, shape, by_cols):
    keys = [(bits | core, half) for bits in chips for half in range(2) for core in range(2)]
    pieces = after([have[key] for key in keys], dep)
    return place(out, pieces, [me ^ key[0] for key in keys], [key[1] for key in keys], shape, by_cols)


def solution(mesh):
    size = mesh.shape["data"] * mesh.shape["model"]

    def step(teacher_in, student_in, teacher_gain, teacher_up_w, teacher_down, student_gain, student_up, student_down, student_proj):
        me = lax.axis_index("data") * 2 + lax.axis_index("model")
        n_layers = teacher_up_w.shape[0]
        t_width = teacher_in.shape[2]
        _, seq_len, s_width = student_in.shape
        s_hidden = student_up.shape[2]
        part = s_hidden // size
        total = size * seq_len * s_width
        grad_scale = 2.0 / total

        own = student_in[0]
        side = lax.axis_index("model")
        last = n_layers - 1
        hidden = [teacher_in, teacher_in]

        def finish(c, delta):
            *feats, target = finish_part(me, hidden[c], delta, student_proj, size)
            targets = lax.all_gather(target, AXES, axis=0, tiled=True)
            pieces = [flip(feats[bits], bits, size) if bits else feats[0] for bits in range(size)]
            return target, targets, pieces

        def normed(c, delta, layer):
            hidden[c], act = teacher_norm(hidden[c], delta, teacher_gain, layer, c)
            return act, lax.all_gather(act, "model", axis=0, tiled=True)

        def teach(act, layer, **window):
            return mlp(act, teacher_up_w, teacher_down, layer, **window)

        acts = [normed(c, (), 0)[1] for c in range(2)]
        for layer in range(n_layers):
            if layer == 0:
                all_in = lax.all_gather(after(own, acts[0]), AXES, axis=0, tiled=False)
            if layer == 1:
                all_out = lax.all_gather(after(own_out, acts[0]), AXES, axis=0, tiled=False)
            partial = teach(acts[0], layer)
            delta_0 = (lax.psum_scatter(partial, "model", scatter_dimension=0, tiled=True),)
            if layer == 0:
                partial = teach(acts[1], layer)
                delta_1 = (lax.psum_scatter(partial, "model", scatter_dimension=0, tiled=True),)
                act, acts[0] = normed(0, after(delta_0, partial), layer + 1)
                own_act = teacher_norm(after(own, act), (), student_gain, 0)[1]
                own_out = mlp(own_act, student_up, student_down, 0, own)
                delta_1 = after(delta_1, (own_out, all_in))
            else:
                rows = acts[1].shape[0] // 2
                partial = teach(acts[1], layer, rows=rows, where=1 - side)
                moved = flip(partial, 1, size)
                delta_0 = after(delta_0, partial)
                if layer < last:
                    ready, acts[0] = normed(0, delta_0, layer + 1)
                else:
                    ready, targets_0, feat_0 = finish(0, delta_0)
                partial = teach(after(acts[1], ready), layer, rows=rows, where=side)
                delta_1 = (partial, moved)
            if layer < last:
                if layer == 1:
                    delta_1 = after(delta_1, all_out)
                acts[1] = normed(1, delta_1, layer + 1)[1]
        target_1, targets_1, feat_1 = finish(1, delta_1)

        all_in, all_out = after((all_in, all_out), target_1)
        acts, pre, ups = zip(*[pre_of(me, all_in, student_gain, student_up, c, part) for c in range(2)])
        proj_sum, square_0 = proj_part(me, feat_0, after(targets_0, ups), all_out, 0, grad_scale, None, False)
        d_out_0, down_sum = down_part_of(ups[0], after(targets_0, (proj_sum, ups[1])), all_out, 0, grad_scale, None, False)
        targets_1 = after(targets_1, down_sum)
        *proj_halves, square_1 = proj_part(me, feat_1, targets_1, all_out, 1, grad_scale, proj_sum, True)
        proj_have = relay(send(proj_halves, size), size)
        loss = jnp.sum(square_0 + square_1) / total
        d_out_1, *down_halves = down_part_of(ups[1], after(targets_1, proj_halves), all_out, 1, grad_scale, down_sum, True)
        down_have = relay(send(down_halves, size), size)
        up_sum, gain_0 = rest_part(me, after(d_out_0, down_halves), pre[0], acts[0], all_in, student_up, student_down, 0, None, False)
        *up_halves, gain_1 = rest_part(me, d_out_1, pre[1], acts[1], all_in, student_up, student_down, 1, up_sum, True)
        up_have = send(up_halves, size)
        grad_gain = jnp.sum(gain_0 + gain_1, axis=0)
        for bits in (CORE, X, Y):
            grad_gain = grad_gain + flip(grad_gain, bits, size)

        grad_proj = collect(None, proj_have, me, (0, X, Y, X | Y), up_halves, (t_width, s_width), False)
        grad_down = collect(None, down_have, me, (0, X, Y), grad_proj, (s_hidden, s_width), False)
        up_have = relay(up_have, size, grad_down)
        grad_down = collect(grad_down, down_have, me, (X | Y,), (), (s_hidden, s_width), False)
        shape = (s_width, s_hidden)
        grad_up = collect(None, up_have, me, (0,), grad_down, shape, True)
        grad_up = collect(grad_up, up_have, me, (X, Y), (), shape, True)
        grad_up = collect(grad_up, up_have, me, (X | Y,), (), shape, True)
        return (loss, grad_up[None], grad_down[None], grad_gain[None], grad_proj[None])

    return jax.shard_map(
        step,
        mesh=mesh,
        in_specs=(
            P("data", "model", None),
            P(("data", "model"), None, None),
            P(),
            P(None, None, "model"),
            P(None, "model", None),
            P(),
            P(),
            P(),
            P(),
        ),
        out_specs=(P(), P(), P(), P(), P()),
        check_vma=False,
    )
```

```python
import functools

import jax
import jax.numpy as jnp
from jax import lax
from jax.experimental import pallas as pl
from jax.experimental.pallas import tpu as pltpu
from jax.sharding import PartitionSpec as P


EPS = 1e-6
BF16 = jnp.bfloat16
F32 = jnp.float32
GELU_SCALE = 0.7978845608028654
GELU_BEND = 0.044715
VMEM_CAP = 64 * 1024 * 1024 - 65536
AXES = ("data", "model")


PARAMS = pltpu.CompilerParams(vmem_limit_bytes=VMEM_CAP)
ONCE = pl.Buffered(1)
ANY = pl.BlockSpec(memory_space=pl.ANY)
ROWS = (((1,), (0,)), ((), ()))
BOTH_ROWS = (((0,), (0,)), ((), ()))
BOTH_COLS = (((1,), (1,)), ((), ()))


def dot(a, b, dims=ROWS):
    return lax.dot_general(a, b, dims, preferred_element_type=F32)


def fixed(*shape, **options):
    return pl.BlockSpec(shape, lambda *_: (0,) * len(shape), **options)


def cost(flops, nbytes, exps=0):
    return pl.CostEstimate(flops=flops, bytes_accessed=nbytes, transcendentals=exps)


def array(dtype, *shape):
    return jax.ShapeDtypeStruct(shape, dtype)


def inverse_rms(state):
    return lax.rsqrt(jnp.mean(state * state, axis=-1, keepdims=True) + EPS)


def cut(size, count):
    return [slice(start, start + size // count) for start in range(0, size, size // count)]


def after(values, dep):
    return lax.optimization_barrier((values, dep))[0]


def mlp_kernel(layer, steps, wide, residual, where_ref, *refs):
    if residual:
        a_hbm, up_hbm, down_hbm, s_hbm, o_hbm, a_ref, up_ref, down_ref, first, second, act, acc, out, a_sem, up_sem, down_sem, o_sem, s_ref, s_sem = refs
    else:
        a_hbm, up_hbm, down_hbm, o_hbm, a_ref, up_ref, down_ref, first, second, act, acc, out, a_sem, up_sem, down_sem, o_sem = refs
    j = pl.program_id(0)
    rows, width = acc.shape
    tile = act.shape[2]
    half = tile // 2
    parts = 4
    size = rows // parts
    now = lax.rem(j, 2)

    def a_copy(r):
        source = pl.ds(pl.multiple_of(where_ref[0] * rows + r * size, size), size)
        return pltpu.make_async_copy(a_hbm.at[source], a_ref.at[pl.ds(r * size, size)], a_sem.at[r])

    def up_copy(k):
        return pltpu.make_async_copy(up_hbm.at[layer, :, pl.ds(pl.multiple_of(k * tile, tile), tile)], up_ref.at[lax.rem(k, 2)], up_sem.at[lax.rem(k, 2)])

    def down_copy(k):
        return pltpu.make_async_copy(down_hbm.at[layer, pl.ds(pl.multiple_of(k * tile, tile), tile)], down_ref.at[lax.rem(k, 2)], down_sem.at[lax.rem(k, 2)])

    def out_copy(k):
        cols = pl.ds(k * wide, wide)
        return pltpu.make_async_copy(out.at[:, cols], o_hbm.at[:, cols], o_sem.at[k])

    @pl.when(j == 0)
    def _():
        up_copy(0).start()
        for r in range(parts):
            a_copy(r).start()
        up_copy(1).start()
        down_copy(0).start()
        if residual:
            pltpu.make_async_copy(s_hbm, s_ref, s_sem.at[0]).start()
        up_copy(0).wait()
        for r, part in enumerate(cut(rows, parts)):
            a_copy(r).wait()
            first[part, :] = dot(a_ref[part, :], up_ref[0, :, :half])
            second[part, :] = dot(a_ref[part, :], up_ref[0, :, half:])
        act[0, :, :half] = gelu(first[...]).astype(BF16)

    @pl.when((j > 0) & (j < steps))
    def _():
        @pl.when(j + 1 < steps)
        def _():
            up_copy(j + 1).start()

        down_copy(j).start()
        up_copy(j).wait()
        act[1 - now, :, half:] = gelu(second[...]).astype(BF16)
        first[...] = dot(a_ref[...], up_ref[now, :, :half])
        for part in cut(rows, parts):
            act[now, part, :half] = gelu(first[part, :]).astype(BF16)
            second[part, :] = dot(a_ref[part, :], up_ref[now, :, half:])

    @pl.when(j == steps)
    def _():
        act[1 - now, :, half:] = gelu(second[...]).astype(BF16)

    def down(first_tile, last_tile):
        down_copy(j - 1).wait()
        if last_tile and residual:
            pltpu.make_async_copy(s_hbm, s_ref, s_sem.at[0]).wait()
        for k, cols in enumerate(cut(width, width // wide)):
            total = dot(act[1 - now], down_ref[1 - now, :, cols])
            if not first_tile:
                total = acc[:, cols] + total
            if not last_tile:
                acc[:, cols] = total
            else:
                if residual:
                    total = s_ref[:, cols].astype(F32) + total
                out[:, cols] = total.astype(BF16)
                out_copy(k).start()
        if last_tile:
            for k in range(width // wide):
                out_copy(k).wait()

    @pl.when(j == 1)
    def _():
        down(True, False)

    @pl.when((j > 1) & (j < steps))
    def _():
        down(False, False)

    @pl.when(j == steps)
    def _():
        down(False, True)


def mlp(a, up, down, layer, state=None, rows=None, where=None, tile=512, wide=512):
    depth = a.shape[1]
    rows = rows or a.shape[0]
    where = jnp.zeros((1,), jnp.int32) if where is None else where.astype(jnp.int32).reshape(1)
    hidden = up.shape[2]
    width = down.shape[2]
    steps = hidden // tile
    hbm = ANY
    scratch = [
        pltpu.VMEM((rows, depth), BF16),
        pltpu.VMEM((2, depth, tile), BF16),
        pltpu.VMEM((2, tile, width), BF16),
        pltpu.VMEM((rows, tile // 2), F32),
        pltpu.VMEM((rows, tile // 2), F32),
        pltpu.VMEM((2, rows, tile), BF16),
        pltpu.VMEM((rows, width), F32),
        pltpu.VMEM((rows, width), BF16),
        pltpu.SemaphoreType.DMA((4,)),
        pltpu.SemaphoreType.DMA((2,)),
        pltpu.SemaphoreType.DMA((2,)),
        pltpu.SemaphoreType.DMA((width // wide,)),
    ]
    args = [a, up, down]
    if state is not None:
        args.append(state)
        scratch += [pltpu.VMEM((rows, width), BF16), pltpu.SemaphoreType.DMA((1,))]
    return pl.pallas_call(
        functools.partial(mlp_kernel, layer, steps, wide, state is not None),
        grid_spec=pltpu.PrefetchScalarGridSpec(
            num_scalar_prefetch=1,
            grid=(steps + 1,),
            in_specs=[hbm] * len(args),
            out_specs=hbm,
            scratch_shapes=scratch,
        ),
        out_shape=array(BF16, rows, width),
        compiler_params=PARAMS,
        cost_estimate=pl.CostEstimate(
            flops=2 * rows * hidden * (depth + width),
            bytes_accessed=2 * (rows * (depth + width) + hidden * (depth + width)),
            transcendentals=rows * hidden,
        ),
        name="mlp",
    )(where, *args)


def norm_kernel(h_ref, g_ref, a_ref):
    state = h_ref[...].astype(F32)
    inv = inverse_rms(state)
    a_ref[...] = (state * inv * g_ref[...]).astype(BF16)


def step_kernel(h_ref, *refs):
    *parts, g_ref, o_ref, a_ref = refs
    delta = parts[0][...].astype(F32)
    if len(parts) > 1:
        delta = (delta + parts[1][...].astype(F32)).astype(BF16).astype(F32)
    state = (h_ref[...].astype(F32) + delta).astype(BF16)
    o_ref[...] = state
    state = state.astype(F32)
    inv = inverse_rms(state)
    a_ref[...] = (state * inv * g_ref[...]).astype(BF16)


def teacher_norm(hidden, delta, gains, layer, which=0, size=2**18):
    rows, width = hidden.shape[-2:]
    block = size // width
    spec = pl.BlockSpec((block, width), lambda i: (i, 0))
    source = spec if hidden.ndim == 2 else pl.BlockSpec((None, block, width), lambda i: (which, i, 0))
    gain_spec = fixed(1, width)
    shape = array(BF16, rows, width)
    count = rows * width
    common = dict(
        grid=(rows // block,),
        compiler_params=PARAMS,
    )
    gain = gains[layer : layer + 1]
    if not delta:
        price = cost(8 * count, 4 * count)
        return hidden, pl.pallas_call(norm_kernel, in_specs=[source, gain_spec], out_specs=spec, out_shape=shape, cost_estimate=price, name="norm", **common)(hidden, gain)
    price = cost(10 * count, 8 * count)
    return pl.pallas_call(step_kernel, in_specs=[source] + [spec] * len(delta) + [gain_spec], out_specs=[spec, spec], out_shape=[shape, shape], cost_estimate=price, name="step", **common)(hidden, *delta, gain)


def pre_kernel(sub, me_ref, s_ref, g_ref, w_ref, a_ref, p_ref, u_ref):
    for part in cut(s_ref.shape[0], s_ref.shape[0] // sub):
        state = s_ref[part, :].astype(F32)
        inv = inverse_rms(state)
        a_ref[part, :] = (state * inv * g_ref[...]).astype(BF16)
    for part in cut(s_ref.shape[0], s_ref.shape[0] // sub):
        pre = dot(a_ref[part, :], w_ref[...])
        p_ref[part, :] = pre
        u_ref[part, :] = gelu(pre).astype(BF16)


def pre_of(me, states, gain, weights, parity, cols, block=512, sub=256):
    n_seq, seq_len, width = states.shape
    half = n_seq // 2
    rows = half * seq_len
    steps = seq_len // block
    out = lambda w: pl.BlockSpec((block, w), lambda i, j, me: (i * steps + j, 0))
    return pl.pallas_call(
        functools.partial(pre_kernel, sub),
        grid_spec=pltpu.PrefetchScalarGridSpec(
            num_scalar_prefetch=1,
            grid=(half, steps),
            in_specs=[
                pl.BlockSpec((None, block, width), lambda i, j, me: (2 * i + parity, j, 0)),
                fixed(1, width),
                pl.BlockSpec((None, width, cols), lambda i, j, me: (0, 0, me[0])),
            ],
            out_specs=[out(width), out(cols), out(cols)],
        ),
        out_shape=[
            array(BF16, rows, width),
            array(F32, rows, cols),
            array(BF16, rows, cols),
        ],
        compiler_params=PARAMS,
        cost_estimate=cost(2 * rows * width * cols, rows * (4 * width + 6 * cols), rows * cols),
        name="pre",
    )(me.reshape(1), states, gain, weights)


def errors_at(z_ref, s_ref, part):
    state = s_ref[part, :].astype(F32)
    inv = inverse_rms(state)
    unit = state * inv
    return z_ref[part, :].astype(F32) - unit, unit, inv


def finish_kernel(count, size, wide, me_ref, h_ref, *refs):
    parts = refs[:count]
    q_ref = refs[count]
    feats = refs[-2 - size : -2]
    z_ref, acc = refs[-2:]
    k = pl.program_id(0)
    delta = parts[0][...].astype(F32)
    if count > 1:
        delta = (delta + parts[1][...].astype(F32)).astype(BF16).astype(F32)
    feat = (h_ref[...].astype(F32) + delta).astype(BF16)
    for own, cols in enumerate(cut(feat.shape[1], wide)):
        for bits in range(size):

            @pl.when(me_ref[0] ^ (k * wide + own) == bits)
            def _():
                feats[bits][...] = feat[:, cols]

    @pl.when(k == 0)
    def _():
        acc[...] = jnp.zeros_like(acc)

    acc[...] += dot(feat, q_ref[...])

    @pl.when(k == pl.num_programs(0) - 1)
    def _():
        z_ref[...] = acc[...].astype(BF16)


def finish_part(me, hidden, delta, proj, size, wide=2):
    rows, width = hidden.shape
    cols = width // size
    out = proj.shape[2]
    deep = cols * wide
    spec = pl.BlockSpec((rows, deep), lambda k, me: (0, k))
    return pl.pallas_call(
        functools.partial(finish_kernel, len(delta), size, wide),
        grid_spec=pltpu.PrefetchScalarGridSpec(
            num_scalar_prefetch=1,
            grid=(size // wide,),
            in_specs=[spec] * (1 + len(delta)) + [pl.BlockSpec((None, deep, out), lambda k, me: (0, k, 0))],
            out_specs=[fixed(rows, cols)] * size + [fixed(rows, out)],
            scratch_shapes=[pltpu.VMEM((rows, out), F32)],
        ),
        out_shape=[array(BF16, rows, cols)] * size + [array(BF16, rows, out)],
        compiler_params=PARAMS,
        cost_estimate=cost(2 * rows * width * out, 2 * width * (4 * rows + out)),
        name="finish",
    )(me.reshape(1), hidden, *delta, proj)


def proj_kernel(scale, first, last, count, chunk, me_ref, *refs):
    pieces = refs[:count]
    z_ref, s_ref = refs[count : count + 2]
    outs = refs[count + (2 if first else 3) : -4]
    sq_ref, total, feat, error_buf = refs[-4:]
    k = pl.program_id(0)
    rows, width = z_ref.shape

    @pl.when(k == 0)
    def _():
        sq_ref[...] = jnp.zeros_like(sq_ref)
        if first:
            total[...] = jnp.zeros_like(total)
        else:
            total[...] = refs[count + 2][...]

    for i in range(count):

        @pl.when(k == i)
        def _():
            feat[...] = pieces[i][...]

    for part in cut(rows, rows // chunk):
        error = errors_at(z_ref, s_ref, part)[0]
        error_buf[part, :] = error.astype(BF16)
        sq_ref[...] += jnp.sum((error * error).reshape(chunk // 8, 8, width), axis=0)
    total[...] += dot(feat[...], error_buf[...], BOTH_ROWS)

    @pl.when(k == pl.num_programs(0) - 1)
    def _():
        if last:
            half = total.shape[0] // 2
            outs[0][...] = (scale * total[:half, :]).astype(BF16)
            outs[1][...] = (scale * total[half:, :]).astype(BF16)
        else:
            outs[0][...] = total[...]


def proj_part(me, pieces, targets, states, parity, scale, total, last, chunk=16):
    n_seq, _, width = states.shape
    size = n_seq
    rows, cols = pieces[0].shape
    whole = fixed(cols, width)
    in_specs = [fixed(rows, cols)] * size + [
        pl.BlockSpec((rows, width), lambda k, me: (me[0] ^ k, 0)),
        pl.BlockSpec((None, rows, width), lambda k, me: (2 * ((me[0] ^ k) // 2) + parity, (me[0] ^ k) % 2, 0)),
    ]
    args = [me.reshape(1), *pieces, targets, states]
    if total is not None:
        in_specs.append(whole)
        args.append(total)
    outs = [(cols // 2, BF16)] * 2 if last else [(cols, F32)]
    return pl.pallas_call(
        functools.partial(proj_kernel, scale, total is None, last, size, chunk),
        grid_spec=pltpu.PrefetchScalarGridSpec(
            num_scalar_prefetch=1,
            grid=(size,),
            in_specs=in_specs,
            out_specs=[fixed(h, width) for h, _ in outs] + [fixed(8, width)],
            scratch_shapes=[
                pltpu.VMEM((cols, width), F32),
                pltpu.VMEM((rows, cols), BF16),
                pltpu.VMEM((rows, width), BF16),
            ],
        ),
        out_shape=[array(t, h, width) for h, t in outs] + [array(F32, 8, width)],
        compiler_params=PARAMS,
        cost_estimate=cost(2 * size * rows * cols * width, size * rows * (4 * width + 2 * cols)),
        name="proj",
    )(*args)


def down_kernel(scale, first, last, chunk, z_ref, s_ref, u_ref, *refs):
    d_ref, *outs = refs[0 if first else 1 : -3]
    total, z_scale, s_scale = refs[-3:]
    k = pl.program_id(0) * pl.num_programs(1) + pl.program_id(1)

    @pl.when(k == 0)
    def _():
        total[...] = jnp.zeros_like(total) if first else refs[0][...]

    width = z_ref.shape[1]
    for part in cut(z_ref.shape[0], z_ref.shape[0] // chunk):
        state = s_ref[part, :].astype(F32)
        square = jnp.sum(state * state, axis=-1, keepdims=True) / width
        cross = jnp.sum(state * z_ref[part, :].astype(F32), axis=-1, keepdims=True) / width
        inv = lax.rsqrt(square + EPS)
        lean = inv * cross - inv * inv * square
        z_scale[part, :] = jnp.broadcast_to(-scale * inv, (chunk, 128))
        s_scale[part, :] = jnp.broadcast_to(scale * inv * inv * (1.0 + lean), (chunk, 128))
    for part in cut(z_ref.shape[0], z_ref.shape[0] // chunk):
        d_ref[part, :] = (s_ref[part, :].astype(F32) * s_scale[part, :1] + z_ref[part, :].astype(F32) * z_scale[part, :1]).astype(BF16)
    cols = total.shape[0]
    total[...] += dot(u_ref[...], d_ref[...], BOTH_ROWS)

    @pl.when(k == pl.num_programs(0) * pl.num_programs(1) - 1)
    def _():
        if last:
            outs[0][...] = total[: cols // 2, :].astype(BF16)
            outs[1][...] = total[cols // 2 :, :].astype(BF16)
        else:
            outs[0][...] = total[...]


def down_part_of(ups, targets, states, parity, scale, total, last, block=512, chunk=16):
    n_seq, seq_len, width = states.shape
    half = n_seq // 2
    cols = ups.shape[1]
    rows = half * seq_len
    steps = seq_len // block
    spec = lambda w: pl.BlockSpec((block, w), lambda i, j: (i * steps + j, 0))
    whole = fixed(cols, width, pipeline_mode=ONCE)
    in_specs = [spec(width), pl.BlockSpec((None, block, width), lambda i, j: (2 * i + parity, j, 0)), spec(cols)]
    args = [targets, states, ups]
    if total is not None:
        in_specs.append(whole)
        args.append(total)
    outs = [(cols // 2, BF16)] * 2 if last else [(cols, F32)]
    return pl.pallas_call(
        functools.partial(down_kernel, scale, total is None, last, chunk),
        grid=(half, steps),
        in_specs=in_specs,
        out_specs=[spec(width)] + [fixed(h, width, pipeline_mode=ONCE) for h, _ in outs],
        out_shape=[array(BF16, rows, width)] + [array(t, h, width) for h, t in outs],
        scratch_shapes=[pltpu.VMEM((cols, width), F32), pltpu.VMEM((block, 128), F32), pltpu.VMEM((block, 128), F32)],
        compiler_params=PARAMS,
        cost_estimate=cost(2 * rows * width * cols, rows * (6 * width + 2 * cols)),
        name="down",
    )(*args)


def place_kernel(count, ahead, owner_ref, half_ref, *refs):
    pieces = refs[:count]
    out_ref, buf, sem = refs[-3:]
    block = out_ref.shape[0]
    steps = pl.num_programs(1)
    now = pl.program_id(0) * steps + pl.program_id(1)
    slots = ahead + 1

    def copy(own, step):
        slot = lax.rem(step, slots)
        rows = pl.ds(pl.multiple_of(lax.rem(step, steps) * block, block), block)
        return pltpu.make_async_copy(pieces[own].at[rows], buf.at[slot], sem.at[slot])

    def fetch(step):
        for own in range(count):

            @pl.when((step >= own * steps) & (step < (own + 1) * steps))
            def _():
                copy(own, step).start()

    @pl.when(now == 0)
    def _():
        for step in range(ahead):
            fetch(step)

    fetch(now + ahead)
    copy(0, now).wait()
    out_ref[...] = buf[lax.rem(now, slots)].astype(F32)


def place(out, pieces, owners, halves, shape, by_cols, ahead=3):
    rows, cols = pieces[0].shape
    block = rows // 2
    count = len(pieces)
    if by_cols:
        where = lambda h, i, owner, half: (half[h] * 2 + i, owner[h])
    else:
        where = lambda h, i, owner, half: ((owner[h] * 2 + half[h]) * 2 + i, 0)
    args = [jnp.stack(owners).astype(jnp.int32), jnp.array(halves, jnp.int32), *pieces]
    alias = {}
    if out is not None:
        alias = {len(args): 0}
        args.append(out)
    return pl.pallas_call(
        functools.partial(place_kernel, count, ahead),
        grid_spec=pltpu.PrefetchScalarGridSpec(
            num_scalar_prefetch=2,
            grid=(count, 2),
            in_specs=[ANY] * (len(args) - 2),
            out_specs=pl.BlockSpec((block, cols), where),
            scratch_shapes=[pltpu.VMEM((ahead + 1, block, cols), BF16), pltpu.SemaphoreType.DMA((ahead + 1,))],
        ),
        out_shape=array(F32, *shape),
        input_output_aliases=alias,
        compiler_params=PARAMS,
        cost_estimate=cost(count * rows * cols, 6 * count * rows * cols),
        name="place",
    )(*args)


def gelu(pre):
    half = 0.5 * pre
    return half + half * jnp.tanh(pre * (GELU_SCALE + GELU_SCALE * GELU_BEND * (pre * pre)))


def gelu_slope(pre):
    square = pre * pre
    bend = jnp.tanh(GELU_SCALE * pre * (1.0 + GELU_BEND * square))
    return 0.5 * (1.0 + bend) + (0.5 * GELU_SCALE) * pre * (1.0 - bend * bend) * (1.0 + 3.0 * GELU_BEND * square)


def rest_kernel(first, last, sub, me_ref, d_ref, p_ref, a_ref, s_ref, up_ref, down_ref, *refs):
    outs, (gain_ref, total, dp) = refs[:-3], refs[-3:]
    outs = outs[0 if first else 1 :]
    k = pl.program_id(0) * pl.num_programs(1) + pl.program_id(1)
    rows, width = s_ref.shape

    @pl.when(k == 0)
    def _():
        gain_ref[...] = jnp.zeros_like(gain_ref)
        total[...] = jnp.zeros_like(total) if first else refs[0][...]

    for part in cut(rows, rows // sub):
        d_up = dot(d_ref[part, :], down_ref[...], BOTH_COLS)
        dp[part, :] = (gelu_slope(p_ref[part, :]) * d_up).astype(BF16)
    total[...] += dot(a_ref[...], dp[...], BOTH_ROWS)
    for part in cut(rows, rows // sub):
        state = s_ref[part, :].astype(F32)
        inv = inverse_rms(state)
        d_act = dot(dp[part, :], up_ref[...], BOTH_COLS)
        gain_ref[...] += jnp.sum((d_act * (s_ref[part, :].astype(F32) * inv)).reshape(sub // 8, 8, width), axis=0)

    @pl.when(k == pl.num_programs(0) * pl.num_programs(1) - 1)
    def _():
        if last:
            half = width // 2
            outs[0][...] = total[:half, :].astype(BF16)
            outs[1][...] = total[half:, :].astype(BF16)
        else:
            outs[0][...] = total[...]


def rest_part(me, d_out, pre, act, states, up, down, parity, total, last, block=512, sub=256):
    n_seq, seq_len, width = states.shape
    cols = pre.shape[1]
    half = n_seq // 2
    rows = half * seq_len
    steps = seq_len // block
    spec = lambda w: pl.BlockSpec((block, w), lambda i, j, me: (i * steps + j, 0))
    whole = lambda h: fixed(h, cols, pipeline_mode=ONCE)
    in_specs = [
        spec(width),
        spec(cols),
        spec(width),
        pl.BlockSpec((None, block, width), lambda i, j, me: (2 * i + parity, j, 0)),
        pl.BlockSpec((None, width, cols), lambda i, j, me: (0, 0, me[0]), pipeline_mode=ONCE),
        pl.BlockSpec((None, cols, width), lambda i, j, me: (0, me[0], 0), pipeline_mode=ONCE),
    ]
    args = [me.reshape(1), d_out, pre, act, states, up, down]
    if total is not None:
        in_specs.append(whole(width))
        args.append(total)
    outs = [(width // 2, BF16)] * 2 if last else [(width, F32)]
    return pl.pallas_call(
        functools.partial(rest_kernel, total is None, last, sub),
        grid_spec=pltpu.PrefetchScalarGridSpec(
            num_scalar_prefetch=1,
            grid=(half, steps),
            in_specs=in_specs,
            out_specs=[whole(h) for h, _ in outs] + [fixed(8, width)],
            scratch_shapes=[pltpu.VMEM((width, cols), F32), pltpu.VMEM((block, cols), BF16)],
        ),
        out_shape=[array(t, h, cols) for h, t in outs] + [array(F32, 8, width)],
        compiler_params=PARAMS,
        cost_estimate=cost(6 * rows * width * cols, rows * (6 * width + 4 * cols), rows * cols),
        name="rest",
    )(*args)


def flip(value, bits, size):
    return lax.ppermute(value, AXES, [(i, i ^ bits) for i in range(size)])


CORE, X, Y = 1, 2, 4


def send(halves, size):
    have = {(0, half): value for half, value in enumerate(halves)}

    def pass_on(*moves):
        for bits, half in moves:
            have[bits, half] = flip(halves[half], bits, size)

    pass_on((X, 0), (Y, 1))
    pass_on((X, 1), (Y, 0))
    pass_on((CORE, 0), (CORE, 1))
    return have


def relay(have, size, dep=()):
    firsts = after((have[X, 0], have[Y, 1]), dep)
    diag = {(X | Y, half): flip(value, (X | Y) ^ bits, size) for half, (bits, value) in enumerate(zip((X, Y), firsts))}
    near = {(bits | CORE, half): flip(have[bits, half], CORE, size) for bits in (X, Y) for half in range(2)}
    far = {(bits | CORE, half): flip(value, CORE, size) for (bits, half), value in diag.items()}
    return {**have, **diag, **near, **far}


def collect(out, have, me, chips, dep, shape, by_cols):
    keys = [(bits | core, half) for bits in chips for half in range(2) for core in range(2)]
    pieces = after([have[key] for key in keys], dep)
    return place(out, pieces, [me ^ key[0] for key in keys], [key[1] for key in keys], shape, by_cols)


def solution(mesh):
    size = mesh.shape["data"] * mesh.shape["model"]

    def step(teacher_in, student_in, teacher_gain, teacher_up_w, teacher_down, student_gain, student_up, student_down, student_proj):
        me = lax.axis_index("data") * 2 + lax.axis_index("model")
        n_layers = teacher_up_w.shape[0]
        t_width = teacher_in.shape[2]
        _, seq_len, s_width = student_in.shape
        s_hidden = student_up.shape[2]
        part = s_hidden // size
        total = size * seq_len * s_width
        grad_scale = 2.0 / total

        own = student_in[0]
        side = lax.axis_index("model")
        last = n_layers - 1
        hidden = [teacher_in, teacher_in]

        def finish(c, delta):
            *feats, target = finish_part(me, hidden[c], delta, student_proj, size)
            targets = lax.all_gather(target, AXES, axis=0, tiled=True)
            pieces = [flip(feats[bits], bits, size) if bits else feats[0] for bits in range(size)]
            return target, targets, pieces

        def normed(c, delta, layer):
            hidden[c], act = teacher_norm(hidden[c], delta, teacher_gain, layer, c)
            return act, lax.all_gather(act, "model", axis=0, tiled=True)

        def teach(act, layer, **window):
            return mlp(act, teacher_up_w, teacher_down, layer, **window)

        acts = [normed(c, (), 0)[1] for c in range(2)]
        own_act = teacher_norm(own, (), student_gain, 0)[1]
        for layer in range(n_layers):
            if layer == 0:
                all_in = lax.all_gather(after(own, (acts[0], own_act)), AXES, axis=0, tiled=False)
            if layer == 1:
                all_out = lax.all_gather(after(own_out, acts[0]), AXES, axis=0, tiled=False)
            partial = teach(acts[0], layer)
            delta_0 = (lax.psum_scatter(partial, "model", scatter_dimension=0, tiled=True),)
            if layer == 0:
                partial = teach(acts[1], layer)
                delta_1 = (lax.psum_scatter(partial, "model", scatter_dimension=0, tiled=True),)
                act, acts[0] = normed(0, after(delta_0, partial), layer + 1)
                own_out = mlp(after(own_act, act), student_up, student_down, 0, own)
                delta_1 = after(delta_1, (own_out, all_in))
            else:
                rows = acts[1].shape[0] // 2
                partial = teach(acts[1], layer, rows=rows, where=1 - side)
                moved = flip(partial, 1, size)
                delta_0 = after(delta_0, partial)
                if layer < last:
                    ready, acts[0] = normed(0, delta_0, layer + 1)
                else:
                    ready, targets_0, feat_0 = finish(0, delta_0)
                partial = teach(after(acts[1], ready), layer, rows=rows, where=side)
                delta_1 = (partial, moved)
            if layer < last:
                if layer == 1:
                    delta_1 = after(delta_1, all_out)
                acts[1] = normed(1, delta_1, layer + 1)[1]
        target_1, targets_1, feat_1 = finish(1, delta_1)

        all_in, all_out = after((all_in, all_out), target_1)
        acts, pre, ups = zip(*[pre_of(me, all_in, student_gain, student_up, c, part) for c in range(2)])
        proj_sum, square_0 = proj_part(me, feat_0, after(targets_0, ups), all_out, 0, grad_scale, None, False)
        d_out_0, down_sum = down_part_of(ups[0], after(targets_0, (proj_sum, ups[1])), all_out, 0, grad_scale, None, False)
        targets_1 = after(targets_1, down_sum)
        *proj_halves, square_1 = proj_part(me, feat_1, targets_1, all_out, 1, grad_scale, proj_sum, True)
        proj_have = relay(send(proj_halves, size), size)
        loss = jnp.sum(square_0 + square_1) / total
        d_out_1, *down_halves = down_part_of(ups[1], after(targets_1, proj_halves), all_out, 1, grad_scale, down_sum, True)
        down_have = relay(send(down_halves, size), size)
        up_sum, gain_0 = rest_part(me, after(d_out_0, down_halves), pre[0], acts[0], all_in, student_up, student_down, 0, None, False)
        *up_halves, gain_1 = rest_part(me, d_out_1, pre[1], acts[1], all_in, student_up, student_down, 1, up_sum, True)
        up_have = send(up_halves, size)
        grad_gain = jnp.sum(gain_0 + gain_1, axis=0)
        for bits in (CORE, X, Y):
            grad_gain = grad_gain + flip(grad_gain, bits, size)

        grad_proj = collect(None, proj_have, me, (0, X, Y, X | Y), up_halves, (t_width, s_width), False)
        grad_down = collect(None, down_have, me, (0, X, Y), grad_proj, (s_hidden, s_width), False)
        up_have = relay(up_have, size, grad_down)
        grad_down = collect(grad_down, down_have, me, (X | Y,), (), (s_hidden, s_width), False)
        shape = (s_width, s_hidden)
        grad_up = collect(None, up_have, me, (0,), grad_down, shape, True)
        grad_up = collect(grad_up, up_have, me, (X, Y), (), shape, True)
        grad_up = collect(grad_up, up_have, me, (X | Y,), (), shape, True)
        return (loss, grad_up[None], grad_down[None], grad_gain[None], grad_proj[None])

    return jax.shard_map(
        step,
        mesh=mesh,
        in_specs=(
            P("data", "model", None),
            P(("data", "model"), None, None),
            P(),
            P(None, None, "model"),
            P(None, "model", None),
            P(),
            P(),
            P(),
            P(),
        ),
        out_specs=(P(), P(), P(), P(), P()),
        check_vma=False,
    )
```

```python
import functools

import jax
import jax.numpy as jnp
from jax import lax
from jax.experimental import pallas as pl
from jax.experimental.pallas import tpu as pltpu
from jax.sharding import PartitionSpec as P


EPS = 1e-6
BF16 = jnp.bfloat16
F32 = jnp.float32
GELU_SCALE = 0.7978845608028654
GELU_BEND = 0.044715
VMEM_CAP = 64 * 1024 * 1024 - 65536
AXES = ("data", "model")


PARAMS = pltpu.CompilerParams(vmem_limit_bytes=VMEM_CAP)
ONCE = pl.Buffered(1)
ANY = pl.BlockSpec(memory_space=pl.ANY)
ROWS = (((1,), (0,)), ((), ()))
BOTH_ROWS = (((0,), (0,)), ((), ()))
BOTH_COLS = (((1,), (1,)), ((), ()))


def dot(a, b, dims=ROWS):
    return lax.dot_general(a, b, dims, preferred_element_type=F32)


def fixed(*shape, **options):
    return pl.BlockSpec(shape, lambda *_: (0,) * len(shape), **options)


def cost(flops, nbytes, exps=0):
    return pl.CostEstimate(flops=flops, bytes_accessed=nbytes, transcendentals=exps)


def array(dtype, *shape):
    return jax.ShapeDtypeStruct(shape, dtype)


def inverse_rms(state):
    return lax.rsqrt(jnp.mean(state * state, axis=-1, keepdims=True) + EPS)


def cut(size, count):
    return [slice(start, start + size // count) for start in range(0, size, size // count)]


def after(values, dep):
    return lax.optimization_barrier((values, dep))[0]


def mlp_kernel(layer, steps, wide, residual, where_ref, *refs):
    if residual:
        a_hbm, up_hbm, down_hbm, s_hbm, o_hbm, a_ref, up_ref, down_ref, first, second, act, acc, out, a_sem, up_sem, down_sem, o_sem, s_ref, s_sem = refs
    else:
        a_hbm, up_hbm, down_hbm, o_hbm, a_ref, up_ref, down_ref, first, second, act, acc, out, a_sem, up_sem, down_sem, o_sem = refs
    j = pl.program_id(0)
    rows, width = acc.shape
    tile = act.shape[2]
    half = tile // 2
    parts = 4
    size = rows // parts
    now = lax.rem(j, 2)

    def a_copy(r):
        source = pl.ds(pl.multiple_of(where_ref[0] * rows + r * size, size), size)
        return pltpu.make_async_copy(a_hbm.at[source], a_ref.at[pl.ds(r * size, size)], a_sem.at[r])

    def up_copy(k):
        return pltpu.make_async_copy(up_hbm.at[layer, :, pl.ds(pl.multiple_of(k * tile, tile), tile)], up_ref.at[lax.rem(k, 2)], up_sem.at[lax.rem(k, 2)])

    def down_copy(k):
        return pltpu.make_async_copy(down_hbm.at[layer, pl.ds(pl.multiple_of(k * tile, tile), tile)], down_ref.at[lax.rem(k, 2)], down_sem.at[lax.rem(k, 2)])

    def out_copy(k):
        cols = pl.ds(k * wide, wide)
        return pltpu.make_async_copy(out.at[:, cols], o_hbm.at[:, cols], o_sem.at[k])

    @pl.when(j == 0)
    def _():
        up_copy(0).start()
        for r in range(parts):
            a_copy(r).start()
        up_copy(1).start()
        down_copy(0).start()
        if residual:
            pltpu.make_async_copy(s_hbm, s_ref, s_sem.at[0]).start()
        up_copy(0).wait()
        for r, part in enumerate(cut(rows, parts)):
            a_copy(r).wait()
            first[part, :] = dot(a_ref[part, :], up_ref[0, :, :half])
            second[part, :] = dot(a_ref[part, :], up_ref[0, :, half:])
        act[0, :, :half] = gelu(first[...]).astype(BF16)

    @pl.when((j > 0) & (j < steps))
    def _():
        @pl.when(j + 1 < steps)
        def _():
            up_copy(j + 1).start()

        down_copy(j).start()
        up_copy(j).wait()
        act[1 - now, :, half:] = gelu(second[...]).astype(BF16)
        first[...] = dot(a_ref[...], up_ref[now, :, :half])
        for part in cut(rows, parts):
            act[now, part, :half] = gelu(first[part, :]).astype(BF16)
            second[part, :] = dot(a_ref[part, :], up_ref[now, :, half:])

    @pl.when(j == steps)
    def _():
        act[1 - now, :, half:] = gelu(second[...]).astype(BF16)

    def down(first_tile, last_tile):
        down_copy(j - 1).wait()
        if last_tile and residual:
            pltpu.make_async_copy(s_hbm, s_ref, s_sem.at[0]).wait()
        for k, cols in enumerate(cut(width, width // wide)):
            total = dot(act[1 - now], down_ref[1 - now, :, cols])
            if not first_tile:
                total = acc[:, cols] + total
            if not last_tile:
                acc[:, cols] = total
            else:
                if residual:
                    total = s_ref[:, cols].astype(F32) + total
                out[:, cols] = total.astype(BF16)
                out_copy(k).start()
        if last_tile:
            for k in range(width // wide):
                out_copy(k).wait()

    @pl.when(j == 1)
    def _():
        down(True, False)

    @pl.when((j > 1) & (j < steps))
    def _():
        down(False, False)

    @pl.when(j == steps)
    def _():
        down(False, True)


def mlp(a, up, down, layer, state=None, rows=None, where=None, tile=512, wide=512):
    depth = a.shape[1]
    rows = rows or a.shape[0]
    where = jnp.zeros((1,), jnp.int32) if where is None else where.astype(jnp.int32).reshape(1)
    hidden = up.shape[2]
    width = down.shape[2]
    steps = hidden // tile
    hbm = ANY
    scratch = [
        pltpu.VMEM((rows, depth), BF16),
        pltpu.VMEM((2, depth, tile), BF16),
        pltpu.VMEM((2, tile, width), BF16),
        pltpu.VMEM((rows, tile // 2), F32),
        pltpu.VMEM((rows, tile // 2), F32),
        pltpu.VMEM((2, rows, tile), BF16),
        pltpu.VMEM((rows, width), F32),
        pltpu.VMEM((rows, width), BF16),
        pltpu.SemaphoreType.DMA((4,)),
        pltpu.SemaphoreType.DMA((2,)),
        pltpu.SemaphoreType.DMA((2,)),
        pltpu.SemaphoreType.DMA((width // wide,)),
    ]
    args = [a, up, down]
    if state is not None:
        args.append(state)
        scratch += [pltpu.VMEM((rows, width), BF16), pltpu.SemaphoreType.DMA((1,))]
    return pl.pallas_call(
        functools.partial(mlp_kernel, layer, steps, wide, state is not None),
        grid_spec=pltpu.PrefetchScalarGridSpec(
            num_scalar_prefetch=1,
            grid=(steps + 1,),
            in_specs=[hbm] * len(args),
            out_specs=hbm,
            scratch_shapes=scratch,
        ),
        out_shape=array(BF16, rows, width),
        compiler_params=PARAMS,
        cost_estimate=pl.CostEstimate(
            flops=2 * rows * hidden * (depth + width),
            bytes_accessed=2 * (rows * (depth + width) + hidden * (depth + width)),
            transcendentals=rows * hidden,
        ),
        name="mlp",
    )(where, *args)


def norm_kernel(h_ref, g_ref, a_ref):
    state = h_ref[...].astype(F32)
    inv = inverse_rms(state)
    a_ref[...] = (state * inv * g_ref[...]).astype(BF16)


def step_kernel(h_ref, *refs):
    *parts, g_ref, o_ref, a_ref = refs
    delta = parts[0][...].astype(F32)
    if len(parts) > 1:
        delta = (delta + parts[1][...].astype(F32)).astype(BF16).astype(F32)
    state = (h_ref[...].astype(F32) + delta).astype(BF16)
    o_ref[...] = state
    state = state.astype(F32)
    inv = inverse_rms(state)
    a_ref[...] = (state * inv * g_ref[...]).astype(BF16)


def teacher_norm(hidden, delta, gains, layer, which=0, size=2**19):
    rows, width = hidden.shape[-2:]
    block = size // width
    spec = pl.BlockSpec((block, width), lambda i: (i, 0))
    source = spec if hidden.ndim == 2 else pl.BlockSpec((None, block, width), lambda i: (which, i, 0))
    gain_spec = fixed(1, width)
    shape = array(BF16, rows, width)
    count = rows * width
    common = dict(
        grid=(rows // block,),
        compiler_params=PARAMS,
    )
    gain = gains[layer : layer + 1]
    if not delta:
        price = cost(8 * count, 4 * count)
        return hidden, pl.pallas_call(norm_kernel, in_specs=[source, gain_spec], out_specs=spec, out_shape=shape, cost_estimate=price, name="norm", **common)(hidden, gain)
    price = cost(10 * count, 8 * count)
    return pl.pallas_call(step_kernel, in_specs=[source] + [spec] * len(delta) + [gain_spec], out_specs=[spec, spec], out_shape=[shape, shape], cost_estimate=price, name="step", **common)(hidden, *delta, gain)


def pre_kernel(sub, me_ref, s_ref, g_ref, w_ref, a_ref, p_ref, u_ref):
    for part in cut(s_ref.shape[0], s_ref.shape[0] // sub):
        state = s_ref[part, :].astype(F32)
        inv = inverse_rms(state)
        a_ref[part, :] = (state * inv * g_ref[...]).astype(BF16)
    for part in cut(s_ref.shape[0], s_ref.shape[0] // sub):
        pre = dot(a_ref[part, :], w_ref[...])
        p_ref[part, :] = pre
        u_ref[part, :] = gelu(pre).astype(BF16)


def pre_of(me, states, gain, weights, cols, block=512, sub=256):
    n_seq, seq_len, width = states.shape
    rows = n_seq * seq_len
    steps = seq_len // block
    out = lambda w: pl.BlockSpec((block, w), lambda i, j, me: (i * steps + j, 0))
    return pl.pallas_call(
        functools.partial(pre_kernel, sub),
        grid_spec=pltpu.PrefetchScalarGridSpec(
            num_scalar_prefetch=1,
            grid=(n_seq, steps),
            in_specs=[
                pl.BlockSpec((None, block, width), lambda i, j, me: (i, j, 0)),
                fixed(1, width),
                pl.BlockSpec((None, width, cols), lambda i, j, me: (0, 0, me[0])),
            ],
            out_specs=[out(width), out(cols), out(cols)],
        ),
        out_shape=[
            array(BF16, rows, width),
            array(F32, rows, cols),
            array(BF16, rows, cols),
        ],
        compiler_params=PARAMS,
        cost_estimate=cost(2 * rows * width * cols, rows * (4 * width + 6 * cols), rows * cols),
        name="pre",
    )(me.reshape(1), states, gain, weights)


def errors_at(z_ref, s_ref, part):
    state = s_ref[part, :].astype(F32)
    inv = inverse_rms(state)
    unit = state * inv
    return z_ref[part, :].astype(F32) - unit, unit, inv


def finish_kernel(count, size, wide, me_ref, h_ref, *refs):
    parts = refs[:count]
    q_ref = refs[count]
    feats = refs[-2 - size : -2]
    z_ref, acc = refs[-2:]
    k = pl.program_id(0)
    delta = parts[0][...].astype(F32)
    if count > 1:
        delta = (delta + parts[1][...].astype(F32)).astype(BF16).astype(F32)
    feat = (h_ref[...].astype(F32) + delta).astype(BF16)
    for own, cols in enumerate(cut(feat.shape[1], wide)):
        for bits in range(size):

            @pl.when(me_ref[0] ^ (k * wide + own) == bits)
            def _():
                feats[bits][...] = feat[:, cols]

    @pl.when(k == 0)
    def _():
        acc[...] = jnp.zeros_like(acc)

    acc[...] += dot(feat, q_ref[...])

    @pl.when(k == pl.num_programs(0) - 1)
    def _():
        z_ref[...] = acc[...].astype(BF16)


def finish_part(me, hidden, delta, proj, size, wide=2):
    rows, width = hidden.shape
    cols = width // size
    out = proj.shape[2]
    deep = cols * wide
    spec = pl.BlockSpec((rows, deep), lambda k, me: (0, k))
    return pl.pallas_call(
        functools.partial(finish_kernel, len(delta), size, wide),
        grid_spec=pltpu.PrefetchScalarGridSpec(
            num_scalar_prefetch=1,
            grid=(size // wide,),
            in_specs=[spec] * (1 + len(delta)) + [pl.BlockSpec((None, deep, out), lambda k, me: (0, k, 0))],
            out_specs=[fixed(rows, cols)] * size + [fixed(rows, out)],
            scratch_shapes=[pltpu.VMEM((rows, out), F32)],
        ),
        out_shape=[array(BF16, rows, cols)] * size + [array(BF16, rows, out)],
        compiler_params=PARAMS,
        cost_estimate=cost(2 * rows * width * out, 2 * width * (4 * rows + out)),
        name="finish",
    )(me.reshape(1), hidden, *delta, proj)


def proj_kernel(scale, first, last, count, chunk, me_ref, *refs):
    pieces = refs[:count]
    z_ref, s_ref = refs[count : count + 2]
    outs = refs[count + (2 if first else 3) : -4]
    sq_ref, total, feat, error_buf = refs[-4:]
    k = pl.program_id(0)
    rows, width = z_ref.shape

    @pl.when(k == 0)
    def _():
        sq_ref[...] = jnp.zeros_like(sq_ref)
        if first:
            total[...] = jnp.zeros_like(total)
        else:
            total[...] = refs[count + 2][...]

    for i in range(count):

        @pl.when(k == i)
        def _():
            feat[...] = pieces[i][...]

    for part in cut(rows, rows // chunk):
        error = errors_at(z_ref, s_ref, part)[0]
        error_buf[part, :] = error.astype(BF16)
        sq_ref[...] += jnp.sum((error * error).reshape(chunk // 8, 8, width), axis=0)
    total[...] += dot(feat[...], error_buf[...], BOTH_ROWS)

    @pl.when(k == pl.num_programs(0) - 1)
    def _():
        if last:
            half = total.shape[0] // 2
            outs[0][...] = (scale * total[:half, :]).astype(BF16)
            outs[1][...] = (scale * total[half:, :]).astype(BF16)
        else:
            outs[0][...] = total[...]


def proj_part(me, pieces, targets, states, parity, scale, total, last, chunk=16):
    n_seq, _, width = states.shape
    size = n_seq
    rows, cols = pieces[0].shape
    whole = fixed(cols, width)
    in_specs = [fixed(rows, cols)] * size + [
        pl.BlockSpec((rows, width), lambda k, me: (me[0] ^ k, 0)),
        pl.BlockSpec((None, rows, width), lambda k, me: (2 * ((me[0] ^ k) // 2) + parity, (me[0] ^ k) % 2, 0)),
    ]
    args = [me.reshape(1), *pieces, targets, states]
    if total is not None:
        in_specs.append(whole)
        args.append(total)
    outs = [(cols // 2, BF16)] * 2 if last else [(cols, F32)]
    return pl.pallas_call(
        functools.partial(proj_kernel, scale, total is None, last, size, chunk),
        grid_spec=pltpu.PrefetchScalarGridSpec(
            num_scalar_prefetch=1,
            grid=(size,),
            in_specs=in_specs,
            out_specs=[fixed(h, width) for h, _ in outs] + [fixed(8, width)],
            scratch_shapes=[
                pltpu.VMEM((cols, width), F32),
                pltpu.VMEM((rows, cols), BF16),
                pltpu.VMEM((rows, width), BF16),
            ],
        ),
        out_shape=[array(t, h, width) for h, t in outs] + [array(F32, 8, width)],
        compiler_params=PARAMS,
        cost_estimate=cost(2 * size * rows * cols * width, size * rows * (4 * width + 2 * cols)),
        name="proj",
    )(*args)


def down_kernel(scale, first, last, chunk, z_ref, s_ref, u_ref, *refs):
    d_ref, *outs = refs[0 if first else 1 : -3]
    total, z_scale, s_scale = refs[-3:]
    k = pl.program_id(0) * pl.num_programs(1) + pl.program_id(1)

    @pl.when(k == 0)
    def _():
        total[...] = jnp.zeros_like(total) if first else refs[0][...]

    width = z_ref.shape[1]
    for part in cut(z_ref.shape[0], z_ref.shape[0] // chunk):
        state = s_ref[part, :].astype(F32)
        square = jnp.sum(state * state, axis=-1, keepdims=True) / width
        cross = jnp.sum(state * z_ref[part, :].astype(F32), axis=-1, keepdims=True) / width
        inv = lax.rsqrt(square + EPS)
        lean = inv * cross - inv * inv * square
        z_scale[part, :] = jnp.broadcast_to(-scale * inv, (chunk, 128))
        s_scale[part, :] = jnp.broadcast_to(scale * inv * inv * (1.0 + lean), (chunk, 128))
    for part in cut(z_ref.shape[0], z_ref.shape[0] // chunk):
        d_ref[part, :] = (s_ref[part, :].astype(F32) * s_scale[part, :1] + z_ref[part, :].astype(F32) * z_scale[part, :1]).astype(BF16)
    cols = total.shape[0]
    total[...] += dot(u_ref[...], d_ref[...], BOTH_ROWS)

    @pl.when(k == pl.num_programs(0) * pl.num_programs(1) - 1)
    def _():
        if last:
            outs[0][...] = total[: cols // 2, :].astype(BF16)
            outs[1][...] = total[cols // 2 :, :].astype(BF16)
        else:
            outs[0][...] = total[...]


def down_part_of(ups, targets, states, parity, scale, total, last, block=512, chunk=16):
    n_seq, seq_len, width = states.shape
    half = n_seq // 2
    cols = ups.shape[1]
    rows = half * seq_len
    steps = seq_len // block
    spec = lambda w: pl.BlockSpec((block, w), lambda i, j: (i * steps + j, 0))
    whole = fixed(cols, width, pipeline_mode=ONCE)
    natural = pl.BlockSpec((block, cols), lambda i, j: ((2 * i + parity) * steps + j, 0))
    in_specs = [spec(width), pl.BlockSpec((None, block, width), lambda i, j: (2 * i + parity, j, 0)), natural]
    args = [targets, states, ups]
    if total is not None:
        in_specs.append(whole)
        args.append(total)
    outs = [(cols // 2, BF16)] * 2 if last else [(cols, F32)]
    return pl.pallas_call(
        functools.partial(down_kernel, scale, total is None, last, chunk),
        grid=(half, steps),
        in_specs=in_specs,
        out_specs=[spec(width)] + [fixed(h, width, pipeline_mode=ONCE) for h, _ in outs],
        out_shape=[array(BF16, rows, width)] + [array(t, h, width) for h, t in outs],
        scratch_shapes=[pltpu.VMEM((cols, width), F32), pltpu.VMEM((block, 128), F32), pltpu.VMEM((block, 128), F32)],
        compiler_params=PARAMS,
        cost_estimate=cost(2 * rows * width * cols, rows * (6 * width + 2 * cols)),
        name="down",
    )(*args)


def place_kernel(count, ahead, owner_ref, half_ref, *refs):
    pieces = refs[:count]
    out_ref, buf, sem = refs[-3:]
    block = out_ref.shape[0]
    steps = pl.num_programs(1)
    now = pl.program_id(0) * steps + pl.program_id(1)
    slots = ahead + 1

    def copy(own, step):
        slot = lax.rem(step, slots)
        rows = pl.ds(pl.multiple_of(lax.rem(step, steps) * block, block), block)
        return pltpu.make_async_copy(pieces[own].at[rows], buf.at[slot], sem.at[slot])

    def fetch(step):
        for own in range(count):

            @pl.when((step >= own * steps) & (step < (own + 1) * steps))
            def _():
                copy(own, step).start()

    @pl.when(now == 0)
    def _():
        for step in range(ahead):
            fetch(step)

    fetch(now + ahead)
    copy(0, now).wait()
    out_ref[...] = buf[lax.rem(now, slots)].astype(F32)


def place(out, pieces, owners, halves, shape, by_cols, ahead=3):
    rows, cols = pieces[0].shape
    block = rows // 2
    count = len(pieces)
    if by_cols:
        where = lambda h, i, owner, half: (half[h] * 2 + i, owner[h])
    else:
        where = lambda h, i, owner, half: ((owner[h] * 2 + half[h]) * 2 + i, 0)
    args = [jnp.stack(owners).astype(jnp.int32), jnp.array(halves, jnp.int32), *pieces]
    alias = {}
    if out is not None:
        alias = {len(args): 0}
        args.append(out)
    return pl.pallas_call(
        functools.partial(place_kernel, count, ahead),
        grid_spec=pltpu.PrefetchScalarGridSpec(
            num_scalar_prefetch=2,
            grid=(count, 2),
            in_specs=[ANY] * (len(args) - 2),
            out_specs=pl.BlockSpec((block, cols), where),
            scratch_shapes=[pltpu.VMEM((ahead + 1, block, cols), BF16), pltpu.SemaphoreType.DMA((ahead + 1,))],
        ),
        out_shape=array(F32, *shape),
        input_output_aliases=alias,
        compiler_params=PARAMS,
        cost_estimate=cost(count * rows * cols, 6 * count * rows * cols),
        name="place",
    )(*args)


def gelu(pre):
    half = 0.5 * pre
    return half + half * jnp.tanh(pre * (GELU_SCALE + GELU_SCALE * GELU_BEND * (pre * pre)))


def gelu_slope(pre):
    square = pre * pre
    bend = jnp.tanh(GELU_SCALE * pre * (1.0 + GELU_BEND * square))
    return 0.5 * (1.0 + bend) + (0.5 * GELU_SCALE) * pre * (1.0 - bend * bend) * (1.0 + 3.0 * GELU_BEND * square)


def rest_kernel(first, last, sub, me_ref, d_ref, p_ref, a_ref, s_ref, up_ref, down_ref, *refs):
    outs, (gain_ref, total, dp) = refs[:-3], refs[-3:]
    outs = outs[0 if first else 1 :]
    k = pl.program_id(0) * pl.num_programs(1) + pl.program_id(1)
    rows, width = s_ref.shape

    @pl.when(k == 0)
    def _():
        gain_ref[...] = jnp.zeros_like(gain_ref)
        total[...] = jnp.zeros_like(total) if first else refs[0][...]

    for part in cut(rows, rows // sub):
        d_up = dot(d_ref[part, :], down_ref[...], BOTH_COLS)
        dp[part, :] = (gelu_slope(p_ref[part, :]) * d_up).astype(BF16)
    total[...] += dot(a_ref[...], dp[...], BOTH_ROWS)
    for part in cut(rows, rows // sub):
        state = s_ref[part, :].astype(F32)
        inv = inverse_rms(state)
        d_act = dot(dp[part, :], up_ref[...], BOTH_COLS)
        gain_ref[...] += jnp.sum((d_act * (s_ref[part, :].astype(F32) * inv)).reshape(sub // 8, 8, width), axis=0)

    @pl.when(k == pl.num_programs(0) * pl.num_programs(1) - 1)
    def _():
        if last:
            half = width // 2
            outs[0][...] = total[:half, :].astype(BF16)
            outs[1][...] = total[half:, :].astype(BF16)
        else:
            outs[0][...] = total[...]


def rest_part(me, d_out, pre, act, states, up, down, parity, total, last, block=512, sub=256):
    n_seq, seq_len, width = states.shape
    cols = pre.shape[1]
    half = n_seq // 2
    rows = half * seq_len
    steps = seq_len // block
    spec = lambda w: pl.BlockSpec((block, w), lambda i, j, me: (i * steps + j, 0))
    natural = lambda w: pl.BlockSpec((block, w), lambda i, j, me: ((2 * i + parity) * steps + j, 0))
    whole = lambda h: fixed(h, cols, pipeline_mode=ONCE)
    in_specs = [
        spec(width),
        natural(cols),
        natural(width),
        pl.BlockSpec((None, block, width), lambda i, j, me: (2 * i + parity, j, 0)),
        pl.BlockSpec((None, width, cols), lambda i, j, me: (0, 0, me[0]), pipeline_mode=ONCE),
        pl.BlockSpec((None, cols, width), lambda i, j, me: (0, me[0], 0), pipeline_mode=ONCE),
    ]
    args = [me.reshape(1), d_out, pre, act, states, up, down]
    if total is not None:
        in_specs.append(whole(width))
        args.append(total)
    outs = [(width // 2, BF16)] * 2 if last else [(width, F32)]
    return pl.pallas_call(
        functools.partial(rest_kernel, total is None, last, sub),
        grid_spec=pltpu.PrefetchScalarGridSpec(
            num_scalar_prefetch=1,
            grid=(half, steps),
            in_specs=in_specs,
            out_specs=[whole(h) for h, _ in outs] + [fixed(8, width)],
            scratch_shapes=[pltpu.VMEM((width, cols), F32), pltpu.VMEM((block, cols), BF16)],
        ),
        out_shape=[array(t, h, cols) for h, t in outs] + [array(F32, 8, width)],
        compiler_params=PARAMS,
        cost_estimate=cost(6 * rows * width * cols, rows * (6 * width + 4 * cols), rows * cols),
        name="rest",
    )(*args)


def flip(value, bits, size):
    return lax.ppermute(value, AXES, [(i, i ^ bits) for i in range(size)])


CORE, X, Y = 1, 2, 4


def send(halves, size):
    have = {(0, half): value for half, value in enumerate(halves)}

    def pass_on(*moves):
        for bits, half in moves:
            have[bits, half] = flip(halves[half], bits, size)

    pass_on((X, 0), (Y, 1))
    pass_on((X, 1), (Y, 0))
    pass_on((CORE, 0), (CORE, 1))
    return have


def relay(have, size, dep=()):
    firsts = after((have[X, 0], have[Y, 1]), dep)
    diag = {(X | Y, half): flip(value, (X | Y) ^ bits, size) for half, (bits, value) in enumerate(zip((X, Y), firsts))}
    near = {(bits | CORE, half): flip(have[bits, half], CORE, size) for bits in (X, Y) for half in range(2)}
    far = {(bits | CORE, half): flip(value, CORE, size) for (bits, half), value in diag.items()}
    return {**have, **diag, **near, **far}


def collect(out, have, me, chips, dep, shape, by_cols, cores=(0, 1)):
    keys = [(bits | core, half) for bits in chips for half in range(2) for core in cores]
    pieces = after([have[key] for key in keys], dep)
    return place(out, pieces, [me ^ key[0] for key in keys], [key[1] for key in keys], shape, by_cols)


def solution(mesh):
    size = mesh.shape["data"] * mesh.shape["model"]

    def step(teacher_in, student_in, teacher_gain, teacher_up_w, teacher_down, student_gain, student_up, student_down, student_proj):
        me = lax.axis_index("data") * 2 + lax.axis_index("model")
        n_layers = teacher_up_w.shape[0]
        t_width = teacher_in.shape[2]
        _, seq_len, s_width = student_in.shape
        s_hidden = student_up.shape[2]
        part = s_hidden // size
        t_part = t_width // size
        total = size * seq_len * s_width
        grad_scale = 2.0 / total

        own = student_in[0]
        side = lax.axis_index("model")
        last = n_layers - 1
        hidden = [teacher_in, teacher_in]

        def finish(c, delta):
            *feats, target = finish_part(me, hidden[c], delta, student_proj, size)
            targets = lax.all_gather(target, AXES, axis=0, tiled=True)
            pieces = [flip(feats[bits], bits, size) if bits else feats[0] for bits in range(size)]
            return target, targets, pieces

        def normed(c, delta, layer):
            hidden[c], act = teacher_norm(hidden[c], delta, teacher_gain, layer, c)
            return act, lax.all_gather(act, "model", axis=0, tiled=True)

        def teach(act, layer, **window):
            return mlp(act, teacher_up_w, teacher_down, layer, **window)

        acts = [normed(c, (), 0)[1] for c in range(2)]
        own_act = teacher_norm(own, (), student_gain, 0)[1]
        for layer in range(n_layers):
            if layer == 0:
                all_in = lax.all_gather(after(own, (acts[0], own_act)), AXES, axis=0, tiled=False)
            if layer == 1:
                all_out = lax.all_gather(after(own_out, acts[0]), AXES, axis=0, tiled=False)
            partial = teach(acts[0], layer)
            delta_0 = (lax.psum_scatter(partial, "model", scatter_dimension=0, tiled=True),)
            if layer == 0:
                partial = teach(acts[1], layer)
                delta_1 = (lax.psum_scatter(partial, "model", scatter_dimension=0, tiled=True),)
                act, acts[0] = normed(0, after(delta_0, partial), layer + 1)
                own_out = mlp(after(own_act, act), student_up, student_down, 0, own)
                delta_1 = after(delta_1, (own_out, all_in))
            else:
                rows = acts[1].shape[0] // 2
                partial = teach(acts[1], layer, rows=rows, where=1 - side)
                moved = flip(partial, 1, size)
                delta_0 = after(delta_0, partial)
                if layer < last:
                    ready, acts[0] = normed(0, delta_0, layer + 1)
                else:
                    feats = (hidden[0].astype(F32) + delta_0[0].astype(F32)).astype(BF16)
                    pieces = [lax.dynamic_slice(feats, (0, (me ^ bits) * t_part), (rows, t_part)) for bits in range(size)]
                    feat_0 = [flip(piece, bits, size) if bits else piece for bits, piece in enumerate(pieces)]
                    ready = dot(feats, student_proj[0]).astype(BF16)
                    targets_0 = lax.all_gather(ready, AXES, axis=0, tiled=True)
                partial = teach(after(acts[1], ready), layer, rows=rows, where=side)
                delta_1 = (partial, moved)
            if layer < last:
                if layer == 1:
                    delta_1 = after(delta_1, all_out)
                acts[1] = normed(1, delta_1, layer + 1)[1]
        target_1, targets_1, feat_1 = finish(1, delta_1)

        all_in, all_out = after((all_in, all_out), target_1)
        acts, pre, ups = pre_of(me, all_in, student_gain, student_up, part)
        proj_sum, square_0 = proj_part(me, feat_0, after(targets_0, ups), all_out, 0, grad_scale, None, False)
        d_out_0, down_sum = down_part_of(ups, after(targets_0, (proj_sum, ups)), all_out, 0, grad_scale, None, False)
        targets_1 = after(targets_1, down_sum)
        *proj_halves, square_1 = proj_part(me, feat_1, targets_1, all_out, 1, grad_scale, proj_sum, True)
        proj_have = relay(send(proj_halves, size), size)
        loss = jnp.sum(square_0 + square_1) / total
        d_out_1, *down_halves = down_part_of(ups, after(targets_1, proj_halves), all_out, 1, grad_scale, down_sum, True)
        down_have = relay(send(down_halves, size), size)
        up_sum, gain_0 = rest_part(me, after(d_out_0, down_halves), pre, acts, all_in, student_up, student_down, 0, None, False)
        *up_halves, gain_1 = rest_part(me, d_out_1, pre, acts, all_in, student_up, student_down, 1, up_sum, True)
        up_have = send(up_halves, size)
        grad_gain = jnp.sum(gain_0 + gain_1, axis=0)
        for bits in (CORE, X, Y):
            grad_gain = grad_gain + flip(grad_gain, bits, size)

        grad_proj = collect(None, proj_have, me, (0, X, Y, X | Y), up_halves, (t_width, s_width), False)
        grad_down = collect(None, down_have, me, (0, X, Y), grad_proj, (s_hidden, s_width), False)
        up_have = relay(up_have, size, grad_down)
        grad_down = collect(grad_down, down_have, me, (X | Y,), (), (s_hidden, s_width), False)
        shape = (s_width, s_hidden)
        grad_up = collect(None, up_have, me, (0,), grad_down, shape, True)
        grad_up = collect(grad_up, up_have, me, (X, Y), (), shape, True)
        for core in range(2):
            grad_up = collect(grad_up, up_have, me, (X | Y,), (), shape, True, (core,))
        return (loss, grad_up[None], grad_down[None], grad_gain[None], grad_proj[None])

    return jax.shard_map(
        step,
        mesh=mesh,
        in_specs=(
            P("data", "model", None),
            P(("data", "model"), None, None),
            P(),
            P(None, None, "model"),
            P(None, "model", None),
            P(),
            P(),
            P(),
            P(),
        ),
        out_specs=(P(), P(), P(), P(), P()),
        check_vma=False,
    )
```
